8 devices in a mesh: dp: 2 (over z, y), kv: 4 (over x, core).
Axes of the slice: x: 2, y: 2, z: 1, core: 2. Of those that a mesh axis runs over, the one named last changes fastest.
Arguments:
- x_first: bfloat16 [32, 1024], P('dp'), parts along dimension 0
- next_emb: bfloat16 [2, 32, 1024], P(None, 'dp'), parts along dimension 1
- k_cache: bfloat16 [32, 1024, 8, 64], P('dp', 'kv'), parts along dimension 0
- v_cache: bfloat16 [32, 1024, 8, 64], P('dp', 'kv'), parts along dimension 0
- seq_len: int32 [32], P('dp'), parts along dimension 0
- ln1_gain: float32 [1024], replicated
- ln1_bias: float32 [1024], replicated
- w_q: bfloat16 [1024, 1024], replicated
- b_q: float32 [1024], replicated
- w_k: bfloat16 [1024, 512], replicated
- b_k: float32 [512], replicated
- w_v: bfloat16 [1024, 512], replicated
- b_v: float32 [512], replicated
- w_o: bfloat16 [1024, 1024], replicated
- b_o: float32 [1024], replicated
- ln2_gain: float32 [1024], replicated
- ln2_bias: float32 [1024], replicated
- w_router: bfloat16 [1024, 32], replicated
- w_gate: bfloat16 [32, 1024, 512], P(None, None, 'kv')
- w_up: bfloat16 [32, 1024, 512], P(None, None, 'kv')
- w_down: bfloat16 [32, 512, 1024], P(None, 'kv')
- long_factor: float32 [32], replicated
- expert_idx: int32 [3, 32, 8], P(None, 'dp'), parts along dimension 1
- route_mask: int32 [3, 32, 8, 32], P(None, 'dp'), parts along dimension 1
Outputs:
- output 1: bfloat16 [3, 32, 1024], P(None, 'dp'), parts along dimension 1
- output 2: bfloat16 [32, 3, 8, 64], P('dp'), parts along dimension 0
- output 3: bfloat16 [32, 3, 8, 64], P('dp'), parts along dimension 0
There are 2 independent parts. The reference program is written for one: setup_inputs(seed, part) draws one part's arguments, and reference() takes and returns one part's arrays. A program takes and returns all parts, laid end to end along the dimension named above; an argument that names none is the same for every part.
All inputs are finite; a program needn't handle non-finite values.
Results may differ from the reference program's by a relative error of at most 0.0125824.
Values sent between devices are 32-bit elements.
A program may use at most 1 GiB of HBM per device.

```python
import math
import jax
import jax.numpy as jnp
from jax import lax

BATCH_SIZE = 16
SHARD_LEN = 256
KV_GROUP = 4
CACHE_LEN = 1024
D_MODEL = 1024
Q_HEADS = 16
KV_HEADS = 8
HEAD_DIM = 64
NUM_EXPERTS = 32
TOP_K = 8
FF_DIM = 512
NUM_STEPS = 3
SEG_COUNT = 64

HALF_DIM = HEAD_DIM // 2
Q_GROUP = Q_HEADS // KV_HEADS
FF_SHARD = FF_DIM // KV_GROUP
ROPE_BASE = 10000.0
ROPE_MSCALE = math.sqrt(1.0 + math.log(32.0) / math.log(4096.0))
NORM_EPS = 1e-5
NEG_FILL = -1e30


def setup_inputs(seed: int = 0, part: int = 0) -> dict:
    base_key = jax.random.key(seed)
    shared_keys = jax.random.split(base_key, 17)
    part_keys = jax.random.split(jax.random.fold_in(base_key, part), 9)
    q_width = Q_HEADS * HEAD_DIM
    kv_width = KV_HEADS * HEAD_DIM
    d_scale = D_MODEL ** -0.5

    def normal(rand_key, arr_dims, factor):
        return jax.random.normal(rand_key, arr_dims, jnp.float32) * factor

    x_first = normal(part_keys[0], (BATCH_SIZE, D_MODEL), 1.0).astype(jnp.bfloat16)
    next_emb = normal(part_keys[1], (NUM_STEPS - 1, BATCH_SIZE, D_MODEL), 1.0).astype(jnp.bfloat16)
    seg_index = (jnp.arange(CACHE_LEN) * SEG_COUNT) // CACHE_LEN
    key_segs = normal(part_keys[2], (BATCH_SIZE, SEG_COUNT, KV_HEADS, HEAD_DIM), 1.0)
    value_segs = normal(part_keys[3], (BATCH_SIZE, SEG_COUNT, KV_HEADS, HEAD_DIM), 4.0)
    cache_dims = (BATCH_SIZE, CACHE_LEN, KV_HEADS, HEAD_DIM)
    k_cache = (normal(part_keys[4], cache_dims, 1.0) + key_segs[:, seg_index]).astype(jnp.bfloat16)
    v_cache = (normal(part_keys[5], cache_dims, 1.0) + value_segs[:, seg_index]).astype(jnp.bfloat16)
    drawn_lens = jax.random.randint(part_keys[6], (BATCH_SIZE,), CACHE_LEN // 4, CACHE_LEN + 1)
    seq_len = jnp.where(jnp.arange(BATCH_SIZE) == 0, CACHE_LEN, drawn_lens).astype(jnp.int32)
    rank_scores = jax.random.randint(part_keys[7], (NUM_STEPS, BATCH_SIZE, NUM_EXPERTS), 0, 1 << 20)
    expert_order = jnp.argsort(rank_scores * NUM_EXPERTS + jnp.arange(NUM_EXPERTS), axis=-1)
    expert_idx = expert_order[..., :TOP_K].astype(jnp.int32)
    chosen = (expert_idx[..., None] == jnp.arange(NUM_EXPERTS)).astype(jnp.int32)
    earlier = jnp.cumsum(chosen, axis=2) - chosen
    coin_flip = jax.random.randint(part_keys[8], (NUM_STEPS, BATCH_SIZE, TOP_K, NUM_EXPERTS), 0, 2)
    route_mask = jnp.where(chosen == 1, 1, jnp.where(earlier > 0, 0, coin_flip)).astype(jnp.int32)
    return {
        'x_first': x_first,
        'next_emb': next_emb,
        'k_cache': k_cache,
        'v_cache': v_cache,
        'seq_len': seq_len,
        'ln1_gain': 1.0 + normal(shared_keys[0], (D_MODEL,), 0.3),
        'ln1_bias': normal(shared_keys[1], (D_MODEL,), 0.3),
        'w_q': normal(shared_keys[2], (D_MODEL, q_width), d_scale).astype(jnp.bfloat16),
        'b_q': normal(shared_keys[3], (q_width,), 0.5),
        'w_k': normal(shared_keys[4], (D_MODEL, kv_width), d_scale).astype(jnp.bfloat16),
        'b_k': normal(shared_keys[5], (kv_width,), 0.5),
        'w_v': normal(shared_keys[6], (D_MODEL, kv_width), d_scale).astype(jnp.bfloat16),
        'b_v': normal(shared_keys[7], (kv_width,), 0.5),
        'w_o': normal(shared_keys[8], (q_width, D_MODEL), q_width ** -0.5).astype(jnp.bfloat16),
        'b_o': normal(shared_keys[9], (D_MODEL,), 0.3),
        'ln2_gain': 1.0 + normal(shared_keys[10], (D_MODEL,), 0.3),
        'ln2_bias': normal(shared_keys[11], (D_MODEL,), 0.3),
        'w_router': normal(shared_keys[12], (D_MODEL, NUM_EXPERTS), 1.5 * d_scale).astype(jnp.bfloat16),
        'w_gate': normal(shared_keys[13], (NUM_EXPERTS, D_MODEL, FF_DIM), d_scale).astype(jnp.bfloat16),
        'w_up': normal(shared_keys[14], (NUM_EXPERTS, D_MODEL, FF_DIM), d_scale).astype(jnp.bfloat16),
        'w_down': normal(shared_keys[15], (NUM_EXPERTS, FF_DIM, D_MODEL), FF_DIM ** -0.5).astype(jnp.bfloat16),
        'long_factor': jnp.exp(jax.random.uniform(shared_keys[16], (HALF_DIM,), jnp.float32, 0.0, 3.5)),
        'expert_idx': expert_idx,
        'route_mask': route_mask,
    }


def layer_norm(x_in, gain_vec, bias_vec):
    x_f32 = x_in.astype(jnp.float32)
    mean_val = jnp.mean(x_f32, axis=-1, keepdims=True)
    centered = x_f32 - mean_val
    var_val = jnp.mean(centered * centered, axis=-1, keepdims=True)
    return (centered * lax.rsqrt(var_val + NORM_EPS) * gain_vec + bias_vec).astype(jnp.bfloat16)


def rotate_heads(x_in, angles):
    cos_half = jnp.cos(angles) * ROPE_MSCALE
    sin_half = jnp.sin(angles) * ROPE_MSCALE
    cos_full = jnp.concatenate([cos_half, cos_half], axis=-1)[:, None, :]
    sin_full = jnp.concatenate([sin_half, sin_half], axis=-1)[:, None, :]
    x_f32 = x_in.astype(jnp.float32)
    rotated = jnp.concatenate([-x_f32[..., HALF_DIM:], x_f32[..., :HALF_DIM]], axis=-1)
    return (x_f32 * cos_full + rotated * sin_full).astype(jnp.bfloat16)


def partial_stats(q_grp, keys, values, keep_mask):
    scores = jnp.einsum('bkgd,btkd->bkgt', q_grp.astype(jnp.float32), keys.astype(jnp.float32)) * (HEAD_DIM ** -0.5)
    keep_full = keep_mask[:, None, None, :]
    scores = jnp.where(keep_full, scores, NEG_FILL)
    run_max = jnp.max(scores, axis=-1)
    weights = jnp.where(keep_full, jnp.exp(scores - run_max[..., None]), 0.0)
    run_sum = jnp.sum(weights, axis=-1)
    out_part = jnp.einsum('bkgt,btkd->bkgd', weights.astype(jnp.bfloat16).astype(jnp.float32), values.astype(jnp.float32))
    return run_max, run_sum, out_part


def reference(x_first, next_emb, k_cache, v_cache, seq_len, ln1_gain, ln1_bias, w_q, b_q, w_k, b_k, w_v, b_v, w_o, b_o, ln2_gain, ln2_bias, w_router, w_gate, w_up, w_down, long_factor, expert_idx, route_mask):
    inv_freq = 1.0 / (long_factor * ROPE_BASE ** (jnp.arange(HALF_DIM, dtype=jnp.float32) * 2.0 / HEAD_DIM))
    step_inputs = jnp.concatenate([x_first[None], next_emb], axis=0)
    shard_ids = jnp.arange(KV_GROUP)
    tail_slots = jnp.arange(NUM_STEPS)

    def decode_step(step_carry, step_in):
        tail_k, tail_v = step_carry
        x_in, idx_step, mask_step, step_idx = step_in
        h_norm = layer_norm(x_in, ln1_gain, ln1_bias)
        q_new = (jnp.dot(h_norm, w_q, preferred_element_type=jnp.float32) + b_q).astype(jnp.bfloat16).reshape(BATCH_SIZE, Q_HEADS, HEAD_DIM)
        k_new = (jnp.dot(h_norm, w_k, preferred_element_type=jnp.float32) + b_k).astype(jnp.bfloat16).reshape(BATCH_SIZE, KV_HEADS, HEAD_DIM)
        v_new = (jnp.dot(h_norm, w_v, preferred_element_type=jnp.float32) + b_v).astype(jnp.bfloat16).reshape(BATCH_SIZE, KV_HEADS, HEAD_DIM)
        angles = (seq_len + step_idx).astype(jnp.float32)[:, None] * inv_freq[None, :]
        q_grp = rotate_heads(q_new, angles).reshape(BATCH_SIZE, KV_HEADS, Q_GROUP, HEAD_DIM)
        k_rot = rotate_heads(k_new, angles)
        tail_k = lax.dynamic_update_slice_in_dim(tail_k, k_rot[:, None], step_idx, axis=1)
        tail_v = lax.dynamic_update_slice_in_dim(tail_v, v_new[:, None], step_idx, axis=1)

        def one_shard(shard_id):
            k_blk = lax.dynamic_slice_in_dim(k_cache, shard_id * SHARD_LEN, SHARD_LEN, axis=1)
            v_blk = lax.dynamic_slice_in_dim(v_cache, shard_id * SHARD_LEN, SHARD_LEN, axis=1)
            positions = shard_id * SHARD_LEN + jnp.arange(SHARD_LEN)
            keep_mask = positions[None, :] < seq_len[:, None]
            return partial_stats(q_grp, k_blk, v_blk, keep_mask)

        cache_max, cache_sum, cache_out = lax.map(one_shard, shard_ids)
        tail_keep = jnp.broadcast_to(tail_slots[None, :] <= step_idx, (BATCH_SIZE, NUM_STEPS))
        tail_max, tail_sum, tail_out = partial_stats(q_grp, tail_k, tail_v, tail_keep)
        max_all = jnp.concatenate([cache_max, tail_max[None]], axis=0)
        sum_all = jnp.concatenate([cache_sum, tail_sum[None]], axis=0)
        out_all = jnp.concatenate([cache_out, tail_out[None]], axis=0)
        top_max = jnp.max(max_all, axis=0, keepdims=True)
        factor = jnp.exp(max_all - top_max)
        total_sum = jnp.sum(sum_all * factor, axis=0)
        merged = jnp.sum(out_all * factor[..., None], axis=0) / total_sum[..., None]
        attn_out = merged.reshape(BATCH_SIZE, Q_HEADS * HEAD_DIM).astype(jnp.bfloat16)
        x_mid = (x_in.astype(jnp.float32) + jnp.dot(attn_out, w_o, preferred_element_type=jnp.float32) + b_o).astype(jnp.bfloat16)
        h_moe = layer_norm(x_mid, ln2_gain, ln2_bias)
        logits = jnp.dot(h_moe, w_router, preferred_element_type=jnp.float32)
        masked = jnp.where(mask_step == 1, logits[:, None, :], NEG_FILL)
        gate_probs = jax.nn.softmax(masked, axis=-1)
        chosen = idx_step[..., None] == jnp.arange(NUM_EXPERTS)[None, None, :]
        gate_mat = jnp.sum(jnp.where(chosen, gate_probs, 0.0), axis=1)

        def expert_body(part_acc, expert_in):
            gate_w, up_w, down_w, gate_col = expert_in
            act_gate = jnp.dot(h_moe, gate_w, preferred_element_type=jnp.float32)
            act_up = jnp.dot(h_moe, up_w, preferred_element_type=jnp.float32)
            mixed_act = (gate_col[:, None] * jax.nn.silu(act_gate) * act_up).astype(jnp.bfloat16)
            blocks = mixed_act.reshape(BATCH_SIZE, KV_GROUP, FF_SHARD).astype(jnp.float32)
            down_blocks = down_w.reshape(KV_GROUP, FF_SHARD, D_MODEL).astype(jnp.float32)
            return part_acc + jnp.einsum('bjf,jfd->bjd', blocks, down_blocks), None

        part_init = jnp.zeros((BATCH_SIZE, KV_GROUP, D_MODEL), jnp.float32)
        part_acc = lax.scan(expert_body, part_init, (w_gate, w_up, w_down, gate_mat.T))[0]
        moe_out = jnp.sum(part_acc.astype(jnp.bfloat16).astype(jnp.float32), axis=1)
        x_out = (x_mid.astype(jnp.float32) + moe_out).astype(jnp.bfloat16)
        return (tail_k, tail_v), x_out

    tail_init = jnp.zeros((BATCH_SIZE, NUM_STEPS, KV_HEADS, HEAD_DIM), jnp.bfloat16)
    final_carry, hidden = lax.scan(decode_step, (tail_init, tail_init), (step_inputs, expert_idx, route_mask, jnp.arange(NUM_STEPS)))
    return hidden, final_carry[0], final_carry[1]
```

```python
import functools
import math

import jax
import jax.numpy as jnp
import numpy as np
from jax import lax
from jax.experimental import pallas as pl
from jax.experimental.pallas import tpu as pltpu
from jax.sharding import PartitionSpec as P

ROPE_BASE = 10000.0
ROPE_MSCALE = math.sqrt(1.0 + math.log(32.0) / math.log(4096.0))
NORM_EPS = 1e-5
NEG_FILL = -1e30
F32 = jnp.float32
BF16 = jnp.bfloat16

S = 3
B = 16
D = 1024
T = 256
KV = 8
HD = 64
E = 32
FS = 128
R = S * B
NCH = 2
CW = D // NCH
HW = CW // 2

NSMALL = 16
L_SMALL = 0
L_WQ = L_SMALL + NSMALL
L_K = L_WQ + 4
L_V = L_K + 4
L_WKV = L_V + 4
L_WO = L_WKV + 4
L_GU = L_WO + 16
L_DN = L_GU + 16
L_OUT = L_DN + 8
NLOCAL = L_OUT + 4

R_ML = 0
R_O = 3
R_C = 5
R_G = 7
R_A = 9
R_B = R_A + NCH
R_Y = R_B + NCH
NREMOTE = R_Y + NCH


def mm(a, b):
    return jnp.dot(a, b, preferred_element_type=F32)


def mm_t(a, b):
    return lax.dot_general(a, b, (((1,), (1,)), ((), ())), preferred_element_type=F32)


def norm_rows(x, gain, bias):
    mean = jnp.mean(x, axis=-1, keepdims=True)
    cen = x - mean
    var = jnp.mean(cen * cen, axis=-1, keepdims=True)
    return (cen * lax.rsqrt(var + NORM_EPS) * gain + bias).astype(BF16)


def lane_iota(shape):
    return lax.broadcasted_iota(jnp.int32, shape, len(shape) - 1)


def kernel(
    x_first, next_emb, k_hbm, v_hbm, seq_hbm, g1_h, b1_h, wq_h, bq_h, wk_h, bk_h, wv_h, bv_h, wo_h, bo_h, g2_h, b2_h,
    wr_h, wg_h, wu_h, wd_h, lf_h, idx_h, rm_h, base_h,
    hid_out, tk_out, tv_out,
    xb, g1, b1, wq, bq, wk, bk, wv, bv, wo, bo, g2, b2, wr, wg, wu, wd, lf, idx, rm, base, seq_s, kc, vc,
    qbuf, kbuf, vbuf, sbuf, wbuf, mlb, mlall, obuf, orecv, c2, ex, ga, gb, tl, oall, xm4, gx, ub, pb, ab, s2, yb, hb, tkb, tvb,
    lsem, ssem, rsem,
):
    me = lax.axis_index("kv")
    core = me % 2
    chip = me // 2
    partner = me + 1 - 2 * core
    peer = (me + 2) % 4
    diag = (partner + 2) % 4

    def local(src, dst, i):
        return pltpu.make_async_copy(src, dst, lsem.at[i])

    def remote(src, dst, i, dev):
        return pltpu.make_async_remote_copy(
            src_ref=src, dst_ref=dst, send_sem=ssem.at[i], recv_sem=rsem.at[i],
            device_id={"kv": dev}, device_id_type=pl.DeviceIdType.MESH)

    first = [
        local(x_first, xb.at[0], 0), local(next_emb, xb.at[pl.ds(1, 2)], 1), local(g1_h, g1, 2), local(b1_h, b1, 3),
        local(bq_h, bq, 4), local(lf_h, lf, 5), local(base_h, base, 6), local(seq_hbm, seq_s, 7),
    ]
    later = [
        local(bk_h, bk, 8), local(bv_h, bv, 9), local(bo_h, bo, 10), local(g2_h, g2, 11), local(b2_h, b2, 12),
        local(wr_h, wr, 13), local(idx_h, idx, 14), local(rm_h, rm, 15),
    ]
    cp_wq = [local(wq_h.at[pl.ds(i * 256, 256)], wq.at[pl.ds(i * 256, 256)], L_WQ + i) for i in range(4)]
    cp_k = [local(k_hbm.at[pl.ds(i * 4, 4)], kc.at[pl.ds(i * 4, 4)], L_K + i) for i in range(4)]

    def v_part(i):
        half = (1 - core) if i < 2 else core
        sl = (pl.ds(half * 8, 8), pl.ds((i % 2) * 4, 4))
        return local(v_hbm.at[sl], vc.at[sl], L_V + i)

    cp_v = [v_part(i) for i in range(4)]
    cp_wkv = []
    for n, (h, v) in enumerate(((wk_h, wk), (wv_h, wv))):
        for i in range(2):
            cp_wkv.append(local(h.at[pl.ds(i * 512, 512)], v.at[pl.ds(i * 512, 512)], L_WKV + 2 * n + i))
    cp_wo = [
        local(wo_h.at[pl.ds(kv * 128 + g * 64, 64)], wo.at[g, pl.ds(kv * 64, 64)], L_WO + 2 * kv + g)
        for kv in range(KV) for g in range(2)
    ]

    def gu_copies(i):
        sl = pl.ds(i * 4, 4)
        return local(wg_h.at[sl], wg.at[sl], L_GU + 2 * i), local(wu_h.at[sl], wu.at[sl], L_GU + 2 * i + 1)

    def dn_copy(i):
        sl = pl.ds(i * 4, 4)
        return local(wd_h.at[sl], wd.at[sl], L_DN + i)

    for c in first + cp_wq + cp_k:
        c.start()
    bar = pltpu.get_barrier_semaphore()
    for dev in (partner, peer, diag):
        pl.semaphore_signal(bar, inc=1, device_id={"kv": dev}, device_id_type=pl.DeviceIdType.MESH)
    for c in cp_v + later + cp_wkv + cp_wo:
        c.start()
    for i in range(8):
        for c in gu_copies(i):
            c.start()
    for i in range(8):
        dn_copy(i).start()

    qbuf[:, 6:8, :] = jnp.zeros((B, 2, 512), F32)

    for c in first:
        c.wait()

    lane48 = lane_iota((R, 128))
    inv = 1.0 / (jnp.concatenate([lf[...]] * 4, axis=1) * base[...])
    row_b = lax.broadcasted_iota(jnp.int32, (B, 128), 0)
    len_rows = jnp.zeros((B, 128), jnp.int32)
    for b in range(B):
        len_rows = jnp.where(row_b == b, seq_s[b], len_rows)
    angles = jnp.concatenate([(len_rows + s).astype(F32) for s in range(S)], axis=0) * inv
    cosv = jnp.cos(angles) * ROPE_MSCALE
    sinv = jnp.sin(angles) * ROPE_MSCALE
    low_half = (lane48 % HD) < (HD // 2)

    def rope(x):
        xf = x.astype(BF16).astype(F32)
        rot = jnp.where(low_half, -pltpu.roll(xf, 96, 1), pltpu.roll(xf, 32, 1))
        return (xf * cosv + rot * sinv).astype(BF16).astype(F32)

    h1 = norm_rows(xb[...].reshape(R, D).astype(F32), g1[...], b1[...])

    for c in cp_wq:
        c.wait()
    q = mm(h1, wq[...]) + bq[...]
    left = lane48 < HD
    for p in range(4):
        qa = rope(q[:, p * 256:p * 256 + 128]) * 0.125
        qb_ = rope(q[:, p * 256 + 128:p * 256 + 256]) * 0.125
        pair = (jnp.where(left, qa, pltpu.roll(qb_, 64, 1)), jnp.where(left, pltpu.roll(qa, 64, 1), qb_))
        for g in range(2):
            for s in range(S):
                qbuf[:, 2 * s + g, p * 128:(p + 1) * 128] = pair[g][s * B:(s + 1) * B]

    rowq = lax.broadcasted_iota(jnp.int32, (32, T), 0)
    laneq = lane_iota((32, T))
    diag_mask = (rowq // 8) == (laneq // HD)
    pos = laneq + me * T
    lane8 = lane_iota((8, 128))

    def scores(b):
        qv = qbuf[b]
        for hh in range(2):
            rep = jnp.concatenate([qv[:, hh * 256:(hh + 1) * 256]] * 4, axis=0)
            lhs = jnp.where(diag_mask, rep, 0.0).astype(BF16)
            sbuf[b, hh] = mm(lhs, kc[b, hh * 4:(hh + 1) * 4].reshape(256, T))

    def soft(b, acc):
        keep = pos < seq_s[b]
        for hh in range(2):
            sc = jnp.where(keep, sbuf[b, hh], NEG_FILL)
            m = jnp.max(sc, axis=1, keepdims=True)
            w = jnp.where(keep, jnp.exp(sc - m), 0.0)
            l = jnp.sum(w, axis=1, keepdims=True)
            wbuf[b, hh] = w.astype(BF16)
            for j in range(4):
                at = (b % 8) * 16 + hh * 4 + j
                acc = jnp.where(lane8 == at, m[j * 8:(j + 1) * 8], acc)
                acc = jnp.where(lane8 == at + 8, l[j * 8:(j + 1) * 8], acc)
        return acc

    acc = [jnp.zeros((8, 128), F32)] * 2
    for c in range(5):
        if c < 4:
            cp_k[c].wait()
            for b in range(c * 4, c * 4 + 4):
                scores(b)
        if c > 0:
            for b in range(c * 4 - 4, c * 4):
                acc[b // 8] = soft(b, acc[b // 8])
    mlb[0] = acc[0]
    mlb[1] = acc[1]
    mlall[me] = mlb[core]

    pl.semaphore_wait(bar, 3)
    send_ml = [
        remote(mlb.at[1 - core], mlall.at[me], R_ML, partner), remote(mlb.at[core], mlall.at[me], R_ML + 1, peer),
        remote(mlb.at[1 - core], mlall.at[me], R_ML + 2, diag),
    ]
    for c in send_ml:
        c.start()

    left8 = lane8 < HD

    def values(half, i, hh):
        b = half * 8 + i
        pv = mm_t(wbuf[b, hh], vc[b, hh * 4:(hh + 1) * 4].reshape(256, T))
        obuf[half, hh, i, :, 0:128] = jnp.where(left8, pv[0:8, 0:128], pv[8:16, 0:128])
        obuf[half, hh, i, :, 128:256] = jnp.where(left8, pv[16:24, 128:256], pv[24:32, 128:256])

    send_o = [remote(obuf.at[1 - core, hh], orecv.at[hh], R_O + hh, partner) for hh in range(2)]
    for hh in range(2):
        cp_v[hh].wait()
        for i in range(8):
            values(1 - core, i, hh)
        send_o[hh].start()
    for hh in range(2):
        cp_v[2 + hh].wait()
        for i in range(8):
            values(core, i, hh)

    send_ml[0].wait()
    ml_a = mlall[me]
    ml_b = mlall[partner]
    m_ab = jnp.maximum(ml_a, ml_b)
    f_a = jnp.exp(ml_a - m_ab)
    f_b = jnp.exp(ml_b - m_ab)
    pick = (lane8 // HD)

    def spread(v, i, p):
        return jnp.take_along_axis(v, pick + (i * 16 + 2 * p), axis=1, mode="promise_in_bounds")

    send_c = [remote(c2.at[hh, chip, pl.ds(0, 6)], c2.at[hh, chip, pl.ds(0, 6)], R_C + hh, peer) for hh in range(2)]
    for hh in range(2):
        send_o[hh].wait()
        for i in range(8):
            oa = obuf[core, hh, i]
            ob = orecv[hh, i]
            for p in range(2):
                ln = slice(p * 128, (p + 1) * 128)
                c2[hh, chip, :, i, ln] = (
                    oa[:, ln] * spread(f_a, i, 2 * hh + p) + ob[:, ln] * spread(f_b, i, 2 * hh + p))
        send_c[hh].start()

    for c in later + cp_wkv:
        c.wait()
    kn = mm(h1, wk[...]) + bk[...]
    vn = (mm(h1, wv[...]) + bv[...]).astype(BF16)
    for p in range(4):
        ln = slice(p * 128, (p + 1) * 128)
        kr = rope(kn[:, ln])
        for s in range(S):
            kbuf[s, :, ln] = kr[s * B:(s + 1) * B]
    for s in range(S):
        vbuf[s] = vn[s * B:(s + 1) * B].astype(F32)
        tkb[s] = kbuf[s].astype(BF16)
        tvb[s] = vn[s * B:(s + 1) * B]
    cp_tail = [local(tkb, tk_out, L_OUT), local(tvb, tv_out, L_OUT + 1)]
    for c in cp_tail:
        c.start()

    rows = pl.ds(pl.multiple_of(core * 8, 8), 8)
    kt = [kbuf[t, rows, :] for t in range(S)]
    vt = [vbuf[t, rows, :] for t in range(S)]
    trip = [(s, g, t) for s in range(S) for g in range(2) for t in range(s + 1)]
    prod = jnp.concatenate([qbuf[rows, 2 * s + g, :] * kt[t] for s, g, t in trip], axis=0)
    hi = prod.astype(BF16)
    lo = (prod - hi.astype(F32)).astype(BF16)
    r2 = lax.broadcasted_iota(jnp.int32, (256, 128), 0)
    ones = jnp.where(((r2 % 128) // HD) == (lane_iota((256, 128)) // HD), 1.0, 0.0).astype(BF16)
    tsc = jnp.concatenate(
        [mm(jnp.concatenate([hi[:, p * 128:(p + 1) * 128], lo[:, p * 128:(p + 1) * 128]], axis=1), ones) for p in range(4)], axis=1)

    for c in send_ml[1:]:
        c.wait()
    ml = [mlall[d] for d in range(4)]
    for ch in range(2):
        a, b_ = ml[2 * ch], ml[2 * ch + 1]
        mc = jnp.maximum(a, b_)
        lc = (pltpu.roll(a, 120, 1) * jnp.exp(a - mc) + pltpu.roll(b_, 120, 1) * jnp.exp(b_ - mc))
        for i in range(8):
            for p in range(4):
                ln = slice(p * 128, (p + 1) * 128)
                ex[2 * ch, :, i, ln] = spread(mc, i, p)
                ex[2 * ch + 1, :, i, ln] = spread(lc, i, p)

    for s in range(S):
        for g in range(2):
            j = 2 * s + g
            sc = [tsc[n * 8:(n + 1) * 8] for n, key in enumerate(trip) if key[:2] == (s, g)]
            mt = functools.reduce(jnp.maximum, sc)
            wt = [jnp.exp(v - mt) for v in sc]
            lt = functools.reduce(jnp.add, wt)
            ot = functools.reduce(jnp.add, [w.astype(BF16).astype(F32) * v for w, v in zip(wt, vt)])
            m0, l0, m1, l1 = ex[0, j], ex[1, j], ex[2, j], ex[3, j]
            top = jnp.maximum(jnp.maximum(m0, m1), mt)
            f0, f1, ft = jnp.exp(m0 - top), jnp.exp(m1 - top), jnp.exp(mt - top)
            inv_l = 1.0 / (l0 * f0 + l1 * f1 + lt * ft)
            ga[j] = f0 * inv_l
            gb[j] = f1 * inv_l
            tl[j] = ot * (ft * inv_l)

    send_g = [remote(oall.at[core, hh], oall.at[core, hh], R_G + hh, partner) for hh in range(2)]
    for hh in range(2):
        send_c[hh].wait()
        ln = slice(hh * 256, (hh + 1) * 256)
        for j in range(6):
            oall[core, hh, j] = c2[hh, 0, j] * ga[j][:, ln] + c2[hh, 1, j] * gb[j][:, ln] + tl[j][:, ln]
        send_g[hh].start()

    for c in cp_wo:
        c.wait()
    for c in send_g:
        c.wait()
    att = None
    for g in range(2):
        o_g = jnp.concatenate([
            jnp.concatenate([jnp.concatenate([oall[h, hh, 2 * s + g] for hh in range(2)], axis=1) for h in range(2)], axis=0)
            for s in range(S)], axis=0).astype(BF16)
        part = mm(o_g, wo[g])
        att = part if att is None else att + part
    xm = (xb[...].reshape(R, D).astype(F32) + att + bo[...]).astype(BF16).astype(F32)
    for n in range(NCH):
        for h in range(2):
            xm4[n, h] = xm[:, n * CW + h * HW:n * CW + (h + 1) * HW]
    h2 = norm_rows(xm, g2[...], b2[...])

    logits = mm_t(h2, wr[...])
    eye = jnp.where(lax.broadcasted_iota(jnp.int32, (B, B), 0) == lane_iota((B, B)), 1.0, 0.0)
    picks = jnp.concatenate([mm_t(eye, idx[s].astype(F32)) for s in range(S)], axis=0)
    lane_e = lane_iota((R, E)).astype(F32)
    gates = jnp.zeros((R, E), F32)
    for k in range(8):
        on = jnp.concatenate([rm[s, :, k, :] for s in range(S)], axis=0) == 1
        mk = jnp.where(on, logits, NEG_FILL)
        pk = jnp.exp(mk - jnp.max(mk, axis=1, keepdims=True))
        pk = pk / jnp.sum(pk, axis=1, keepdims=True)
        gates = gates + jnp.where(picks[:, k:k + 1] == lane_e, pk, 0.0)
    for e in range(E):
        gx[e] = jnp.broadcast_to(gates[:, e:e + 1], (R, 128))

    def gu_body(i, carry):
        for c in gu_copies(i):
            c.wait()
        for n in range(4):
            e = i * 4 + n
            both = mm(h2, jnp.concatenate([wg[e], wu[e]], axis=1))
            a, up = both[:, :FS], both[:, FS:]
            ub[e] = (gx[e] * (a * (1.0 / (1.0 + jnp.exp(-a)))) * up).astype(BF16)
        return carry

    lax.fori_loop(0, 8, gu_body, 0)

    for i in range(8):
        dn_copy(i).wait()
    u = jnp.concatenate([ub[e] for e in range(E)], axis=1)
    send_a = [remote(pb.at[n, 1 - core], ab.at[n], R_A + n, partner) for n in range(NCH)]
    send_b = [remote(s2.at[n, chip], s2.at[n, chip], R_B + n, peer) for n in range(NCH)]
    send_y = [remote(yb.at[n, core], yb.at[n, core], R_Y + n, partner) for n in range(NCH)]
    for n in range(NCH):
        part = mm(u, wd[:, :, n * CW:(n + 1) * CW].reshape(E * FS, CW)).astype(BF16).astype(F32)
        pb[n, 0] = part[:, :HW]
        pb[n, 1] = part[:, HW:]
        send_a[n].start()
    for n in range(NCH):
        send_a[n].wait()
        s2[n, chip] = pb[n, core] + ab[n]
        send_b[n].start()
    for n in range(NCH):
        send_b[n].wait()
        yb[n, core] = xm4[n, core] + (s2[n, 0] + s2[n, 1])
        send_y[n].start()
    for n in range(NCH):
        send_y[n].wait()
        for h in range(2):
            hb[:, :, n * CW + h * HW:n * CW + (h + 1) * HW] = yb[n, h].astype(BF16).reshape(S, B, HW)
    cp_h = local(hb, hid_out, L_OUT + 2)
    cp_h.start()
    for c in cp_tail:
        c.wait()
    cp_h.wait()


def solution(mesh):
    def layer_steps(x_first, next_emb, k_cache, v_cache, seq_len, ln1_gain, ln1_bias, w_q, b_q, w_k, b_k, w_v, b_v, w_o, b_o, ln2_gain, ln2_bias, w_router, w_gate, w_up, w_down, long_factor, expert_idx, route_mask):
        def row(v):
            return v.reshape(1, -1)

        powers = (np.float32(ROPE_BASE) ** (np.arange(32, dtype=np.float32) * np.float32(2.0) / np.float32(HD))).astype(np.float32)
        base = jnp.asarray(np.tile(powers, 4)[None, :])
        args = (
            x_first, next_emb, jnp.transpose(k_cache, (0, 2, 3, 1)), jnp.transpose(v_cache, (0, 2, 3, 1)), seq_len,
            row(ln1_gain), row(ln1_bias), w_q, row(b_q), w_k, row(b_k), w_v, row(b_v), w_o, row(b_o), row(ln2_gain), row(ln2_bias),
            jnp.transpose(w_router), w_gate, w_up, w_down, row(long_factor), jnp.transpose(expert_idx, (0, 2, 1)), route_mask, base,
        )
        V = pltpu.VMEM
        scratch = [
            V((S, B, D), BF16), V((1, D), F32), V((1, D), F32), V((D, D), BF16), V((1, D), F32), V((D, 512), BF16), V((1, 512), F32),
            V((D, 512), BF16), V((1, 512), F32), V((2, 512, D), BF16), V((1, D), F32), V((1, D), F32), V((1, D), F32), V((E, D), BF16),
            V((E, D, FS), BF16), V((E, D, FS), BF16), V((E, FS, D), BF16), V((1, 32), F32), V((S, 8, B), jnp.int32),
            V((S, B, 8, E), jnp.int32), V((1, 128), F32), pltpu.SMEM((B,), jnp.int32), V((B, KV, HD, T), BF16), V((B, KV, HD, T), BF16),
            V((B, 8, 512), F32), V((S, B, 512), F32), V((S, B, 512), F32), V((B, 2, 32, T), F32), V((B, 2, 32, T), BF16),
            V((2, 8, 128), F32), V((4, 8, 128), F32), V((2, 2, 8, 8, 256), F32), V((2, 8, 8, 256), F32), V((2, 2, 8, 8, 256), F32),
            V((4, 8, 8, 512), F32), V((6, 8, 512), F32), V((6, 8, 512), F32), V((6, 8, 512), F32), V((2, 2, 6, 8, 256), F32),
            V((NCH, 2, R, HW), F32), V((E, R, 128), F32), V((E, R, FS), BF16), V((NCH, 2, R, HW), F32), V((NCH, R, HW), F32),
            V((NCH, 2, R, HW), F32), V((NCH, 2, R, HW), F32), V((S, B, D), BF16), V((S, B, 512), BF16), V((S, B, 512), BF16),
            pltpu.SemaphoreType.DMA((NLOCAL,)), pltpu.SemaphoreType.DMA((NREMOTE,)), pltpu.SemaphoreType.DMA((NREMOTE,)),
        ]
        anyspec = pl.BlockSpec(memory_space=pl.ANY)
        hid, tk, tv = pl.pallas_call(
            kernel,
            out_shape=(
                jax.ShapeDtypeStruct((S, B, D), BF16), jax.ShapeDtypeStruct((S, B, 512), BF16), jax.ShapeDtypeStruct((S, B, 512), BF16)),
            in_specs=[anyspec] * len(args),
            out_specs=(anyspec,) * 3,
            scratch_shapes=scratch,
            compiler_params=pltpu.CompilerParams(collective_id=0, has_side_effects=True, vmem_limit_bytes=60 * 1024 * 1024),
        )(*args)

        def tail(v):
            return jnp.transpose(v.reshape(S, B, KV, HD), (1, 0, 2, 3))

        return hid, tail(tk), tail(tv)

    replicated = P()
    in_specs = (P('dp'), P(None, 'dp'), P('dp', 'kv'), P('dp', 'kv'), P('dp')) + (replicated,) * 13 + (P(None, None, 'kv'), P(None, None, 'kv'), P(None, 'kv'), replicated, P(None, 'dp'), P(None, 'dp'))
    out_specs = (P(None, 'dp'), P('dp'), P('dp'))
    return jax.shard_map(layer_steps, mesh=mesh, in_specs=in_specs, out_specs=out_specs, check_vma=False)
```

```python
import functools
import itertools
import math

import jax
import jax.numpy as jnp
import numpy as np
from jax import lax
from jax.experimental import pallas as pl
from jax.experimental.pallas import tpu as pltpu
from jax.sharding import PartitionSpec as P

ROPE_BASE = 10000.0
ROPE_MSCALE = math.sqrt(1.0 + math.log(32.0) / math.log(4096.0))
NORM_EPS = 1e-5
NEG_FILL = -1e30
F32 = jnp.float32
BF16 = jnp.bfloat16

S = 3
B = 16
D = 1024
T = 256
KV = 8
HD = 64
E = 32
FS = 128
R = S * B
NCH = 4
CW = D // NCH
HW = CW // 2

SMALL, PARTS, GROUPS = 16, 4, 8
L_SMALL, L_WQ, L_K, L_V, L_WKV, L_WO, L_GU, L_DN, NLOCAL = itertools.accumulate(
    (SMALL, PARTS, PARTS, PARTS, PARTS, 2 * KV, 2 * GROUPS, GROUPS), initial=0)
R_ML, R_O, R_C, R_G, R_A, R_B, R_Y, NREMOTE = itertools.accumulate((3, 2, 2, 2, NCH, NCH, NCH), initial=0)
LN = 128
HALF = 8


def at(i, width=LN):
    return slice(i * width, (i + 1) * width)


def mm(a, b):
    return jnp.dot(a, b, preferred_element_type=F32)


def mm_t(a, b):
    return lax.dot_general(a, b, (((1,), (1,)), ((), ())), preferred_element_type=F32)


def norm_rows(x, gain, bias):
    mean = jnp.mean(x, axis=-1, keepdims=True)
    cen = x - mean
    var = jnp.mean(cen * cen, axis=-1, keepdims=True)
    return (cen * lax.rsqrt(var + NORM_EPS) * gain + bias).astype(BF16)


def lane_iota(shape):
    return lax.broadcasted_iota(jnp.int32, shape, len(shape) - 1)


def kernel(
    x_first, next_emb, k_hbm, v_hbm, seq_hbm, g1_h, b1_h, wq_h, bq_h, wk_h, bk_h, wv_h, bv_h, wo_h, bo_h, g2_h, b2_h,
    wr_h, wg_h, wu_h, wd_h, lf_h, idx_h, rm_h, base_h,
    hb, tkb, tvb,
    xb, g1, b1, wq, bq, wk, bk, wv, bv, wo, bo, g2, b2, wr, wg, wu, wd, lf, idx, rm, base, seq_s, kc, vc,
    qbuf, kbuf, vbuf, sbuf, wbuf, mlb, mlall, obuf, orecv, c2, ex, ga, gb, tl, oall, xm4, gx, raw, qraw, dsum, ub, pb, ab, s2, yb, tkf, tvf,
    lsem, ssem, rsem,
):
    me = lax.axis_index("kv")
    core = me % 2
    chip = me // 2
    partner = me + 1 - 2 * core
    peer = (me + 2) % 4
    diag = (partner + 2) % 4

    def local(src, dst, i):
        return pltpu.make_async_copy(src, dst, lsem.at[i])

    def remote(src, dst, i, dev):
        return pltpu.make_async_remote_copy(
            src_ref=src, dst_ref=dst, send_sem=ssem.at[i], recv_sem=rsem.at[i],
            device_id={"kv": dev}, device_id_type=pl.DeviceIdType.MESH)

    small = [
        local(src, dst, i) for i, (src, dst) in enumerate((
            (x_first, xb.at[0]), (next_emb, xb.at[pl.ds(1, S - 1)]), (g1_h, g1), (b1_h, b1), (bq_h, bq), (lf_h, lf), (base_h, base),
            (seq_hbm, seq_s), (bk_h, bk), (bv_h, bv), (bo_h, bo), (g2_h, g2), (b2_h, b2), (wr_h, wr), (idx_h, idx), (rm_h, rm)))
    ]
    first, later = small[:HALF], small[HALF:]
    cp_wq = [local(wq_h.at[:, pl.ds(i * T, T)], wq.at[:, pl.ds(i * T, T)], L_WQ + i) for i in range(4)]
    other, own = (1 - core) * 8, core * 8

    def k_part(i):
        sl = pl.ds((other if i < 2 else own) + (i % 2) * 4, 4)
        return local(k_hbm.at[sl], kc.at[sl], L_K + i)

    def v_part(i):
        sl = (pl.ds(other if i < 2 else own, 8), pl.ds((i % 2) * 4, 4))
        return local(v_hbm.at[sl], vc.at[sl], L_V + i)

    cp_k = [k_part(i) for i in range(4)]
    cp_v = [v_part(i) for i in range(4)]
    cp_wkv = []
    for n, (h, v) in enumerate(((wk_h, wk), (wv_h, wv))):
        for i in range(2):
            cp_wkv.append(local(h.at[pl.ds(i * 512, 512)], v.at[pl.ds(i * 512, 512)], L_WKV + 2 * n + i))
    cp_wo = [
        local(wo_h.at[pl.ds(kv * 128 + g * 64, 64)], wo.at[g, pl.ds(kv * 64, 64)], L_WO + 2 * kv + g)
        for kv in range(KV) for g in range(2)
    ]

    def gu_copies(i):
        sl = pl.ds(i * 4, 4)
        return local(wg_h.at[sl], wg.at[sl], L_GU + 2 * i), local(wu_h.at[sl], wu.at[sl], L_GU + 2 * i + 1)

    def dn_copy(i):
        sl = pl.ds(i * 4, 4)
        return local(wd_h.at[sl], wd.at[sl], L_DN + i)

    for c in first + cp_wq + cp_k:
        c.start()
    bar = pltpu.get_barrier_semaphore()
    for dev in (partner, peer, diag):
        pl.semaphore_signal(bar, inc=1, device_id={"kv": dev}, device_id_type=pl.DeviceIdType.MESH)
    qbuf[:, 6:8, :] = jnp.zeros((B, 2, 512), F32)

    for c in first:
        c.wait()
    for c in cp_v:
        c.start()

    lane48 = lane_iota((R, 128))
    inv = 1.0 / (jnp.concatenate([lf[...]] * 4, axis=1) * base[...])
    row_b = lax.broadcasted_iota(jnp.int32, (B, 128), 0)
    len_rows = jnp.zeros((B, 128), jnp.int32)
    for b in range(B):
        len_rows = jnp.where(row_b == b, seq_s[b], len_rows)
    angles = jnp.concatenate([(len_rows + s).astype(F32) for s in range(S)], axis=0) * inv
    cosv = jnp.cos(angles) * ROPE_MSCALE
    sinv = jnp.sin(angles) * ROPE_MSCALE
    low_half = (lane48 % HD) < (HD // 2)

    def rope(x):
        xf = x.astype(BF16).astype(F32)
        rot = jnp.where(low_half, -pltpu.roll(xf, 96, 1), pltpu.roll(xf, 32, 1))
        return (xf * cosv + rot * sinv).astype(BF16).astype(F32)

    h1 = norm_rows(xb[...].reshape(R, D).astype(F32), g1[...], b1[...])

    left = lane48 < HD

    def put_q(q, p):
        qa = rope(q[:, :128]) * 0.125
        qb_ = rope(q[:, 128:]) * 0.125
        pair = (jnp.where(left, qa, pltpu.roll(qb_, 64, 1)), jnp.where(left, pltpu.roll(qa, 64, 1), qb_))
        for g in range(2):
            for s in range(S):
                qbuf[:, 2 * s + g, at(p)] = pair[g][at(s, B)]

    cp_wq[0].wait()
    cp_wq[1].wait()
    q_lo = mm(h1, wq[:, :512]) + bq[:, :512]
    qraw[...] = q_lo
    cp_wq[2].wait()
    cp_wq[3].wait()
    for c in later + cp_wo + cp_wkv:
        c.start()
    q_hi = mm(h1, wq[:, 512:]) + bq[:, 512:]
    for p in range(4):
        put_q(qraw[:, p * 256:(p + 1) * 256] if p < 2 else q_hi[:, (p - 2) * 256:(p - 1) * 256], p)

    rowq = lax.broadcasted_iota(jnp.int32, (32, T), 0)
    laneq = lane_iota((32, T))
    diag_mask = (rowq // 8) == (laneq // HD)
    pos = laneq + me * T
    lane8 = lane_iota((8, 128))

    def scores(start, i):
        qv = qbuf[start + i]
        for hh in range(2):
            rep = jnp.concatenate([qv[:, at(hh, T)]] * 4, axis=0)
            lhs = jnp.where(diag_mask, rep, 0.0).astype(BF16)
            sbuf[start + i, hh] = mm(lhs, kc[start + i, at(hh, 4)].reshape(256, T))

    def soft(start, i, acc):
        keep = pos < seq_s[start + i]
        for hh in range(2):
            sc = jnp.where(keep, sbuf[start + i, hh], NEG_FILL)
            m = jnp.max(sc, axis=1, keepdims=True)
            w = jnp.where(keep, jnp.exp(sc - m), 0.0)
            l = jnp.sum(w, axis=1, keepdims=True)
            wbuf[start + i, hh] = w.astype(BF16)
            for j in range(4):
                spot = i * 16 + hh * 4 + j
                acc = jnp.where(lane8 == spot, m[at(j, 8)], acc)
                acc = jnp.where(lane8 == spot + 8, l[at(j, 8)], acc)
        return acc

    left8 = lane8 < HD

    def values(half, i, hh):
        b = half * 8 + i
        pv = mm_t(wbuf[b, hh], vc[b, at(hh, 4)].reshape(256, T))
        obuf[half, hh, i, :, 0:128] = jnp.where(left8, pv[0:8, 0:128], pv[8:16, 0:128])
        obuf[half, hh, i, :, 128:256] = jnp.where(left8, pv[16:24, 128:256], pv[24:32, 128:256])

    send_ml = [
        remote(mlb.at[1 - core], mlall.at[me], R_ML, partner), remote(mlb.at[core], mlall.at[me], R_ML + 1, peer),
        remote(mlb.at[1 - core], mlall.at[me], R_ML + 2, diag),
    ]
    send_o = [remote(obuf.at[1 - core, hh], orecv.at[hh], R_O + hh, partner) for hh in range(2)]
    zero = jnp.zeros((8, 128), F32)

    cp_k[0].wait()
    for i in range(4):
        scores(other, i)
    cp_k[1].wait()
    for i in range(4):
        scores(other, 4 + i)
    acc = zero
    for i in range(4):
        acc = soft(other, i, acc)
    cp_k[2].wait()
    for i in range(8):
        for c in gu_copies(i):
            c.start()
    for i in range(4):
        scores(own, i)
    for i in range(4):
        acc = soft(other, 4 + i, acc)
    mlb[1 - core] = acc
    pl.semaphore_wait(bar, 3)
    send_ml[0].start()
    send_ml[2].start()

    cp_v[0].wait()
    cp_k[3].wait()
    for i in range(8):
        values(1 - core, i, 0)
    for i in range(4):
        scores(own, 4 + i)
    acc = zero
    for i in range(4):
        acc = soft(own, i, acc)
    send_o[0].start()
    cp_v[1].wait()
    for i in range(8):
        dn_copy(i).start()
    for i in range(8):
        values(1 - core, i, 1)
    for i in range(4):
        acc = soft(own, 4 + i, acc)
    mlb[core] = acc
    mlall[me] = acc
    send_o[1].start()
    send_ml[1].start()

    pick = (lane8 // HD)

    def spread(v, i, p):
        return jnp.take_along_axis(v, pick + (i * 16 + 2 * p), axis=1, mode="promise_in_bounds")

    send_c = [remote(c2.at[hh, chip, pl.ds(0, 6)], c2.at[hh, chip, pl.ds(0, 6)], R_C + hh, peer) for hh in range(2)]
    for hh in range(2):
        cp_v[2 + hh].wait()
        for i in range(8):
            values(core, i, hh)
        if hh == 0:
            send_ml[0].wait()
            ml_a = mlall[me]
            ml_b = mlall[partner]
            m_ab = jnp.maximum(ml_a, ml_b)
            f_a = jnp.exp(ml_a - m_ab)
            f_b = jnp.exp(ml_b - m_ab)
        send_o[hh].wait()
        for i in range(8):
            oa = obuf[core, hh, i]
            ob = orecv[hh, i]
            for p in range(2):
                ln = at(p)
                c2[hh, chip, :, i, ln] = (
                    oa[:, ln] * spread(f_a, i, 2 * hh + p) + ob[:, ln] * spread(f_b, i, 2 * hh + p))
        send_c[hh].start()

    for c in later + cp_wkv:
        c.wait()
    kn = mm(h1, wk[...]) + bk[...]
    vn = (mm(h1, wv[...]) + bv[...]).astype(BF16)
    vn = vn.astype(F32)
    for p in range(4):
        ln = at(p)
        for val, buf, fin in ((rope(kn[:, ln]), kbuf, tkf), (vn[:, ln], vbuf, tvf)):
            swap = pltpu.roll(val, 64, 1)
            for s in range(S):
                r = at(s, B)
                buf[s, :, ln] = val[r]
                fin[:, s, 2 * p, :] = val[r, :HD]
                fin[:, s, 2 * p + 1, :] = swap[r, :HD]
    tkb[...] = tkf[...].astype(BF16)
    tvb[...] = tvf[...].astype(BF16)

    rows = pl.ds(pl.multiple_of(core * 8, 8), 8)
    kt = [kbuf[t, rows, :] for t in range(S)]
    vt = [vbuf[t, rows, :] for t in range(S)]
    trip = [(s, g, t) for s in range(S) for g in range(2) for t in range(s + 1)]
    prod = jnp.concatenate([qbuf[rows, 2 * s + g, :] * kt[t] for s, g, t in trip], axis=0)
    hi = prod.astype(BF16)
    lo = (prod - hi.astype(F32)).astype(BF16)
    r2 = lax.broadcasted_iota(jnp.int32, (256, 128), 0)
    ones = jnp.where(((r2 % 128) // HD) == (lane_iota((256, 128)) // HD), 1.0, 0.0).astype(BF16)
    tsc = jnp.concatenate(
        [mm(jnp.concatenate([hi[:, at(p)], lo[:, at(p)]], axis=1), ones) for p in range(4)], axis=1)

    for c in send_ml[1:]:
        c.wait()
    ml = [mlall[d] for d in range(4)]
    for ch in range(2):
        a, b_ = ml[2 * ch], ml[2 * ch + 1]
        mc = jnp.maximum(a, b_)
        lc = (pltpu.roll(a, 120, 1) * jnp.exp(a - mc) + pltpu.roll(b_, 120, 1) * jnp.exp(b_ - mc))
        for i in range(8):
            for p in range(4):
                ln = at(p)
                ex[2 * ch, :, i, ln] = spread(mc, i, p)
                ex[2 * ch + 1, :, i, ln] = spread(lc, i, p)

    for s in range(S):
        for g in range(2):
            j = 2 * s + g
            sc = [tsc[at(n, 8)] for n, key in enumerate(trip) if key[:2] == (s, g)]
            mt = functools.reduce(jnp.maximum, sc)
            wt = [jnp.exp(v - mt) for v in sc]
            lt = functools.reduce(jnp.add, wt)
            ot = functools.reduce(jnp.add, [w.astype(BF16).astype(F32) * v for w, v in zip(wt, vt)])
            m0, l0, m1, l1 = ex[0, j], ex[1, j], ex[2, j], ex[3, j]
            top = jnp.maximum(jnp.maximum(m0, m1), mt)
            f0, f1, ft = jnp.exp(m0 - top), jnp.exp(m1 - top), jnp.exp(mt - top)
            inv_l = 1.0 / (l0 * f0 + l1 * f1 + lt * ft)
            ga[j] = f0 * inv_l
            gb[j] = f1 * inv_l
            tl[j] = ot * (ft * inv_l)

    send_g = [remote(oall.at[core, hh], oall.at[core, hh], R_G + hh, partner) for hh in range(2)]
    for hh in range(2):
        send_c[hh].wait()
        ln = at(hh, T)
        for j in range(6):
            oall[core, hh, j] = c2[hh, 0, j] * ga[j][:, ln] + c2[hh, 1, j] * gb[j][:, ln] + tl[j][:, ln]
        send_g[hh].start()

    for c in cp_wo:
        c.wait()
    att = None
    for hh in range(2):
        send_g[hh].wait()
        for g in range(2):
            o_g = jnp.concatenate([oall[h, hh, 2 * s + g] for s in range(S) for h in range(2)], axis=0).astype(BF16)
            part = mm(o_g, wo[g, at(hh, T)])
            att = part if att is None else att + part
    xm = (xb[...].reshape(R, D).astype(F32) + att + bo[...]).astype(BF16).astype(F32)
    for n in range(NCH):
        for h in range(2):
            xm4[n, h] = xm[:, at(2 * n + h, HW)]
    h2 = norm_rows(xm, g2[...], b2[...])

    def act(i):
        for n in range(4):
            e = i * 4 + n
            raw[e] = mm(h2, jnp.concatenate([wg[e], wu[e]], axis=1))

    def mix(i):
        for n in range(4):
            e = i * 4 + n
            a, up = raw[e, :, :FS], raw[e, :, FS:]
            ub[e] = (gx[e] * (a * (1.0 / (1.0 + jnp.exp(-a)))) * up).astype(BF16)

    for i in range(8):
        for c in gu_copies(i):
            c.wait()
        dn_copy(i).wait()
    logits = mm_t(h2, wr[...])
    act(0)
    act(1)
    eye = jnp.where(lax.broadcasted_iota(jnp.int32, (B, B), 0) == lane_iota((B, B)), 1.0, 0.0)
    picks = jnp.concatenate([mm_t(eye, idx[s].astype(F32)) for s in range(S)], axis=0)
    lane_e = lane_iota((R, E)).astype(F32)
    gates = jnp.zeros((R, E), F32)
    for k in range(8):
        on = jnp.concatenate([rm[s, :, k, :] for s in range(S)], axis=0) == 1
        mk = jnp.where(on, logits, NEG_FILL)
        pk = jnp.exp(mk - jnp.max(mk, axis=1, keepdims=True))
        pk = pk / jnp.sum(pk, axis=1, keepdims=True)
        gates = gates + jnp.where(picks[:, k:k + 1] == lane_e, pk, 0.0)
    for e in range(E):
        gx[e] = jnp.broadcast_to(gates[:, e:e + 1], (R, 128))

    for i in range(2, 8):
        act(i)
        mix(i - 2)
    mix(6)
    mix(7)

    half = E * FS // 2

    def copy_a(n):
        return remote(pb.at[n, 1 - core], ab.at[n], R_A + n, partner)

    def down(n, carry):
        u = jnp.concatenate([ub[e] for e in range(E)], axis=1)
        wn = wd[:, :, pl.ds(pl.multiple_of(n * CW, CW), CW)].reshape(E * FS, CW)
        dsum[0] = mm(u[:, :half], wn[:half])
        dsum[1] = mm(u[:, half:], wn[half:])
        part = (dsum[0] + dsum[1]).astype(BF16).astype(F32)
        pb[n, 0] = part[:, :HW]
        pb[n, 1] = part[:, HW:]
        copy_a(n).start()
        return carry

    lax.fori_loop(0, NCH, down, 0)
    send_a = [copy_a(n) for n in range(NCH)]
    send_b = [remote(s2.at[n, chip], s2.at[n, chip], R_B + n, peer) for n in range(NCH)]
    send_y = [remote(yb.at[n, core], yb.at[n, core], R_Y + n, partner) for n in range(NCH)]
    for n in range(NCH):
        send_a[n].wait()
        s2[n, chip] = pb[n, core] + ab[n]
        send_b[n].start()
    for n in range(NCH):
        send_b[n].wait()
        yb[n, core] = xm4[n, core] + (s2[n, 0] + s2[n, 1])
        send_y[n].start()
    for n in range(NCH):
        send_y[n].wait()
        for h in range(2):
            hb[:, :, at(2 * n + h, HW)] = yb[n, h].astype(BF16).reshape(S, B, HW)


def write_kernel(h, tk, tv, h_out, tk_out, tv_out, sem):
    copies = [pltpu.make_async_copy(a, b, sem.at[i]) for i, (a, b) in enumerate(((h, h_out), (tk, tk_out), (tv, tv_out)))]
    for c in copies:
        c.start()
    for c in copies:
        c.wait()


def solution(mesh):
    def layer_steps(x_first, next_emb, k_cache, v_cache, seq_len, ln1_gain, ln1_bias, w_q, b_q, w_k, b_k, w_v, b_v, w_o, b_o, ln2_gain, ln2_bias, w_router, w_gate, w_up, w_down, long_factor, expert_idx, route_mask):
        def row(v):
            return v.reshape(1, -1)

        powers = (np.float32(ROPE_BASE) ** (np.arange(32, dtype=np.float32) * np.float32(2.0) / np.float32(HD))).astype(np.float32)
        base = jnp.asarray(np.tile(powers, 4)[None, :])
        args = (
            x_first, next_emb, jnp.transpose(k_cache, (0, 2, 3, 1)), jnp.transpose(v_cache, (0, 2, 3, 1)), seq_len,
            row(ln1_gain), row(ln1_bias), w_q, row(b_q), w_k, row(b_k), w_v, row(b_v), w_o, row(b_o), row(ln2_gain), row(ln2_bias),
            jnp.transpose(w_router), w_gate, w_up, w_down, row(long_factor), jnp.transpose(expert_idx, (0, 2, 1)), route_mask, base,
        )
        V = pltpu.VMEM
        scratch = [
            V((S, B, D), BF16), V((1, D), F32), V((1, D), F32), V((D, D), BF16), V((1, D), F32), V((D, 512), BF16), V((1, 512), F32),
            V((D, 512), BF16), V((1, 512), F32), V((2, 512, D), BF16), V((1, D), F32), V((1, D), F32), V((1, D), F32), V((E, D), BF16),
            V((E, D, FS), BF16), V((E, D, FS), BF16), V((E, FS, D), BF16), V((1, 32), F32), V((S, 8, B), jnp.int32),
            V((S, B, 8, E), jnp.int32), V((1, 128), F32), pltpu.SMEM((B,), jnp.int32), V((B, KV, HD, T), BF16), V((B, KV, HD, T), BF16),
            V((B, 8, 512), F32), V((S, B, 512), F32), V((S, B, 512), F32), V((B, 2, 32, T), F32), V((B, 2, 32, T), BF16),
            V((2, 8, 128), F32), V((4, 8, 128), F32), V((2, 2, 8, 8, 256), F32), V((2, 8, 8, 256), F32), V((2, 2, 8, 8, 256), F32),
            V((4, 8, 8, 512), F32), V((6, 8, 512), F32), V((6, 8, 512), F32), V((6, 8, 512), F32), V((2, 2, 6, 8, 256), F32),
            V((NCH, 2, R, HW), F32), V((E, R, 128), F32), V((E, R, 2 * FS), F32), V((R, 512), F32), V((2, R, CW), F32), V((E, R, FS), BF16), V((NCH, 2, R, HW), F32), V((NCH, R, HW), F32),
            V((NCH, 2, R, HW), F32), V((NCH, 2, R, HW), F32), V((B, S, KV, HD), F32), V((B, S, KV, HD), F32),
            pltpu.SemaphoreType.DMA((NLOCAL,)), pltpu.SemaphoreType.DMA((NREMOTE,)), pltpu.SemaphoreType.DMA((NREMOTE,)),
        ]
        anyspec = pl.BlockSpec(memory_space=pl.ANY)
        outs = [((S, B, D), BF16), ((B, S, KV, HD), BF16), ((B, S, KV, HD), BF16)]
        vmem = pl.BlockSpec(memory_space=pltpu.VMEM)
        parts = pl.pallas_call(
            kernel,
            out_shape=tuple(V(*o) for o in outs),
            in_specs=[anyspec] * len(args),
            out_specs=(vmem,) * 3,
            scratch_shapes=scratch,
            compiler_params=pltpu.CompilerParams(collective_id=0, has_side_effects=True, vmem_limit_bytes=60 * 1024 * 1024),
        )(*args)
        return pl.pallas_call(
            write_kernel,
            out_shape=tuple(jax.ShapeDtypeStruct(*o) for o in outs),
            in_specs=[vmem] * 3,
            out_specs=(anyspec,) * 3,
            scratch_shapes=[pltpu.SemaphoreType.DMA((3,))],
            compiler_params=pltpu.CompilerParams(vmem_limit_bytes=1024 * 1024),
        )(*parts)

    replicated = P()
    in_specs = (P('dp'), P(None, 'dp'), P('dp', 'kv'), P('dp', 'kv'), P('dp')) + (replicated,) * 13 + (P(None, None, 'kv'), P(None, None, 'kv'), P(None, 'kv'), replicated, P(None, 'dp'), P(None, 'dp'))
    out_specs = (P(None, 'dp'), P('dp'), P('dp'))
    return jax.shard_map(layer_steps, mesh=mesh, in_specs=in_specs, out_specs=out_specs, check_vma=False)
```

```python
import functools
import itertools
import math

import jax
import jax.numpy as jnp
import numpy as np
from jax import lax
from jax.experimental import pallas as pl
from jax.experimental.pallas import tpu as pltpu
from jax.sharding import PartitionSpec as P

ROPE_BASE = 10000.0
ROPE_MSCALE = math.sqrt(1.0 + math.log(32.0) / math.log(4096.0))
NORM_EPS = 1e-5
NEG_FILL = -1e30
F32 = jnp.float32
BF16 = jnp.bfloat16

S = 3
B = 16
D = 1024
T = 256
KV = 8
HD = 64
E = 32
FS = 128
R = S * B
NCH = 4
CW = D // NCH
HW = CW // 2

SMALL, PARTS, GROUPS = 16, 4, 8
L_SMALL, L_WQ, L_K, L_V, L_WKV, L_WO, L_GU, L_DN, NLOCAL = itertools.accumulate(
    (SMALL, PARTS, PARTS, PARTS, PARTS, 2 * KV, 2 * GROUPS, GROUPS), initial=0)
R_ML, R_O, R_C, R_G, R_A, R_B, R_Y, NREMOTE = itertools.accumulate((3, 2, 2, 2, NCH, NCH, NCH), initial=0)
LN = 128
HALF = 8


def at(i, width=LN):
    return slice(i * width, (i + 1) * width)


def mm(a, b):
    return jnp.dot(a, b, preferred_element_type=F32)


def mm_t(a, b):
    return lax.dot_general(a, b, (((1,), (1,)), ((), ())), preferred_element_type=F32)


def norm_rows(x, gain, bias):
    mean = jnp.mean(x, axis=-1, keepdims=True)
    cen = x - mean
    var = jnp.mean(cen * cen, axis=-1, keepdims=True)
    return (cen * lax.rsqrt(var + NORM_EPS) * gain + bias).astype(BF16)


def lane_iota(shape):
    return lax.broadcasted_iota(jnp.int32, shape, len(shape) - 1)


def kernel(
    x_first, next_emb, k_hbm, v_hbm, seq_hbm, g1_h, b1_h, wq_h, bq_h, wk_h, bk_h, wv_h, bv_h, wo_h, bo_h, g2_h, b2_h,
    wr_h, wg_h, wu_h, wd_h, lf_h, idx_h, rm_h, base_h,
    hb, tkb, tvb,
    xb, g1, b1, wq, bq, wk, bk, wv, bv, wo, bo, g2, b2, wr, wg, wu, wd, lf, idx, rm, base, seq_s, kc, vc,
    qbuf, kbuf, vbuf, sbuf, wbuf, mlb, mlall, obuf, orecv, c2, ex, ga, gb, tl, oall, xm4, gx, raw, qraw, dsum, ub, pb, ab, s2, yb, tkf, tvf,
    lsem, ssem, rsem,
):
    me = lax.axis_index("kv")
    core = me % 2
    chip = me // 2
    partner = me + 1 - 2 * core
    peer = (me + 2) % 4
    diag = (partner + 2) % 4

    def local(src, dst, i):
        return pltpu.make_async_copy(src, dst, lsem.at[i])

    def remote(src, dst, i, dev):
        return pltpu.make_async_remote_copy(
            src_ref=src, dst_ref=dst, send_sem=ssem.at[i], recv_sem=rsem.at[i],
            device_id={"kv": dev}, device_id_type=pl.DeviceIdType.MESH)

    small = [
        local(src, dst, i) for i, (src, dst) in enumerate((
            (x_first, xb.at[0]), (next_emb, xb.at[pl.ds(1, S - 1)]), (g1_h, g1), (b1_h, b1), (bq_h, bq), (lf_h, lf), (base_h, base),
            (seq_hbm, seq_s), (bk_h, bk), (bv_h, bv), (bo_h, bo), (g2_h, g2), (b2_h, b2), (wr_h, wr), (idx_h, idx), (rm_h, rm)))
    ]
    first, later = small[:HALF], small[HALF:]
    cp_wq = [local(wq_h.at[:, pl.ds(i * T, T)], wq.at[:, pl.ds(i * T, T)], L_WQ + i) for i in range(4)]
    other, own = (1 - core) * 8, core * 8

    def k_part(i):
        sl = pl.ds((other if i < 2 else own) + (i % 2) * 4, 4)
        return local(k_hbm.at[sl], kc.at[sl], L_K + i)

    def v_part(i):
        sl = (pl.ds(other if i < 2 else own, 8), pl.ds((i % 2) * 4, 4))
        return local(v_hbm.at[sl], vc.at[sl], L_V + i)

    cp_k = [k_part(i) for i in range(4)]
    cp_v = [v_part(i) for i in range(4)]
    cp_wkv = []
    for n, (h, v) in enumerate(((wk_h, wk), (wv_h, wv))):
        for i in range(2):
            cp_wkv.append(local(h.at[pl.ds(i * 512, 512)], v.at[pl.ds(i * 512, 512)], L_WKV + 2 * n + i))
    cp_wo = [
        local(wo_h.at[pl.ds(kv * 128 + g * 64, 64)], wo.at[g, pl.ds(kv * 64, 64)], L_WO + 2 * kv + g)
        for kv in range(KV) for g in range(2)
    ]

    def gu_copies(i):
        sl = pl.ds(i * 4, 4)
        return local(wg_h.at[sl], wg.at[sl], L_GU + 2 * i), local(wu_h.at[sl], wu.at[sl], L_GU + 2 * i + 1)

    def dn_copy(i):
        sl = pl.ds(i * 4, 4)
        return local(wd_h.at[sl], wd.at[sl], L_DN + i)

    for c in first + cp_wq + cp_k:
        c.start()
    bar = pltpu.get_barrier_semaphore()
    for dev in (partner, peer, diag):
        pl.semaphore_signal(bar, inc=1, device_id={"kv": dev}, device_id_type=pl.DeviceIdType.MESH)
    qbuf[:, 6:8, :] = jnp.zeros((B, 2, 512), F32)

    for c in first:
        c.wait()
    for c in cp_v:
        c.start()

    lane48 = lane_iota((R, 128))
    inv = 1.0 / (jnp.concatenate([lf[...]] * 4, axis=1) * base[...])
    row_b = lax.broadcasted_iota(jnp.int32, (B, 128), 0)
    len_rows = jnp.zeros((B, 128), jnp.int32)
    for b in range(B):
        len_rows = jnp.where(row_b == b, seq_s[b], len_rows)
    angles = jnp.concatenate([(len_rows + s).astype(F32) for s in range(S)], axis=0) * inv
    cosv = jnp.cos(angles) * ROPE_MSCALE
    sinv = jnp.sin(angles) * ROPE_MSCALE
    low_half = (lane48 % HD) < (HD // 2)

    def rope(x):
        xf = x.astype(BF16).astype(F32)
        rot = jnp.where(low_half, -pltpu.roll(xf, 96, 1), pltpu.roll(xf, 32, 1))
        return (xf * cosv + rot * sinv).astype(BF16).astype(F32)

    h1 = norm_rows(xb[...].reshape(R, D).astype(F32), g1[...], b1[...])

    left = lane48 < HD

    def put_q(q, p):
        qa = rope(q[:, :128]) * 0.125
        qb_ = rope(q[:, 128:]) * 0.125
        pair = (jnp.where(left, qa, pltpu.roll(qb_, 64, 1)), jnp.where(left, pltpu.roll(qa, 64, 1), qb_))
        for g in range(2):
            for s in range(S):
                qbuf[:, 2 * s + g, at(p)] = pair[g][at(s, B)]

    cp_wq[0].wait()
    cp_wq[1].wait()
    q_lo = mm(h1, wq[:, :512]) + bq[:, :512]
    qraw[...] = q_lo
    cp_wq[2].wait()
    cp_wq[3].wait()
    for c in later + cp_wo + cp_wkv:
        c.start()
    q_hi = mm(h1, wq[:, 512:]) + bq[:, 512:]
    for p in range(4):
        put_q(qraw[:, p * 256:(p + 1) * 256] if p < 2 else q_hi[:, (p - 2) * 256:(p - 1) * 256], p)

    rowq = lax.broadcasted_iota(jnp.int32, (32, T), 0)
    laneq = lane_iota((32, T))
    diag_mask = (rowq // 8) == (laneq // HD)
    pos = laneq + me * T
    lane8 = lane_iota((8, 128))

    def scores(start, i):
        qv = qbuf[start + i]
        for hh in range(2):
            rep = jnp.concatenate([qv[:, at(hh, T)]] * 4, axis=0)
            lhs = jnp.where(diag_mask, rep, 0.0).astype(BF16)
            sbuf[start + i, hh] = mm(lhs, kc[start + i, at(hh, 4)].reshape(256, T))

    def soft(start, i, acc):
        keep = pos < seq_s[start + i]
        for hh in range(2):
            sc = jnp.where(keep, sbuf[start + i, hh], NEG_FILL)
            m = jnp.max(sc, axis=1, keepdims=True)
            w = jnp.where(keep, jnp.exp(sc - m), 0.0)
            l = jnp.sum(w, axis=1, keepdims=True)
            wbuf[start + i, hh] = w.astype(BF16)
            for j in range(4):
                spot = i * 16 + hh * 4 + j
                acc = jnp.where(lane8 == spot, m[at(j, 8)], acc)
                acc = jnp.where(lane8 == spot + 8, l[at(j, 8)], acc)
        return acc

    left8 = lane8 < HD

    def values(half, i, hh):
        b = half * 8 + i
        pv = mm_t(wbuf[b, hh], vc[b, at(hh, 4)].reshape(256, T))
        obuf[half, hh, i, :, 0:128] = jnp.where(left8, pv[0:8, 0:128], pv[8:16, 0:128])
        obuf[half, hh, i, :, 128:256] = jnp.where(left8, pv[16:24, 128:256], pv[24:32, 128:256])

    send_ml = [
        remote(mlb.at[1 - core], mlall.at[me], R_ML, partner), remote(mlb.at[core], mlall.at[me], R_ML + 1, peer),
        remote(mlb.at[1 - core], mlall.at[me], R_ML + 2, diag),
    ]
    send_o = [remote(obuf.at[1 - core, hh], orecv.at[hh], R_O + hh, partner) for hh in range(2)]
    zero = jnp.zeros((8, 128), F32)

    cp_k[0].wait()
    for i in range(4):
        scores(other, i)
    cp_k[1].wait()
    for i in range(4):
        scores(other, 4 + i)
    acc = zero
    for i in range(4):
        acc = soft(other, i, acc)
    cp_k[2].wait()
    for i in range(8):
        for c in gu_copies(i):
            c.start()
    for i in range(4):
        scores(own, i)
    for i in range(4):
        acc = soft(other, 4 + i, acc)
    mlb[1 - core] = acc
    pl.semaphore_wait(bar, 3)
    send_ml[0].start()
    send_ml[2].start()

    cp_v[0].wait()
    cp_k[3].wait()
    for i in range(8):
        values(1 - core, i, 0)
    for i in range(4):
        scores(own, 4 + i)
    acc = zero
    for i in range(4):
        acc = soft(own, i, acc)
    send_o[0].start()
    cp_v[1].wait()
    for i in range(8):
        dn_copy(i).start()
    for i in range(8):
        values(1 - core, i, 1)
    for i in range(4):
        acc = soft(own, 4 + i, acc)
    mlb[core] = acc
    mlall[me] = acc
    send_o[1].start()
    send_ml[1].start()

    pick = (lane8 // HD)

    def spread(v, i, p):
        return jnp.take_along_axis(v, pick + (i * 16 + 2 * p), axis=1, mode="promise_in_bounds")

    send_c = [remote(c2.at[hh, chip, pl.ds(0, 6)], c2.at[hh, chip, pl.ds(0, 6)], R_C + hh, peer) for hh in range(2)]
    for hh in range(2):
        cp_v[2 + hh].wait()
        for i in range(8):
            values(core, i, hh)
        if hh == 0:
            send_ml[0].wait()
            ml_a = mlall[me]
            ml_b = mlall[partner]
            m_ab = jnp.maximum(ml_a, ml_b)
            f_a = jnp.exp(ml_a - m_ab)
            f_b = jnp.exp(ml_b - m_ab)
        send_o[hh].wait()
        for i in range(8):
            oa = obuf[core, hh, i]
            ob = orecv[hh, i]
            for p in range(2):
                ln = at(p)
                c2[hh, chip, :, i, ln] = (
                    oa[:, ln] * spread(f_a, i, 2 * hh + p) + ob[:, ln] * spread(f_b, i, 2 * hh + p))
        send_c[hh].start()

    for c in later + cp_wkv:
        c.wait()
    kn = mm(h1, wk[...]) + bk[...]
    vn = (mm(h1, wv[...]) + bv[...]).astype(BF16)
    vn = vn.astype(F32)
    for p in range(4):
        ln = at(p)
        for val, buf, fin in ((rope(kn[:, ln]), kbuf, tkf), (vn[:, ln], vbuf, tvf)):
            swap = pltpu.roll(val, 64, 1)
            for s in range(S):
                r = at(s, B)
                buf[s, :, ln] = val[r]
                fin[:, s, 2 * p, :] = val[r, :HD]
                fin[:, s, 2 * p + 1, :] = swap[r, :HD]
    tkb[...] = tkf[...].astype(BF16)
    tvb[...] = tvf[...].astype(BF16)

    rows = pl.ds(pl.multiple_of(core * 8, 8), 8)
    kt = [kbuf[t, rows, :] for t in range(S)]
    vt = [vbuf[t, rows, :] for t in range(S)]
    trip = [(s, g, t) for s in range(S) for g in range(2) for t in range(s + 1)]
    prod = jnp.concatenate([qbuf[rows, 2 * s + g, :] * kt[t] for s, g, t in trip], axis=0)
    hi = prod.astype(BF16)
    lo = (prod - hi.astype(F32)).astype(BF16)
    r2 = lax.broadcasted_iota(jnp.int32, (256, 128), 0)
    ones = jnp.where(((r2 % 128) // HD) == (lane_iota((256, 128)) // HD), 1.0, 0.0).astype(BF16)
    tsc = jnp.concatenate(
        [mm(jnp.concatenate([hi[:, at(p)], lo[:, at(p)]], axis=1), ones) for p in range(4)], axis=1)

    for c in send_ml[1:]:
        c.wait()
    ml = [mlall[d] for d in range(4)]
    for ch in range(2):
        a, b_ = ml[2 * ch], ml[2 * ch + 1]
        mc = jnp.maximum(a, b_)
        lc = (pltpu.roll(a, 120, 1) * jnp.exp(a - mc) + pltpu.roll(b_, 120, 1) * jnp.exp(b_ - mc))
        for i in range(8):
            for p in range(4):
                ln = at(p)
                ex[2 * ch, :, i, ln] = spread(mc, i, p)
                ex[2 * ch + 1, :, i, ln] = spread(lc, i, p)

    for s in range(S):
        for g in range(2):
            j = 2 * s + g
            sc = [tsc[at(n, 8)] for n, key in enumerate(trip) if key[:2] == (s, g)]
            mt = functools.reduce(jnp.maximum, sc)
            wt = [jnp.exp(v - mt) for v in sc]
            lt = functools.reduce(jnp.add, wt)
            ot = functools.reduce(jnp.add, [w.astype(BF16).astype(F32) * v for w, v in zip(wt, vt)])
            m0, l0, m1, l1 = ex[0, j], ex[1, j], ex[2, j], ex[3, j]
            top = jnp.maximum(jnp.maximum(m0, m1), mt)
            f0, f1, ft = jnp.exp(m0 - top), jnp.exp(m1 - top), jnp.exp(mt - top)
            inv_l = 1.0 / (l0 * f0 + l1 * f1 + lt * ft)
            ga[j] = f0 * inv_l
            gb[j] = f1 * inv_l
            tl[j] = ot * (ft * inv_l)

    send_g = [remote(oall.at[core, hh], oall.at[core, hh], R_G + hh, partner) for hh in range(2)]
    for hh in range(2):
        send_c[hh].wait()
        ln = at(hh, T)
        for j in range(6):
            oall[core, hh, j] = c2[hh, 0, j] * ga[j][:, ln] + c2[hh, 1, j] * gb[j][:, ln] + tl[j][:, ln]
        send_g[hh].start()

    for c in cp_wo:
        c.wait()
    att = None
    for hh in range(2):
        send_g[hh].wait()
        for g in range(2):
            o_g = jnp.concatenate([oall[h, hh, 2 * s + g] for s in range(S) for h in range(2)], axis=0).astype(BF16)
            part = mm(o_g, wo[g, at(hh, T)])
            att = part if att is None else att + part
    xm = (xb[...].reshape(R, D).astype(F32) + att + bo[...]).astype(BF16).astype(F32)
    for n in range(NCH):
        for h in range(2):
            xm4[n, h] = xm[:, at(2 * n + h, HW)]
    h2 = norm_rows(xm, g2[...], b2[...])

    def act(i):
        for n in range(4):
            e = i * 4 + n
            raw[e] = mm(h2, jnp.concatenate([wg[e], wu[e]], axis=1))

    def mix(i):
        for n in range(4):
            e = i * 4 + n
            a, up = raw[e, :, :FS], raw[e, :, FS:]
            ub[e] = (gx[e] * (a * (1.0 / (1.0 + jnp.exp(-a)))) * up).astype(BF16)

    for i in range(8):
        for c in gu_copies(i):
            c.wait()
    logits = mm_t(h2, wr[...])
    act(0)
    act(1)
    eye = jnp.where(lax.broadcasted_iota(jnp.int32, (B, B), 0) == lane_iota((B, B)), 1.0, 0.0)
    picks = jnp.concatenate([mm_t(eye, idx[s].astype(F32)) for s in range(S)], axis=0)
    lane_e = lane_iota((R, E)).astype(F32)
    gates = jnp.zeros((R, E), F32)
    for k in range(8):
        on = jnp.concatenate([rm[s, :, k, :] for s in range(S)], axis=0) == 1
        mk = jnp.where(on, logits, NEG_FILL)
        pk = jnp.exp(mk - jnp.max(mk, axis=1, keepdims=True))
        pk = pk / jnp.sum(pk, axis=1, keepdims=True)
        gates = gates + jnp.where(picks[:, k:k + 1] == lane_e, pk, 0.0)
    for e in range(E):
        gx[e] = jnp.broadcast_to(gates[:, e:e + 1], (R, 128))

    for i in range(2, 8):
        act(i)
        mix(i - 2)
    mix(6)
    mix(7)

    for i in range(GROUPS):
        dn_copy(i).wait()
    half = E * FS // 2

    def copy_a(n):
        return remote(pb.at[n, 1 - core], ab.at[n], R_A + n, partner)

    def down(n, carry):
        u = jnp.concatenate([ub[e] for e in range(E)], axis=1)
        wn = wd[:, :, pl.ds(pl.multiple_of(n * CW, CW), CW)].reshape(E * FS, CW)
        dsum[0] = mm(u[:, :half], wn[:half])
        dsum[1] = mm(u[:, half:], wn[half:])
        part = (dsum[0] + dsum[1]).astype(BF16).astype(F32)
        pb[n, 0] = part[:, :HW]
        pb[n, 1] = part[:, HW:]
        copy_a(n).start()
        return carry

    lax.fori_loop(0, NCH, down, 0)
    send_a = [copy_a(n) for n in range(NCH)]
    send_b = [remote(s2.at[n, chip], s2.at[n, chip], R_B + n, peer) for n in range(NCH)]
    send_y = [remote(yb.at[n, core], yb.at[n, core], R_Y + n, partner) for n in range(NCH)]
    for n in range(NCH):
        send_a[n].wait()
        s2[n, chip] = pb[n, core] + ab[n]
        send_b[n].start()
    for n in range(NCH):
        send_b[n].wait()
        yb[n, core] = xm4[n, core] + (s2[n, 0] + s2[n, 1])
        send_y[n].start()
    for n in range(NCH):
        send_y[n].wait()
        for h in range(2):
            hb[:, :, at(2 * n + h, HW)] = yb[n, h].astype(BF16).reshape(S, B, HW)


def write_kernel(h, tk, tv, h_out, tk_out, tv_out, sem):
    copies = [pltpu.make_async_copy(a, b, sem.at[i]) for i, (a, b) in enumerate(((h, h_out), (tk, tk_out), (tv, tv_out)))]
    for c in copies:
        c.start()
    for c in copies:
        c.wait()


def solution(mesh):
    def layer_steps(x_first, next_emb, k_cache, v_cache, seq_len, ln1_gain, ln1_bias, w_q, b_q, w_k, b_k, w_v, b_v, w_o, b_o, ln2_gain, ln2_bias, w_router, w_gate, w_up, w_down, long_factor, expert_idx, route_mask):
        def row(v):
            return v.reshape(1, -1)

        powers = (np.float32(ROPE_BASE) ** (np.arange(32, dtype=np.float32) * np.float32(2.0) / np.float32(HD))).astype(np.float32)
        base = jnp.asarray(np.tile(powers, 4)[None, :])
        args = (
            x_first, next_emb, jnp.transpose(k_cache, (0, 2, 3, 1)), jnp.transpose(v_cache, (0, 2, 3, 1)), seq_len,
            row(ln1_gain), row(ln1_bias), w_q, row(b_q), w_k, row(b_k), w_v, row(b_v), w_o, row(b_o), row(ln2_gain), row(ln2_bias),
            jnp.transpose(w_router), w_gate, w_up, w_down, row(long_factor), jnp.transpose(expert_idx, (0, 2, 1)), route_mask, base,
        )
        V = pltpu.VMEM
        scratch = [
            V((S, B, D), BF16), V((1, D), F32), V((1, D), F32), V((D, D), BF16), V((1, D), F32), V((D, 512), BF16), V((1, 512), F32),
            V((D, 512), BF16), V((1, 512), F32), V((2, 512, D), BF16), V((1, D), F32), V((1, D), F32), V((1, D), F32), V((E, D), BF16),
            V((E, D, FS), BF16), V((E, D, FS), BF16), V((E, FS, D), BF16), V((1, 32), F32), V((S, 8, B), jnp.int32),
            V((S, B, 8, E), jnp.int32), V((1, 128), F32), pltpu.SMEM((B,), jnp.int32), V((B, KV, HD, T), BF16), V((B, KV, HD, T), BF16),
            V((B, 8, 512), F32), V((S, B, 512), F32), V((S, B, 512), F32), V((B, 2, 32, T), F32), V((B, 2, 32, T), BF16),
            V((2, 8, 128), F32), V((4, 8, 128), F32), V((2, 2, 8, 8, 256), F32), V((2, 8, 8, 256), F32), V((2, 2, 8, 8, 256), F32),
            V((4, 8, 8, 512), F32), V((6, 8, 512), F32), V((6, 8, 512), F32), V((6, 8, 512), F32), V((2, 2, 6, 8, 256), F32),
            V((NCH, 2, R, HW), F32), V((E, R, 128), F32), V((E, R, 2 * FS), F32), V((R, 512), F32), V((2, R, CW), F32), V((E, R, FS), BF16), V((NCH, 2, R, HW), F32), V((NCH, R, HW), F32),
            V((NCH, 2, R, HW), F32), V((NCH, 2, R, HW), F32), V((B, S, KV, HD), F32), V((B, S, KV, HD), F32),
            pltpu.SemaphoreType.DMA((NLOCAL,)), pltpu.SemaphoreType.DMA((NREMOTE,)), pltpu.SemaphoreType.DMA((NREMOTE,)),
        ]
        anyspec = pl.BlockSpec(memory_space=pl.ANY)
        outs = [((S, B, D), BF16), ((B, S, KV, HD), BF16), ((B, S, KV, HD), BF16)]
        vmem = pl.BlockSpec(memory_space=pltpu.VMEM)
        parts = pl.pallas_call(
            kernel,
            out_shape=tuple(V(*o) for o in outs),
            in_specs=[anyspec] * len(args),
            out_specs=(vmem,) * 3,
            scratch_shapes=scratch,
            compiler_params=pltpu.CompilerParams(collective_id=0, has_side_effects=True, vmem_limit_bytes=60 * 1024 * 1024),
        )(*args)
        return pl.pallas_call(
            write_kernel,
            out_shape=tuple(jax.ShapeDtypeStruct(*o) for o in outs),
            in_specs=[vmem] * 3,
            out_specs=(anyspec,) * 3,
            scratch_shapes=[pltpu.SemaphoreType.DMA((3,))],
            compiler_params=pltpu.CompilerParams(vmem_limit_bytes=1024 * 1024),
        )(*parts)

    replicated = P()
    in_specs = (P('dp'), P(None, 'dp'), P('dp', 'kv'), P('dp', 'kv'), P('dp')) + (replicated,) * 13 + (P(None, None, 'kv'), P(None, None, 'kv'), P(None, 'kv'), replicated, P(None, 'dp'), P(None, 'dp'))
    out_specs = (P(None, 'dp'), P('dp'), P('dp'))
    return jax.shard_map(layer_steps, mesh=mesh, in_specs=in_specs, out_specs=out_specs, check_vma=False)
```

```python
import functools
import itertools
import math

import jax
import jax.numpy as jnp
import numpy as np
from jax import lax
from jax.experimental import pallas as pl
from jax.experimental.pallas import tpu as pltpu
from jax.sharding import PartitionSpec as P

ROPE_BASE = 10000.0
ROPE_MSCALE = math.sqrt(1.0 + math.log(32.0) / math.log(4096.0))
NORM_EPS = 1e-5
NEG_FILL = -1e30
F32 = jnp.float32
BF16 = jnp.bfloat16

S = 3
B = 16
D = 1024
T = 256
KV = 8
HD = 64
E = 32
FS = 128
R = S * B
NCH = 4
CW = D // NCH

GROUPS = 8
SMALL, PARTS = 8, 4
L_SMALL, L_WQ, L_K, L_V, L_WO, L_GU, L_DN, NLOCAL = itertools.accumulate((SMALL, 2, PARTS, PARTS, 1, 2, 1), initial=0)
R_ML, R_O, R_C, R_G, R_P, R_B, NRECV = itertools.accumulate((3, 2, 2, 2, NCH, NCH), initial=0)
S_ML, S_O, S_C, S_G, S_P, S_B, NSEND = range(7)
LN = 128
HALF = 8


def at(i, width=LN):
    return slice(i * width, (i + 1) * width)


def mm(a, b):
    return jnp.dot(a, b, preferred_element_type=F32)


def mm_t(a, b):
    return lax.dot_general(a, b, (((1,), (1,)), ((), ())), preferred_element_type=F32)


def norm_rows(x, gain, bias):
    mean = jnp.mean(x, axis=-1, keepdims=True)
    cen = x - mean
    var = jnp.mean(cen * cen, axis=-1, keepdims=True)
    return (cen * lax.rsqrt(var + NORM_EPS) * gain + bias).astype(BF16)


def lane_iota(shape):
    return lax.broadcasted_iota(jnp.int32, shape, len(shape) - 1)


def kernel(
    x_first, next_emb, k_hbm, v_hbm, seq_hbm, g1_h, b1_h, wq_h, bq_h, wk_h, bk_h, wv_h, bv_h, wo_h, bo_h, g2_h, b2_h,
    wr_h, wg_h, wu_h, wd_h, lf_h, idx_h, rm_h, base_h,
    hb, tkb, tvb,
    xb, g1, b1, wq, bq, wk, bk, wv, bv, wo, bo, g2, b2, wr, wg, wu, wd, lf, idx, rm, base, seq_s, kc, vc,
    qbuf, kbuf, vbuf, sbuf, wbuf, mlb, mlall, obuf, orecv, c2, ex, ga, gb, tl, oall, xm4, gx, raw, qraw, picks, ub, pb, ab, s2, yb, tkf, tvf,
    lsem, ssem, rsem,
):
    me = lax.axis_index("kv")
    core = me % 2
    chip = me // 2
    partner = me + 1 - 2 * core
    peer = (me + 2) % 4
    diag = (partner + 2) % 4

    def local(src, dst, i):
        return pltpu.make_async_copy(src, dst, lsem.at[i])

    def remote(src, dst, snd, rcv, dev):
        return pltpu.make_async_remote_copy(
            src_ref=src, dst_ref=dst, send_sem=ssem.at[snd], recv_sem=rsem.at[rcv],
            device_id={"kv": dev}, device_id_type=pl.DeviceIdType.MESH)

    small = [
        local(src, dst, L_SMALL + i % SMALL) for i, (src, dst) in enumerate((
            (x_first, xb.at[0]), (next_emb, xb.at[pl.ds(1, S - 1)]), (g1_h, g1), (b1_h, b1), (bq_h, bq), (lf_h, lf), (base_h, base),
            (seq_hbm, seq_s), (bk_h, bk), (bv_h, bv), (bo_h, bo), (g2_h, g2), (b2_h, b2), (wr_h, wr), (idx_h, idx), (rm_h, rm)))
    ]
    first, later = small[:SMALL], small[SMALL:]
    cp_wq = [local(wq_h.at[:, pl.ds(i * 512, 512)], wq.at[:, pl.ds(i * 512, 512)], L_WQ + i) for i in range(2)]
    other, own = (1 - core) * 8, core * 8

    def k_part(i):
        sl = pl.ds((other if i < 2 else own) + (i % 2) * 4, 4)
        return local(k_hbm.at[sl], kc.at[sl], L_K + i)

    def v_part(i):
        sl = (pl.ds(other if i < 2 else own, 8), pl.ds((i % 2) * 4, 4))
        return local(v_hbm.at[sl], vc.at[sl], L_V + i)

    cp_k = [k_part(i) for i in range(4)]
    cp_v = [v_part(i) for i in range(4)]
    cp_wkv = [local(wk_h, wk, L_WQ), local(wv_h, wv, L_WQ + 1)]
    cp_wo = [
        local(wo_h.at[pl.ds(kv * 128 + g * 64, 64)], wo.at[g, pl.ds(kv * 64, 64)], L_WO) for kv in range(KV) for g in range(2)
    ]

    def up_copy(src, dst, i, sem):
        sl = pl.ds(i * 4, 4)
        return local(src.at[sl], dst.at[sl], sem)

    for c in first + cp_wq + cp_k:
        c.start()
    bar = pltpu.get_barrier_semaphore()
    for dev in (partner, peer, diag):
        pl.semaphore_signal(bar, inc=1, device_id={"kv": dev}, device_id_type=pl.DeviceIdType.MESH)
    qbuf[:, 6:8, :] = jnp.zeros((B, 2, 512), F32)

    for c in first:
        c.wait()
    for c in cp_v:
        c.start()

    lane48 = lane_iota((R, 128))
    inv = 1.0 / (jnp.concatenate([lf[...]] * 4, axis=1) * base[...])
    row_b = lax.broadcasted_iota(jnp.int32, (B, 128), 0)
    len_rows = jnp.zeros((B, 128), jnp.int32)
    for b in range(B):
        len_rows = jnp.where(row_b == b, seq_s[b], len_rows)
    angles = jnp.concatenate([(len_rows + s).astype(F32) for s in range(S)], axis=0) * inv
    cosv = jnp.cos(angles) * ROPE_MSCALE
    sinv = jnp.sin(angles) * ROPE_MSCALE
    low_half = (lane48 % HD) < (HD // 2)

    def rope(x):
        xf = x.astype(BF16).astype(F32)
        rot = jnp.where(low_half, -pltpu.roll(xf, 96, 1), pltpu.roll(xf, 32, 1))
        return (xf * cosv + rot * sinv).astype(BF16).astype(F32)

    h1 = norm_rows(xb[...].reshape(R, D).astype(F32), g1[...], b1[...])

    left = lane48 < HD

    def put_q(q, p):
        qa = rope(q[:, :128]) * 0.125
        qb_ = rope(q[:, 128:]) * 0.125
        pair = (jnp.where(left, qa, pltpu.roll(qb_, 64, 1)), jnp.where(left, pltpu.roll(qa, 64, 1), qb_))
        for g in range(2):
            for s in range(S):
                qbuf[:, 2 * s + g, at(p)] = pair[g][at(s, B)]

    cp_wq[0].wait()
    q_lo = mm(h1, wq[:, :512]) + bq[:, :512]
    qraw[...] = q_lo
    cp_wq[1].wait()
    for c in later + cp_wo + cp_wkv:
        c.start()
    q_hi = mm(h1, wq[:, 512:]) + bq[:, 512:]
    for p in range(4):
        put_q(qraw[:, p * 256:(p + 1) * 256] if p < 2 else q_hi[:, (p - 2) * 256:(p - 1) * 256], p)

    rowq = lax.broadcasted_iota(jnp.int32, (32, T), 0)
    laneq = lane_iota((32, T))
    diag_mask = (rowq // 8) == (laneq // HD)
    pos = laneq + me * T
    lane8 = lane_iota((8, 128))

    def scores(start, i):
        qv = qbuf[start + i]
        for hh in range(2):
            rep = jnp.concatenate([qv[:, at(hh, T)]] * 4, axis=0)
            lhs = jnp.where(diag_mask, rep, 0.0).astype(BF16)
            sbuf[start + i, hh] = mm(lhs, kc[start + i, at(hh, 4)].reshape(256, T))

    def soft(start, i, acc):
        keep = pos < seq_s[start + i]
        for hh in range(2):
            sc = jnp.where(keep, sbuf[start + i, hh], NEG_FILL)
            m = jnp.max(sc, axis=1, keepdims=True)
            w = jnp.where(keep, jnp.exp(sc - m), 0.0)
            l = jnp.sum(w, axis=1, keepdims=True)
            wbuf[start + i, hh] = w.astype(BF16)
            for j in range(4):
                spot = i * 16 + hh * 4 + j
                acc = jnp.where(lane8 == spot, m[at(j, 8)], acc)
                acc = jnp.where(lane8 == spot + 8, l[at(j, 8)], acc)
        return acc

    left8 = lane8 < HD

    def values(half, i, hh):
        b = half * 8 + i
        pv = mm_t(wbuf[b, hh], vc[b, at(hh, 4)].reshape(256, T))
        obuf[half, hh, i, :, 0:128] = jnp.where(left8, pv[0:8, 0:128], pv[8:16, 0:128])
        obuf[half, hh, i, :, 128:256] = jnp.where(left8, pv[16:24, 128:256], pv[24:32, 128:256])

    send_ml = [
        remote(mlb.at[1 - core], mlall.at[me], S_ML, R_ML, partner), remote(mlb.at[core], mlall.at[me], S_ML, R_ML + 1, peer),
        remote(mlb.at[1 - core], mlall.at[me], S_ML, R_ML + 2, diag),
    ]
    send_o = [remote(obuf.at[1 - core, hh], orecv.at[hh], S_O, R_O + hh, partner) for hh in range(2)]
    zero = jnp.zeros((8, 128), F32)

    cp_k[0].wait()
    for i in range(4):
        scores(other, i)
    cp_k[1].wait()
    for i in range(4):
        scores(other, 4 + i)
    acc = zero
    for i in range(4):
        acc = soft(other, i, acc)
    cp_k[2].wait()
    for i in range(GROUPS):
        up_copy(wg_h, wg, i, L_GU).start()
        up_copy(wu_h, wu, i, L_GU + 1).start()
    for i in range(4):
        scores(own, i)
    for i in range(4):
        acc = soft(other, 4 + i, acc)
    mlb[1 - core] = acc
    pl.semaphore_wait(bar, 3)
    send_ml[0].start()
    send_ml[2].start()

    cp_v[0].wait()
    cp_k[3].wait()
    for i in range(8):
        values(1 - core, i, 0)
    for i in range(4):
        scores(own, 4 + i)
    acc = zero
    for i in range(4):
        acc = soft(own, i, acc)
    send_o[0].start()
    cp_v[1].wait()
    for i in range(GROUPS):
        up_copy(wd_h, wd, i, L_DN).start()
    for i in range(8):
        values(1 - core, i, 1)
    for i in range(4):
        acc = soft(own, 4 + i, acc)
    mlb[core] = acc
    mlall[me] = acc
    send_o[1].start()
    send_ml[1].start()

    pick = (lane8 // HD)

    def spread(v, i, p):
        return jnp.take_along_axis(v, pick + (i * 16 + 2 * p), axis=1, mode="promise_in_bounds")

    send_c = [remote(c2.at[hh, chip, pl.ds(0, 6)], c2.at[hh, chip, pl.ds(0, 6)], S_C, R_C + hh, peer) for hh in range(2)]
    for hh in range(2):
        cp_v[2 + hh].wait()
        for i in range(8):
            values(core, i, hh)
        if hh == 0:
            send_ml[0].wait_recv()
            ml_a = mlall[me]
            ml_b = mlall[partner]
            m_ab = jnp.maximum(ml_a, ml_b)
            f_a = jnp.exp(ml_a - m_ab)
            f_b = jnp.exp(ml_b - m_ab)
        send_o[hh].wait_recv()
        for i in range(8):
            oa = obuf[core, hh, i]
            ob = orecv[hh, i]
            for p in range(2):
                ln = at(p)
                c2[hh, chip, :, i, ln] = (
                    oa[:, ln] * spread(f_a, i, 2 * hh + p) + ob[:, ln] * spread(f_b, i, 2 * hh + p))
        send_c[hh].start()

    for c in later + cp_wkv:
        c.wait()
    kn = mm(h1, wk[...]) + bk[...]
    vn = (mm(h1, wv[...]) + bv[...]).astype(BF16)
    vn = vn.astype(F32)
    for p in range(4):
        ln = at(p)
        for val, buf, fin in ((rope(kn[:, ln]), kbuf, tkf), (vn[:, ln], vbuf, tvf)):
            swap = pltpu.roll(val, 64, 1)
            for s in range(S):
                r = at(s, B)
                buf[s, :, ln] = val[r]
                fin[:, s, 2 * p, :] = val[r, :HD]
                fin[:, s, 2 * p + 1, :] = swap[r, :HD]
    tkb[...] = tkf[...].astype(BF16)
    tvb[...] = tvf[...].astype(BF16)

    rows = pl.ds(pl.multiple_of(core * 8, 8), 8)
    kt = [kbuf[t, rows, :] for t in range(S)]
    vt = [vbuf[t, rows, :] for t in range(S)]
    trip = [(s, g, t) for s in range(S) for g in range(2) for t in range(s + 1)]
    prod = jnp.concatenate([qbuf[rows, 2 * s + g, :] * kt[t] for s, g, t in trip], axis=0)
    hi = prod.astype(BF16)
    lo = (prod - hi.astype(F32)).astype(BF16)
    r2 = lax.broadcasted_iota(jnp.int32, (256, 128), 0)
    ones = jnp.where(((r2 % 128) // HD) == (lane_iota((256, 128)) // HD), 1.0, 0.0).astype(BF16)
    tsc = jnp.concatenate(
        [mm(jnp.concatenate([hi[:, at(p)], lo[:, at(p)]], axis=1), ones) for p in range(4)], axis=1)

    eye = jnp.where(lax.broadcasted_iota(jnp.int32, (B, B), 0) == lane_iota((B, B)), 1.0, 0.0)
    picks[...] = jnp.concatenate([mm_t(eye, idx[s].astype(F32)) for s in range(S)], axis=0)

    for c in send_ml[1:]:
        c.wait_recv()
    ml = [mlall[d] for d in range(4)]
    for ch in range(2):
        a, b_ = ml[2 * ch], ml[2 * ch + 1]
        mc = jnp.maximum(a, b_)
        lc = (pltpu.roll(a, 120, 1) * jnp.exp(a - mc) + pltpu.roll(b_, 120, 1) * jnp.exp(b_ - mc))
        for i in range(8):
            for p in range(4):
                ln = at(p)
                ex[2 * ch, :, i, ln] = spread(mc, i, p)
                ex[2 * ch + 1, :, i, ln] = spread(lc, i, p)

    for s in range(S):
        for g in range(2):
            j = 2 * s + g
            sc = [tsc[at(n, 8)] for n, key in enumerate(trip) if key[:2] == (s, g)]
            mt = functools.reduce(jnp.maximum, sc)
            wt = [jnp.exp(v - mt) for v in sc]
            lt = functools.reduce(jnp.add, wt)
            ot = functools.reduce(jnp.add, [w.astype(BF16).astype(F32) * v for w, v in zip(wt, vt)])
            m0, l0, m1, l1 = ex[0, j], ex[1, j], ex[2, j], ex[3, j]
            top = jnp.maximum(jnp.maximum(m0, m1), mt)
            f0, f1, ft = jnp.exp(m0 - top), jnp.exp(m1 - top), jnp.exp(mt - top)
            inv_l = 1.0 / (l0 * f0 + l1 * f1 + lt * ft)
            ga[j] = f0 * inv_l
            gb[j] = f1 * inv_l
            tl[j] = ot * (ft * inv_l)

    send_g = [remote(oall.at[core, hh], oall.at[core, hh], S_G, R_G + hh, partner) for hh in range(2)]
    for hh in range(2):
        send_c[hh].wait_recv()
        ln = at(hh, T)
        for j in range(6):
            oall[core, hh, j] = c2[hh, 0, j] * ga[j][:, ln] + c2[hh, 1, j] * gb[j][:, ln] + tl[j][:, ln]
        send_g[hh].start()

    local(wo, wo, L_WO).wait()
    att = None
    for hh in range(2):
        send_g[hh].wait_recv()
        for g in range(2):
            o_g = jnp.concatenate([oall[h, hh, 2 * s + g] for s in range(S) for h in range(2)], axis=0).astype(BF16)
            part = mm(o_g, wo[g, at(hh, T)])
            att = part if att is None else att + part
    xm = (xb[...].reshape(R, D).astype(F32) + att + bo[...]).astype(BF16).astype(F32)
    for n in range(NCH):
        xm4[n] = xm[:, at(n, CW)]
    h2 = norm_rows(xm, g2[...], b2[...])

    def act(i):
        for n in range(4):
            e = i * 4 + n
            raw[e] = mm(h2, jnp.concatenate([wg[e], wu[e]], axis=1))

    def mix(i):
        for n in range(4):
            e = i * 4 + n
            a, up = raw[e, :, :FS], raw[e, :, FS:]
            ub[e] = (gx[e] * (a * (1.0 / (1.0 + jnp.exp(-a)))) * up).astype(BF16)

    local(wg, wg, L_GU).wait()
    local(wu, wu, L_GU + 1).wait()
    logits = mm_t(h2, wr[...])
    for i in range(4):
        act(i)
    lane_e = lane_iota((R, E)).astype(F32)
    chosen = picks[...]
    gates = jnp.zeros((R, E), F32)
    for k in range(8):
        on = jnp.concatenate([rm[s, :, k, :] for s in range(S)], axis=0) == 1
        mk = jnp.where(on, logits, NEG_FILL)
        pk = jnp.exp(mk - jnp.max(mk, axis=1, keepdims=True))
        pk = pk / jnp.sum(pk, axis=1, keepdims=True)
        gates = gates + jnp.where(chosen[:, k:k + 1] == lane_e, pk, 0.0)
    for e in range(E):
        gx[e] = jnp.broadcast_to(gates[:, e:e + 1], (R, 128))

    for i in range(4, 6):
        act(i)
        mix(i - 4)

    def down(m):
        u = jnp.concatenate([ub[e] for e in range(E)], axis=1)
        part = mm(u, wd[:, :, at(m, 2 * CW)].reshape(E * FS, 2 * CW)).astype(BF16).astype(F32)
        pb[2 * m] = part[:, :CW]
        pb[2 * m + 1] = part[:, CW:]

    send_a = [remote(pb.at[n], ab.at[n], S_P, R_P + n, partner) for n in range(NCH)]
    send_b = [remote(s2.at[n, chip], s2.at[n, chip], S_B, R_B + n, peer) for n in range(NCH)]
    send_y = [remote(yb.at[n], yb.at[n], S_P, R_P + n, partner) for n in range(NCH)]

    local(wd, wd, L_DN).wait()
    for i in range(6, 8):
        act(i)
        mix(i - 4)
    for i in range(4, 8):
        mix(i)
    for m in range(2):
        down(m)

        @pl.when(core == 0)
        def _():
            for n in (2 * m, 2 * m + 1):
                send_a[n].start()

    @pl.when(core == 1)
    def _():
        for n in range(NCH):
            send_a[n].wait_recv()
            s2[n, chip] = ab[n] + pb[n]
            send_b[n].start()
        for n in range(NCH):
            send_b[n].wait_recv()
            yb[n] = xm4[n] + (s2[n, 0] + s2[n, 1])
            send_y[n].start()
            hb[:, :, at(n, CW)] = yb[n].astype(BF16).reshape(S, B, CW)
        remote(s2.at[:, chip], s2.at[:, chip], S_B, R_B, peer).wait_send()

    @pl.when(core == 0)
    def _():
        for n in range(NCH):
            send_y[n].wait_recv()
            hb[:, :, at(n, CW)] = yb[n].astype(BF16).reshape(S, B, CW)

    for ref, snd in ((mlall.at[pl.ds(0, 3)], S_ML), (obuf.at[1 - core], S_O), (c2.at[:, chip, pl.ds(0, 6)], S_C), (oall.at[core], S_G), (pb, S_P)):
        remote(ref, ref, snd, R_ML, partner).wait_send()


def write_kernel(h, tk, tv, h_out, tk_out, tv_out, sem):
    copies = [pltpu.make_async_copy(a, b, sem.at[i]) for i, (a, b) in enumerate(((h, h_out), (tk, tk_out), (tv, tv_out)))]
    for c in copies:
        c.start()
    for c in copies:
        c.wait()


def solution(mesh):
    def layer_steps(x_first, next_emb, k_cache, v_cache, seq_len, ln1_gain, ln1_bias, w_q, b_q, w_k, b_k, w_v, b_v, w_o, b_o, ln2_gain, ln2_bias, w_router, w_gate, w_up, w_down, long_factor, expert_idx, route_mask):
        def row(v):
            return v.reshape(1, -1)

        powers = (np.float32(ROPE_BASE) ** (np.arange(32, dtype=np.float32) * np.float32(2.0) / np.float32(HD))).astype(np.float32)
        base = jnp.asarray(np.tile(powers, 4)[None, :])
        args = (
            x_first, next_emb, jnp.transpose(k_cache, (0, 2, 3, 1)), jnp.transpose(v_cache, (0, 2, 3, 1)), seq_len,
            row(ln1_gain), row(ln1_bias), w_q, row(b_q), w_k, row(b_k), w_v, row(b_v), w_o, row(b_o), row(ln2_gain), row(ln2_bias),
            jnp.transpose(w_router), w_gate, w_up, w_down, row(long_factor), jnp.transpose(expert_idx, (0, 2, 1)), route_mask, base,
        )
        V = pltpu.VMEM
        scratch = [
            V((S, B, D), BF16), V((1, D), F32), V((1, D), F32), V((D, D), BF16), V((1, D), F32), V((D, 512), BF16), V((1, 512), F32),
            V((D, 512), BF16), V((1, 512), F32), V((2, 512, D), BF16), V((1, D), F32), V((1, D), F32), V((1, D), F32), V((E, D), BF16),
            V((E, D, FS), BF16), V((E, D, FS), BF16), V((E, FS, D), BF16), V((1, 32), F32), V((S, 8, B), jnp.int32),
            V((S, B, 8, E), jnp.int32), V((1, 128), F32), pltpu.SMEM((B,), jnp.int32), V((B, KV, HD, T), BF16), V((B, KV, HD, T), BF16),
            V((B, 8, 512), F32), V((S, B, 512), F32), V((S, B, 512), F32), V((B, 2, 32, T), F32), V((B, 2, 32, T), BF16),
            V((2, 8, 128), F32), V((4, 8, 128), F32), V((2, 2, 8, 8, 256), F32), V((2, 8, 8, 256), F32), V((2, 2, 8, 8, 256), F32),
            V((4, 8, 8, 512), F32), V((6, 8, 512), F32), V((6, 8, 512), F32), V((6, 8, 512), F32), V((2, 2, 6, 8, 256), F32),
            V((NCH, R, CW), F32), V((E, R, 128), F32), V((E, R, 2 * FS), F32), V((R, 512), F32), V((R, 8), F32), V((E, R, FS), BF16), V((NCH, R, CW), F32),
            V((NCH, R, CW), F32), V((NCH, 2, R, CW), F32), V((NCH, R, CW), F32), V((B, S, KV, HD), F32), V((B, S, KV, HD), F32),
            pltpu.SemaphoreType.DMA((NLOCAL,)), pltpu.SemaphoreType.DMA((NSEND,)), pltpu.SemaphoreType.DMA((NRECV,)),
        ]
        anyspec = pl.BlockSpec(memory_space=pl.ANY)
        outs = [((S, B, D), BF16), ((B, S, KV, HD), BF16), ((B, S, KV, HD), BF16)]
        vmem = pl.BlockSpec(memory_space=pltpu.VMEM)
        parts = pl.pallas_call(
            kernel,
            out_shape=tuple(V(*o) for o in outs),
            in_specs=[anyspec] * len(args),
            out_specs=(vmem,) * 3,
            scratch_shapes=scratch,
            compiler_params=pltpu.CompilerParams(collective_id=0, has_side_effects=True, vmem_limit_bytes=60 * 1024 * 1024),
        )(*args)
        return pl.pallas_call(
            write_kernel,
            out_shape=tuple(jax.ShapeDtypeStruct(*o) for o in outs),
            in_specs=[vmem] * 3,
            out_specs=(anyspec,) * 3,
            scratch_shapes=[pltpu.SemaphoreType.DMA((3,))],
            compiler_params=pltpu.CompilerParams(vmem_limit_bytes=1024 * 1024),
        )(*parts)

    replicated = P()
    in_specs = (P('dp'), P(None, 'dp'), P('dp', 'kv'), P('dp', 'kv'), P('dp')) + (replicated,) * 13 + (P(None, None, 'kv'), P(None, None, 'kv'), P(None, 'kv'), replicated, P(None, 'dp'), P(None, 'dp'))
    out_specs = (P(None, 'dp'), P('dp'), P('dp'))
    return jax.shard_map(layer_steps, mesh=mesh, in_specs=in_specs, out_specs=out_specs, check_vma=False)
```

```python
import functools
import itertools
import math

import jax
import jax.numpy as jnp
import numpy as np
from jax import lax
from jax.experimental import pallas as pl
from jax.experimental.pallas import tpu as pltpu
from jax.sharding import PartitionSpec as P

ROPE_BASE = 10000.0
ROPE_MSCALE = math.sqrt(1.0 + math.log(32.0) / math.log(4096.0))
NORM_EPS = 1e-5
NEG_FILL = -1e30
F32 = jnp.float32
BF16 = jnp.bfloat16

S = 3
B = 16
D = 1024
T = 256
KV = 8
HD = 64
E = 32
FS = 128
R = S * B
NCH = 4
CW = D // NCH

GROUPS = 8
SMALL, PARTS = 8, 4
L_SMALL, L_WQ, L_K, L_V, L_WO, L_GU, L_DN, NLOCAL = itertools.accumulate((SMALL, 2, PARTS, PARTS, 1, 2, 2), initial=0)
R_ML, R_O, R_C, R_G, R_P, R_B, NRECV = itertools.accumulate((3, 2, 2, 2, NCH, NCH + 1), initial=0)
S_ML, S_O, S_C, S_G, S_P, S_B, NSEND = range(7)
LN = 128
HALF = 8


def at(i, width=LN):
    return slice(i * width, (i + 1) * width)


def mm(a, b):
    return jnp.dot(a, b, preferred_element_type=F32)


def mm_t(a, b):
    return lax.dot_general(a, b, (((1,), (1,)), ((), ())), preferred_element_type=F32)


def norm_rows(x, gain, bias):
    mean = jnp.mean(x, axis=-1, keepdims=True)
    cen = x - mean
    var = jnp.mean(cen * cen, axis=-1, keepdims=True)
    return (cen * lax.rsqrt(var + NORM_EPS) * gain + bias).astype(BF16)


def lane_iota(shape):
    return lax.broadcasted_iota(jnp.int32, shape, len(shape) - 1)


def kernel(
    x_first, next_emb, k_hbm, v_hbm, seq_hbm, g1_h, b1_h, wq_h, bq_h, wk_h, bk_h, wv_h, bv_h, wo_h, bo_h, g2_h, b2_h,
    wr_h, wg_h, wu_h, wd_h, lf_h, idx_h, rm_h, base_h,
    hb, tkb, tvb,
    xb, g1, b1, wq, bq, wk, bk, wv, bv, wo, bo, g2, b2, wr, wg, wu, wd, lf, idx, rm, base, seq_s, kc, vc,
    qbuf, kbuf, vbuf, sbuf, wbuf, mlb, mlall, obuf, orecv, c2, ex, ga, gb, tl, oall, xm4, gx, raw, qraw, picks, wrt, h2, ub, pb, ab, db, s2, yb, tkf, tvf,
    lsem, ssem, rsem,
):
    me = lax.axis_index("kv")
    core = me % 2
    chip = me // 2
    partner = me + 1 - 2 * core
    peer = (me + 2) % 4
    diag = (partner + 2) % 4

    def local(src, dst, i):
        return pltpu.make_async_copy(src, dst, lsem.at[i])

    def remote(src, dst, snd, rcv, dev):
        return pltpu.make_async_remote_copy(
            src_ref=src, dst_ref=dst, send_sem=ssem.at[snd], recv_sem=rsem.at[rcv],
            device_id={"kv": dev}, device_id_type=pl.DeviceIdType.MESH)

    small = [
        local(src, dst, L_SMALL + i % SMALL) for i, (src, dst) in enumerate((
            (x_first, xb.at[0]), (next_emb, xb.at[pl.ds(1, S - 1)]), (g1_h, g1), (b1_h, b1), (bq_h, bq), (lf_h, lf), (base_h, base),
            (seq_hbm, seq_s), (bk_h, bk), (bv_h, bv), (bo_h, bo), (g2_h, g2), (b2_h, b2), (wr_h, wr), (idx_h, idx), (rm_h, rm)))
    ]
    first, later = small[:SMALL], small[SMALL:]
    cp_wq = [local(wq_h.at[:, pl.ds(i * 512, 512)], wq.at[:, pl.ds(i * 512, 512)], L_WQ + i) for i in range(2)]
    other, own = (1 - core) * 8, core * 8

    def k_part(i):
        sl = pl.ds((other if i < 2 else own) + (i % 2) * 4, 4)
        return local(k_hbm.at[sl], kc.at[sl], L_K + i)

    def v_part(i):
        sl = (pl.ds(other if i < 2 else own, 8), pl.ds((i % 2) * 4, 4))
        return local(v_hbm.at[sl], vc.at[sl], L_V + i)

    cp_k = [k_part(i) for i in range(4)]
    cp_v = [v_part(i) for i in range(4)]
    cp_wkv = [local(wk_h, wk, L_WQ), local(wv_h, wv, L_WQ + 1)]
    cp_wo = [
        local(wo_h.at[pl.ds(kv * 128 + g * 64, 64)], wo.at[g, pl.ds(kv * 64, 64)], L_WO) for kv in range(KV) for g in range(2)
    ]

    def up_copy(src, dst, i, sem):
        sl = pl.ds(i * 4, 4)
        return local(src.at[sl], dst.at[sl], sem)

    def down_copy(m, e, n):
        sl = (pl.ds(e, n), pl.ds(0, FS), pl.ds(m * 2 * CW, 2 * CW))
        return local(wd_h.at[sl], wd.at[sl], L_DN + m)

    for c in first + cp_wq + cp_k:
        c.start()
    bar = pltpu.get_barrier_semaphore()
    for dev in (partner, peer, diag):
        pl.semaphore_signal(bar, inc=1, device_id={"kv": dev}, device_id_type=pl.DeviceIdType.MESH)
    qbuf[:, 6:8, :] = jnp.zeros((B, 2, 512), F32)

    for c in first:
        c.wait()
    for c in cp_v:
        c.start()

    lane48 = lane_iota((R, 128))
    inv = 1.0 / (jnp.concatenate([lf[...]] * 4, axis=1) * base[...])
    row_b = lax.broadcasted_iota(jnp.int32, (B, 128), 0)
    len_rows = jnp.zeros((B, 128), jnp.int32)
    for b in range(B):
        len_rows = jnp.where(row_b == b, seq_s[b], len_rows)
    angles = jnp.concatenate([(len_rows + s).astype(F32) for s in range(S)], axis=0) * inv
    cosv = jnp.cos(angles) * ROPE_MSCALE
    sinv = jnp.sin(angles) * ROPE_MSCALE
    low_half = (lane48 % HD) < (HD // 2)

    def rope(x, both=False):
        xf = x.astype(BF16).astype(F32)
        up, down_ = pltpu.roll(xf, 96, 1), pltpu.roll(xf, 32, 1)
        plain = (xf * cosv + jnp.where(low_half, -up, down_) * sinv).astype(BF16).astype(F32)
        if not both:
            return plain
        return plain, (pltpu.roll(xf, HD, 1) * cosv + jnp.where(low_half, -down_, up) * sinv).astype(BF16).astype(F32)

    h1 = norm_rows(xb[...].reshape(R, D).astype(F32), g1[...], b1[...])

    left = lane48 < HD

    def put_q(q, p):
        qa, qa_x = rope(q[:, :LN], True)
        qb, qb_x = rope(q[:, LN:], True)
        pair = (jnp.where(left, qa, qb_x) * 0.125, jnp.where(left, qa_x, qb) * 0.125)
        for g in range(2):
            for s in range(S):
                qbuf[:, 2 * s + g, at(p)] = pair[g][at(s, B)]

    cp_wq[0].wait()
    q_lo = mm(h1, wq[:, :512]) + bq[:, :512]
    qraw[...] = q_lo
    cp_wq[1].wait()
    for c in later + cp_wo + cp_wkv:
        c.start()
    q_hi = mm(h1, wq[:, 512:]) + bq[:, 512:]
    for p in range(4):
        put_q(qraw[:, p * 256:(p + 1) * 256] if p < 2 else q_hi[:, (p - 2) * 256:(p - 1) * 256], p)

    rowq = lax.broadcasted_iota(jnp.int32, (32, T), 0)
    laneq = lane_iota((32, T))
    diag_mask = (rowq // 8) == (laneq // HD)
    pos = laneq + me * T
    lane8 = lane_iota((8, 128))

    def scores(start, i):
        qv = qbuf[start + i]
        for hh in range(2):
            rep = jnp.concatenate([qv[:, at(hh, T)]] * 4, axis=0)
            lhs = jnp.where(diag_mask, rep, 0.0).astype(BF16)
            sbuf[start + i, hh] = mm(lhs, kc[start + i, at(hh, 4)].reshape(256, T))

    def soft(start, i, acc):
        keep = pos < seq_s[start + i]
        for hh in range(2):
            sc = jnp.where(keep, sbuf[start + i, hh], NEG_FILL)
            m = jnp.max(sc, axis=1, keepdims=True)
            w = jnp.where(keep, jnp.exp(sc - m), 0.0)
            l = jnp.sum(w, axis=1, keepdims=True)
            wbuf[start + i, hh] = w.astype(BF16)
            for j in range(4):
                spot = i * 16 + hh * 4 + j
                acc = jnp.where(lane8 == spot, m[at(j, 8)], acc)
                acc = jnp.where(lane8 == spot + 8, l[at(j, 8)], acc)
        return acc

    left8 = lane8 < HD

    def values(half, i, hh):
        b = half * 8 + i
        pv = mm_t(wbuf[b, hh], vc[b, at(hh, 4)].reshape(256, T))
        obuf[half, hh, i, :, 0:128] = jnp.where(left8, pv[0:8, 0:128], pv[8:16, 0:128])
        obuf[half, hh, i, :, 128:256] = jnp.where(left8, pv[16:24, 128:256], pv[24:32, 128:256])

    send_ml = [
        remote(mlb.at[1 - core], mlall.at[me], S_ML, R_ML, partner), remote(mlb.at[core], mlall.at[me], S_ML, R_ML + 1, peer),
        remote(mlb.at[1 - core], mlall.at[me], S_ML, R_ML + 2, diag),
    ]
    send_o = [remote(obuf.at[1 - core, hh], orecv.at[hh], S_O, R_O + hh, partner) for hh in range(2)]
    zero = jnp.zeros((8, 128), F32)

    cp_k[0].wait()
    for i in range(4):
        scores(other, i)
    cp_k[1].wait()
    for i in range(4):
        scores(other, 4 + i)
    acc = zero
    for i in range(4):
        acc = soft(other, i, acc)
    cp_k[2].wait()
    for i in range(GROUPS):
        up_copy(wg_h, wg, i, L_GU).start()
        up_copy(wu_h, wu, i, L_GU + 1).start()
    for i in range(4):
        scores(own, i)
    for i in range(4):
        acc = soft(other, 4 + i, acc)
    mlb[1 - core] = acc
    pl.semaphore_wait(bar, 3)
    send_ml[0].start()
    send_ml[2].start()

    cp_v[0].wait()
    cp_k[3].wait()
    for i in range(8):
        values(1 - core, i, 0)
    for i in range(4):
        scores(own, 4 + i)
    acc = zero
    for i in range(4):
        acc = soft(own, i, acc)
    send_o[0].start()
    cp_v[1].wait()
    for i in range(GROUPS):
        down_copy(0, i * 4, 4).start()
    for i in range(GROUPS):
        down_copy(1, i * 4, 4).start()
    for i in range(8):
        values(1 - core, i, 1)
    for i in range(4):
        acc = soft(own, 4 + i, acc)
    mlb[core] = acc
    mlall[me] = acc
    send_o[1].start()
    send_ml[1].start()

    pick = (lane8 // HD)

    def spread(v, i, p):
        return jnp.take_along_axis(v, pick + (i * 16 + 2 * p), axis=1, mode="promise_in_bounds")

    send_c = [remote(c2.at[hh, chip, pl.ds(0, 6)], c2.at[hh, chip, pl.ds(0, 6)], S_C, R_C + hh, peer) for hh in range(2)]
    for hh in range(2):
        cp_v[2 + hh].wait()
        for i in range(8):
            values(core, i, hh)
        if hh == 0:
            send_ml[0].wait_recv()
            ml_a = mlall[me]
            ml_b = mlall[partner]
            m_ab = jnp.maximum(ml_a, ml_b)
            f_a = jnp.exp(ml_a - m_ab)
            f_b = jnp.exp(ml_b - m_ab)
        send_o[hh].wait_recv()
        for i in range(8):
            oa = obuf[core, hh, i]
            ob = orecv[hh, i]
            for p in range(2):
                ln = at(p)
                c2[hh, chip, :, i, ln] = (
                    oa[:, ln] * spread(f_a, i, 2 * hh + p) + ob[:, ln] * spread(f_b, i, 2 * hh + p))
        send_c[hh].start()

    for c in later + cp_wkv:
        c.wait()
    kn = mm(h1, wk[...]) + bk[...]
    vn = (mm(h1, wv[...]) + bv[...]).astype(BF16)
    vn = vn.astype(F32)
    for p in range(4):
        ln = at(p)
        for val, buf, fin in ((rope(kn[:, ln]), kbuf, tkf), (vn[:, ln], vbuf, tvf)):
            swap = pltpu.roll(val, 64, 1)
            for s in range(S):
                r = at(s, B)
                buf[s, :, ln] = val[r]
                fin[:, s, 2 * p, :] = val[r, :HD]
                fin[:, s, 2 * p + 1, :] = swap[r, :HD]
    tkb[...] = tkf[...].astype(BF16)
    tvb[...] = tvf[...].astype(BF16)

    rows = pl.ds(pl.multiple_of(core * 8, 8), 8)
    kt = [kbuf[t, rows, :] for t in range(S)]
    vt = [vbuf[t, rows, :] for t in range(S)]
    trip = [(s, g, t) for s in range(S) for g in range(2) for t in range(s + 1)]
    prod = jnp.concatenate([qbuf[rows, 2 * s + g, :] * kt[t] for s, g, t in trip], axis=0)
    hi = prod.astype(BF16)
    lo = (prod - hi.astype(F32)).astype(BF16)
    r2 = lax.broadcasted_iota(jnp.int32, (256, 128), 0)
    ones = jnp.where(((r2 % 128) // HD) == (lane_iota((256, 128)) // HD), 1.0, 0.0).astype(BF16)
    tsc = jnp.concatenate(
        [mm(jnp.concatenate([hi[:, at(p)], lo[:, at(p)]], axis=1), ones) for p in range(4)], axis=1)

    eye = jnp.where(lax.broadcasted_iota(jnp.int32, (B, B), 0) == lane_iota((B, B)), 1.0, 0.0)
    picks[...] = jnp.concatenate([mm_t(eye, idx[s].astype(F32)) for s in range(S)], axis=0)

    eye_e = jnp.where(lax.broadcasted_iota(jnp.int32, (E, E), 0) == lane_iota((E, E)), 1.0, 0.0).astype(BF16)
    wrt[...] = lax.dot_general(wr[...], eye_e, (((0,), (0,)), ((), ())), preferred_element_type=F32).astype(BF16)

    for c in send_ml[1:]:
        c.wait_recv()
    ml = [mlall[d] for d in range(4)]
    for ch in range(2):
        a, b_ = ml[2 * ch], ml[2 * ch + 1]
        mc = jnp.maximum(a, b_)
        lc = (pltpu.roll(a, 120, 1) * jnp.exp(a - mc) + pltpu.roll(b_, 120, 1) * jnp.exp(b_ - mc))
        for i in range(8):
            for p in range(4):
                ln = at(p)
                ex[2 * ch, :, i, ln] = spread(mc, i, p)
                ex[2 * ch + 1, :, i, ln] = spread(lc, i, p)

    for s in range(S):
        for g in range(2):
            j = 2 * s + g
            sc = [tsc[at(n, 8)] for n, key in enumerate(trip) if key[:2] == (s, g)]
            mt = functools.reduce(jnp.maximum, sc)
            wt = [jnp.exp(v - mt) for v in sc]
            lt = functools.reduce(jnp.add, wt)
            ot = functools.reduce(jnp.add, [w.astype(BF16).astype(F32) * v for w, v in zip(wt, vt)])
            m0, l0, m1, l1 = ex[0, j], ex[1, j], ex[2, j], ex[3, j]
            top = jnp.maximum(jnp.maximum(m0, m1), mt)
            f0, f1, ft = jnp.exp(m0 - top), jnp.exp(m1 - top), jnp.exp(mt - top)
            inv_l = 1.0 / (l0 * f0 + l1 * f1 + lt * ft)
            ga[j] = f0 * inv_l
            gb[j] = f1 * inv_l
            tl[j] = ot * (ft * inv_l)

    send_g = [remote(oall.at[core, hh], oall.at[core, hh], S_G, R_G + hh, partner) for hh in range(2)]
    for hh in range(2):
        send_c[hh].wait_recv()
        ln = at(hh, T)
        for j in range(6):
            oall[core, hh, j] = c2[hh, 0, j] * ga[j][:, ln] + c2[hh, 1, j] * gb[j][:, ln] + tl[j][:, ln]
        send_g[hh].start()

    here = me < 4

    @pl.when(here)
    def _():
        local(wo, wo, L_WO).wait()
        att = None
        for hh in range(2):
            send_g[hh].wait_recv()
            for g in range(2):
                o_g = jnp.concatenate([oall[h, hh, 2 * s + g] for s in range(S) for h in range(2)], axis=0).astype(BF16)
                part = mm(o_g, wo[g, at(hh, T)])
                att = part if att is None else att + part
        xm = (xb[...].reshape(R, D).astype(F32) + att + bo[...]).astype(BF16).astype(F32)
        for n in range(NCH):
            xm4[n] = xm[:, at(n, CW)]
        h2[...] = norm_rows(xm, g2[...], b2[...])

    def act(i):
        for n in range(4):
            e = i * 4 + n
            raw[e] = mm(h2[...], jnp.concatenate([wg[e], wu[e]], axis=1))

    def mix(i):
        for n in range(4):
            e = i * 4 + n
            a, up = raw[e, :, :FS], raw[e, :, FS:]
            ub[e] = (gx[e] * (a * (1.0 / (1.0 + jnp.exp(-a)))) * up).astype(BF16)

    local(wg, wg, L_GU).wait()
    local(wu, wu, L_GU + 1).wait()

    @pl.when(here)
    def _():
        logits = mm(h2[...], wrt[...])
        for i in range(4):
            act(i)
        lane_e = lane_iota((R, E)).astype(F32)
        chosen = picks[...]
        gates = jnp.zeros((R, E), F32)
        for k in range(8):
            on = jnp.concatenate([rm[s, :, k, :] for s in range(S)], axis=0) == 1
            mk = jnp.where(on, logits, NEG_FILL)
            pk = jnp.exp(mk - jnp.max(mk, axis=1, keepdims=True))
            pk = pk / jnp.sum(pk, axis=1, keepdims=True)
            gates = gates + jnp.where(chosen[:, k:k + 1] == lane_e, pk, 0.0)
        for e in range(E):
            gx[e] = jnp.broadcast_to(gates[:, e:e + 1], (R, 128))

        act(4)

    def down(m):
        u = jnp.concatenate([ub[e] for e in range(E)], axis=1)
        part = mm(u, wd[:, :, at(m, 2 * CW)].reshape(E * FS, 2 * CW)).astype(BF16).astype(F32)
        pb[2 * m] = part[:, :CW]
        pb[2 * m + 1] = part[:, CW:]

    send_a = [remote(pb.at[n], ab.at[n], S_P, R_P + n, partner) for n in range(NCH)]
    send_b = [remote(s2.at[n, chip], s2.at[n, chip], S_B, R_B + n, peer) for n in range(NCH)]
    send_d = [remote(pb.at[0], db.at[0], S_B, R_B + NCH, diag), remote(pb.at[0], db.at[1], S_B, R_B, peer)]
    send_y = [remote(yb.at[n], yb.at[n], S_P, R_P + n, partner) for n in range(NCH)]

    for m in range(2):
        down_copy(m, 0, E).wait()

        @pl.when(here)
        def _():
            if m == 0:
                for i in range(5, 8):
                    act(i)
                    mix(i - 5)
                for i in range(3, 8):
                    mix(i)
            down(m)

        @pl.when(core == 0)
        def _():
            for n in (2 * m, 2 * m + 1):
                send_a[n].start()
            if m == 0:
                send_d[0].start()

        if m == 0:
            @pl.when(core == 1)
            def _():
                send_d[1].start()

    @pl.when(core == 1)
    def _():
        for n in range(NCH):
            send_a[n].wait_recv()
            s2[n, chip] = ab[n] + pb[n]
            if n > 0:
                send_b[n].start()
        for c in send_d:
            c.wait_recv()
        s2[0, 1 - chip] = db[0] + db[1]
        for n in range(NCH):
            if n > 0:
                send_b[n].wait_recv()
            yb[n] = xm4[n] + (s2[n, 0] + s2[n, 1])
            send_y[n].start()
            hb[:, :, at(n, CW)] = yb[n].astype(BF16).reshape(S, B, CW)
        remote(s2.at[:, chip], s2.at[:, chip], S_B, R_B, peer).wait_send()

    @pl.when(core == 0)
    def _():
        send_d[0].wait_send()
        for n in range(NCH):
            send_y[n].wait_recv()
            hb[:, :, at(n, CW)] = yb[n].astype(BF16).reshape(S, B, CW)

    for ref, snd in ((mlall.at[pl.ds(0, 3)], S_ML), (obuf.at[1 - core], S_O), (c2.at[:, chip, pl.ds(0, 6)], S_C), (oall.at[core], S_G), (pb, S_P)):
        remote(ref, ref, snd, R_ML, partner).wait_send()


def write_kernel(h, tk, tv, h_out, tk_out, tv_out, sem):
    copies = [pltpu.make_async_copy(a, b, sem.at[i]) for i, (a, b) in enumerate(((h, h_out), (tk, tk_out), (tv, tv_out)))]
    for c in copies:
        c.start()
    for c in copies:
        c.wait()


def solution(mesh):
    def layer_steps(x_first, next_emb, k_cache, v_cache, seq_len, ln1_gain, ln1_bias, w_q, b_q, w_k, b_k, w_v, b_v, w_o, b_o, ln2_gain, ln2_bias, w_router, w_gate, w_up, w_down, long_factor, expert_idx, route_mask):
        def row(v):
            return v.reshape(1, -1)

        powers = (np.float32(ROPE_BASE) ** (np.arange(32, dtype=np.float32) * np.float32(2.0) / np.float32(HD))).astype(np.float32)
        base = jnp.asarray(np.tile(powers, 4)[None, :])
        args = (
            x_first, next_emb, jnp.transpose(k_cache, (0, 2, 3, 1)), jnp.transpose(v_cache, (0, 2, 3, 1)), seq_len,
            row(ln1_gain), row(ln1_bias), w_q, row(b_q), w_k, row(b_k), w_v, row(b_v), w_o, row(b_o), row(ln2_gain), row(ln2_bias),
            jnp.transpose(w_router), w_gate, w_up, w_down, row(long_factor), jnp.transpose(expert_idx, (0, 2, 1)), route_mask, base,
        )
        V = pltpu.VMEM
        scratch = [
            V((S, B, D), BF16), V((1, D), F32), V((1, D), F32), V((D, D), BF16), V((1, D), F32), V((D, 512), BF16), V((1, 512), F32),
            V((D, 512), BF16), V((1, 512), F32), V((2, 512, D), BF16), V((1, D), F32), V((1, D), F32), V((1, D), F32), V((E, D), BF16),
            V((E, D, FS), BF16), V((E, D, FS), BF16), V((E, FS, D), BF16), V((1, 32), F32), V((S, 8, B), jnp.int32),
            V((S, B, 8, E), jnp.int32), V((1, 128), F32), pltpu.SMEM((B,), jnp.int32), V((B, KV, HD, T), BF16), V((B, KV, HD, T), BF16),
            V((B, 8, 512), F32), V((S, B, 512), F32), V((S, B, 512), F32), V((B, 2, 32, T), F32), V((B, 2, 32, T), BF16),
            V((2, 8, 128), F32), V((4, 8, 128), F32), V((2, 2, 8, 8, 256), F32), V((2, 8, 8, 256), F32), V((2, 2, 8, 8, 256), F32),
            V((4, 8, 8, 512), F32), V((6, 8, 512), F32), V((6, 8, 512), F32), V((6, 8, 512), F32), V((2, 2, 6, 8, 256), F32),
            V((NCH, R, CW), F32), V((E, R, 128), F32), V((E, R, 2 * FS), F32), V((R, 512), F32), V((R, 8), F32), V((D, E), BF16), V((R, D), BF16), V((E, R, FS), BF16), V((NCH, R, CW), F32),
            V((NCH, R, CW), F32), V((2, R, CW), F32), V((NCH, 2, R, CW), F32), V((NCH, R, CW), F32), V((B, S, KV, HD), F32), V((B, S, KV, HD), F32),
            pltpu.SemaphoreType.DMA((NLOCAL,)), pltpu.SemaphoreType.DMA((NSEND,)), pltpu.SemaphoreType.DMA((NRECV,)),
        ]
        anyspec = pl.BlockSpec(memory_space=pl.ANY)
        outs = [((S, B, D), BF16), ((B, S, KV, HD), BF16), ((B, S, KV, HD), BF16)]
        vmem = pl.BlockSpec(memory_space=pltpu.VMEM)
        parts = pl.pallas_call(
            kernel,
            out_shape=tuple(V(*o) for o in outs),
            in_specs=[anyspec] * len(args),
            out_specs=(vmem,) * 3,
            scratch_shapes=scratch,
            compiler_params=pltpu.CompilerParams(collective_id=0, has_side_effects=True, vmem_limit_bytes=60 * 1024 * 1024),
        )(*args)
        return pl.pallas_call(
            write_kernel,
            out_shape=tuple(jax.ShapeDtypeStruct(*o) for o in outs),
            in_specs=[vmem] * 3,
            out_specs=(anyspec,) * 3,
            scratch_shapes=[pltpu.SemaphoreType.DMA((3,))],
            compiler_params=pltpu.CompilerParams(vmem_limit_bytes=1024 * 1024),
        )(*parts)

    replicated = P()
    in_specs = (P('dp'), P(None, 'dp'), P('dp', 'kv'), P('dp', 'kv'), P('dp')) + (replicated,) * 13 + (P(None, None, 'kv'), P(None, None, 'kv'), P(None, 'kv'), replicated, P(None, 'dp'), P(None, 'dp'))
    out_specs = (P(None, 'dp'), P('dp'), P('dp'))
    return jax.shard_map(layer_steps, mesh=mesh, in_specs=in_specs, out_specs=out_specs, check_vma=False)
```

```python
import functools
import itertools
import math

import jax
import jax.numpy as jnp
import numpy as np
from jax import lax
from jax.experimental import pallas as pl
from jax.experimental.pallas import tpu as pltpu
from jax.sharding import PartitionSpec as P

ROPE_BASE = 10000.0
ROPE_MSCALE = math.sqrt(1.0 + math.log(32.0) / math.log(4096.0))
NORM_EPS = 1e-5
NEG_FILL = -1e30
F32 = jnp.float32
BF16 = jnp.bfloat16

S = 3
B = 16
D = 1024
T = 256
KV = 8
HD = 64
E = 32
FS = 128
R = S * B
NCH = 4
CW = D // NCH

GROUPS = 8
SMALL, PARTS = 8, 4
L_SMALL, L_WQ, L_K, L_V, L_WO, L_GU, L_DN, NLOCAL = itertools.accumulate((SMALL, 2, PARTS, PARTS, 1, PARTS, 2), initial=0)
R_ML, R_O, R_C, R_G, R_P, R_B, NRECV = itertools.accumulate((3, 2, 2, 2, NCH, NCH + 1), initial=0)
S_ML, S_O, S_C, S_G, S_P, S_B, NSEND = range(7)
LN = 128
TWO, FOUR, EIGHT = range(2), range(4), range(8)


def at(i, width=LN):
    return slice(i * width, (i + 1) * width)


def mm(a, b):
    return jnp.dot(a, b, preferred_element_type=F32)


def mm_t(a, b):
    return lax.dot_general(a, b, (((1,), (1,)), ((), ())), preferred_element_type=F32)


def norm_rows(x, gain, bias):
    mean = jnp.mean(x, axis=-1, keepdims=True)
    cen = x - mean
    var = jnp.mean(cen * cen, axis=-1, keepdims=True)
    return (cen * lax.rsqrt(var + NORM_EPS) * gain + bias).astype(BF16)


def lane_iota(shape):
    return lax.broadcasted_iota(jnp.int32, shape, len(shape) - 1)


def kernel(
    x_first, next_emb, k_hbm, v_hbm, seq_hbm, g1_h, b1_h, wq_h, bq_h, wk_h, bk_h, wv_h, bv_h, wo_h, bo_h, g2_h, b2_h,
    wr_h, wg_h, wu_h, wd_h, lf_h, idx_h, rm_h, base_h,
    hb, tkb, tvb,
    xb, g1, b1, wq, bq, wk, bk, wv, bv, wo, bo, g2, b2, wr, wg, wu, wd, lf, idx, rm, base, seq_s, kc, vc,
    qbuf, kbuf, vbuf, sbuf, wbuf, mlb, mlall, obuf, orecv, c2, ex, ga, gb, tl, oall, xm4, gx, raw, qraw, dsum, picks, wrt, h2, ub, pb, ab, db, s2, yb, tkf, tvf,
    lsem, ssem, rsem,
):
    me = lax.axis_index("kv")
    core = me % 2
    chip = me // 2
    partner = me + 1 - 2 * core
    peer = (me + 2) % 4
    diag = (partner + 2) % 4

    def local(src, dst, i):
        return pltpu.make_async_copy(src, dst, lsem.at[i])

    def remote(src, dst, snd, rcv, dev):
        return pltpu.make_async_remote_copy(
            src_ref=src, dst_ref=dst, send_sem=ssem.at[snd], recv_sem=rsem.at[rcv],
            device_id={"kv": dev}, device_id_type=pl.DeviceIdType.MESH)

    small = [
        local(src, dst, L_SMALL + i % SMALL) for i, (src, dst) in enumerate((
            (x_first, xb.at[0]), (next_emb, xb.at[pl.ds(1, S - 1)]), (g1_h, g1), (b1_h, b1), (bq_h, bq), (lf_h, lf), (base_h, base),
            (seq_hbm, seq_s), (bk_h, bk), (bv_h, bv), (bo_h, bo), (g2_h, g2), (b2_h, b2), (wr_h, wr), (idx_h, idx), (rm_h, rm)))
    ]
    first, later = small[:SMALL], small[SMALL:]
    cp_wq = [local(wq_h.at[:, pl.ds(i * 512, 512)], wq.at[:, pl.ds(i * 512, 512)], L_WQ + i) for i in TWO]
    other, own = (1 - core) * 8, core * 8

    def k_part(i):
        sl = pl.ds((other if i < 2 else own) + (i % 2) * 4, 4)
        return local(k_hbm.at[sl], kc.at[sl], L_K + i)

    def v_part(i):
        sl = (pl.ds(other if i < 2 else own, 8), pl.ds((i % 2) * 4, 4))
        return local(v_hbm.at[sl], vc.at[sl], L_V + i)

    cp_k = [k_part(i) for i in FOUR]
    cp_v = [v_part(i) for i in FOUR]
    cp_wkv = [local(wk_h, wk, L_WQ), local(wv_h, wv, L_WQ + 1)]
    cp_wo = [
        local(wo_h.at[pl.ds(kv * 128 + g * 64, 64)], wo.at[g, pl.ds(kv * 64, 64)], L_WO) for kv in range(KV) for g in TWO
    ]

    def up_copy(src, dst, i, sem):
        sl = pl.ds(i * 4, 4)
        return local(src.at[sl], dst.at[sl], sem)

    def down_copy(m, e, n):
        sl = (pl.ds(e, n), pl.ds(0, FS), pl.ds(m * 2 * CW, 2 * CW))
        return local(wd_h.at[sl], wd.at[sl], L_DN + m)

    for c in first + cp_wq + cp_k[:3] + cp_v[:1] + cp_k[3:]:
        c.start()
    bar = pltpu.get_barrier_semaphore()
    for dev in (partner, peer, diag):
        pl.semaphore_signal(bar, inc=1, device_id={"kv": dev}, device_id_type=pl.DeviceIdType.MESH)
    qbuf[:, 6:8, :] = jnp.zeros((B, 2, 512), F32)

    for c in first:
        c.wait()
    for c in cp_v[1:]:
        c.start()

    lane48 = lane_iota((R, 128))
    inv = 1.0 / (jnp.concatenate([lf[...]] * 4, axis=1) * base[...])
    row_b = lax.broadcasted_iota(jnp.int32, (B, 128), 0)
    len_rows = jnp.zeros((B, 128), jnp.int32)
    for b in range(B):
        len_rows = jnp.where(row_b == b, seq_s[b], len_rows)
    angles = jnp.concatenate([(len_rows + s).astype(F32) for s in range(S)], axis=0) * inv
    cosv = jnp.cos(angles) * ROPE_MSCALE
    sinv = jnp.sin(angles) * ROPE_MSCALE
    low_half = (lane48 % HD) < (HD // 2)

    def rope(x, both=False):
        xf = x.astype(BF16).astype(F32)
        up, down_ = pltpu.roll(xf, 96, 1), pltpu.roll(xf, 32, 1)
        plain = (xf * cosv + jnp.where(low_half, -up, down_) * sinv).astype(BF16).astype(F32)
        if not both:
            return plain
        return plain, (pltpu.roll(xf, HD, 1) * cosv + jnp.where(low_half, -down_, up) * sinv).astype(BF16).astype(F32)

    h1 = norm_rows(xb[...].reshape(R, D).astype(F32), g1[...], b1[...])

    left = lane48 < HD

    def put_q(q, p):
        qa, qa_x = rope(q[:, :LN], True)
        qb, qb_x = rope(q[:, LN:], True)
        pair = (jnp.where(left, qa, qb_x) * 0.125, jnp.where(left, qa_x, qb) * 0.125)
        for g in TWO:
            for s in range(S):
                qbuf[:, 2 * s + g, at(p)] = pair[g][at(s, B)]

    cp_wq[0].wait()
    q_lo = mm(h1, wq[:, :512]) + bq[:, :512]
    qraw[...] = q_lo
    cp_wq[1].wait()
    for c in later + cp_wo + cp_wkv:
        c.start()
    q_hi = mm(h1, wq[:, 512:]) + bq[:, 512:]
    for p in FOUR:
        put_q(qraw[:, p * 256:(p + 1) * 256] if p < 2 else q_hi[:, (p - 2) * 256:(p - 1) * 256], p)

    rowq = lax.broadcasted_iota(jnp.int32, (32, T), 0)
    laneq = lane_iota((32, T))
    diag_mask = (rowq // 8) == (laneq // HD)
    pos = laneq + me * T
    lane8 = lane_iota((8, 128))

    def scores(start, i):
        qv = qbuf[start + i]
        for hh in TWO:
            rep = jnp.concatenate([qv[:, at(hh, T)]] * 4, axis=0)
            lhs = jnp.where(diag_mask, rep, 0.0).astype(BF16)
            sbuf[start + i, hh] = mm(lhs, kc[start + i, at(hh, 4)].reshape(256, T))

    def soft(start, i, acc):
        keep = pos < seq_s[start + i]
        for hh in TWO:
            sc = jnp.where(keep, sbuf[start + i, hh], NEG_FILL)
            m = jnp.max(sc, axis=1, keepdims=True)
            w = jnp.where(keep, jnp.exp(sc - m), 0.0)
            l = jnp.sum(w, axis=1, keepdims=True)
            wbuf[start + i, hh] = w.astype(BF16)
            for j in FOUR:
                spot = i * 16 + hh * 4 + j
                acc = jnp.where(lane8 == spot, m[at(j, 8)], acc)
                acc = jnp.where(lane8 == spot + 8, l[at(j, 8)], acc)
        return acc

    left8 = lane8 < HD

    def values(half, i, hh):
        b = half * 8 + i
        pv = mm_t(wbuf[b, hh], vc[b, at(hh, 4)].reshape(256, T))
        obuf[half, hh, i, :, 0:128] = jnp.where(left8, pv[0:8, 0:128], pv[8:16, 0:128])
        obuf[half, hh, i, :, 128:256] = jnp.where(left8, pv[16:24, 128:256], pv[24:32, 128:256])

    send_ml = [
        remote(mlb.at[1 - core], mlall.at[me], S_ML, R_ML, partner), remote(mlb.at[core], mlall.at[me], S_ML, R_ML + 1, peer),
        remote(mlb.at[1 - core], mlall.at[me], S_ML, R_ML + 2, diag),
    ]
    send_o = [remote(obuf.at[1 - core, hh], orecv.at[hh], S_O, R_O + hh, partner) for hh in TWO]
    zero = jnp.zeros((8, 128), F32)

    cp_k[0].wait()
    for i in FOUR:
        scores(other, i)
    cp_k[1].wait()
    for i in FOUR:
        scores(other, 4 + i)
    acc = zero
    for i in FOUR:
        acc = soft(other, i, acc)
    cp_k[2].wait()
    for i in range(GROUPS):
        sem = L_GU + 2 * (i // 5)
        up_copy(wg_h, wg, i, sem).start()
        up_copy(wu_h, wu, i, sem + 1).start()
    for i in FOUR:
        scores(own, i)
    for i in FOUR:
        acc = soft(other, 4 + i, acc)
    mlb[1 - core] = acc
    pl.semaphore_wait(bar, 3)
    send_ml[0].start()
    send_ml[2].start()

    cp_v[0].wait()
    for i in EIGHT:
        values(1 - core, i, 0)
    acc = zero
    for i in FOUR:
        acc = soft(own, i, acc)
    send_o[0].start()
    cp_v[1].wait()
    cp_k[3].wait()
    for i in range(GROUPS):
        down_copy(0, i * 4, 4).start()
    for i in range(GROUPS):
        down_copy(1, i * 4, 4).start()
    for i in EIGHT:
        values(1 - core, i, 1)
    for i in FOUR:
        scores(own, 4 + i)
    send_o[1].start()
    cp_v[2].wait()
    for i in FOUR:
        acc = soft(own, 4 + i, acc)
    mlb[core] = acc
    mlall[me] = acc
    for i in EIGHT:
        values(core, i, 0)
    send_ml[1].start()

    pick = (lane8 // HD)

    def spread(v, i, p):
        return jnp.take_along_axis(v, pick + (i * 16 + 2 * p), axis=1, mode="promise_in_bounds")

    send_c = [remote(c2.at[hh, chip, pl.ds(0, 6)], c2.at[hh, chip, pl.ds(0, 6)], S_C, R_C + hh, peer) for hh in TWO]
    for hh in TWO:
        if hh == 1:
            cp_v[3].wait()
            for i in EIGHT:
                values(core, i, 1)
        else:
            send_ml[0].wait_recv()
            ml_a = mlall[me]
            ml_b = mlall[partner]
            m_ab = jnp.maximum(ml_a, ml_b)
            f_a = jnp.exp(ml_a - m_ab)
            f_b = jnp.exp(ml_b - m_ab)
        send_o[hh].wait_recv()
        for i in EIGHT:
            oa = obuf[core, hh, i]
            ob = orecv[hh, i]
            for p in TWO:
                ln = at(p)
                c2[hh, chip, :, i, ln] = (
                    oa[:, ln] * spread(f_a, i, 2 * hh + p) + ob[:, ln] * spread(f_b, i, 2 * hh + p))
        send_c[hh].start()

    for c in later + cp_wkv:
        c.wait()
    kn = mm(h1, wk[...]) + bk[...]
    vn = (mm(h1, wv[...]) + bv[...]).astype(BF16)
    vn = vn.astype(F32)
    for p in FOUR:
        ln = at(p)
        for val, buf, fin in ((rope(kn[:, ln]), kbuf, tkf), (vn[:, ln], vbuf, tvf)):
            swap = pltpu.roll(val, 64, 1)
            for s in range(S):
                r = at(s, B)
                buf[s, :, ln] = val[r]
                fin[:, s, 2 * p, :] = val[r, :HD]
                fin[:, s, 2 * p + 1, :] = swap[r, :HD]
    tkb[...] = tkf[...].astype(BF16)
    tvb[...] = tvf[...].astype(BF16)

    rows = pl.ds(pl.multiple_of(core * 8, 8), 8)
    kt = [kbuf[t, rows, :] for t in range(S)]
    vt = [vbuf[t, rows, :] for t in range(S)]
    trip = [(s, g, t) for s in range(S) for g in TWO for t in range(s + 1)]
    prod = jnp.concatenate([qbuf[rows, 2 * s + g, :] * kt[t] for s, g, t in trip], axis=0)
    hi = prod.astype(BF16)
    lo = (prod - hi.astype(F32)).astype(BF16)
    r2 = lax.broadcasted_iota(jnp.int32, (256, 128), 0)
    ones = jnp.where(((r2 % 128) // HD) == (lane_iota((256, 128)) // HD), 1.0, 0.0).astype(BF16)
    tsc = jnp.concatenate(
        [mm(jnp.concatenate([hi[:, at(p)], lo[:, at(p)]], axis=1), ones) for p in FOUR], axis=1)

    eye = jnp.where(lax.broadcasted_iota(jnp.int32, (B, B), 0) == lane_iota((B, B)), 1.0, 0.0)
    picks[...] = jnp.concatenate([mm_t(eye, idx[s].astype(F32)) for s in range(S)], axis=0)

    eye_e = jnp.where(lax.broadcasted_iota(jnp.int32, (E, E), 0) == lane_iota((E, E)), 1.0, 0.0).astype(BF16)
    wrt[...] = lax.dot_general(wr[...], eye_e, (((0,), (0,)), ((), ())), preferred_element_type=F32).astype(BF16)

    for c in send_ml[1:]:
        c.wait_recv()
    ml = [mlall[d] for d in FOUR]
    for ch in TWO:
        a, b_ = ml[2 * ch], ml[2 * ch + 1]
        mc = jnp.maximum(a, b_)
        lc = (pltpu.roll(a, 120, 1) * jnp.exp(a - mc) + pltpu.roll(b_, 120, 1) * jnp.exp(b_ - mc))
        for i in EIGHT:
            for p in FOUR:
                ln = at(p)
                ex[2 * ch, :, i, ln] = spread(mc, i, p)
                ex[2 * ch + 1, :, i, ln] = spread(lc, i, p)

    for s in range(S):
        for g in TWO:
            j = 2 * s + g
            sc = [tsc[at(n, 8)] for n, key in enumerate(trip) if key[:2] == (s, g)]
            mt = functools.reduce(jnp.maximum, sc)
            wt = [jnp.exp(v - mt) for v in sc]
            lt = functools.reduce(jnp.add, wt)
            ot = functools.reduce(jnp.add, [w.astype(BF16).astype(F32) * v for w, v in zip(wt, vt)])
            m0, l0, m1, l1 = ex[0, j], ex[1, j], ex[2, j], ex[3, j]
            top = jnp.maximum(jnp.maximum(m0, m1), mt)
            f0, f1, ft = jnp.exp(m0 - top), jnp.exp(m1 - top), jnp.exp(mt - top)
            inv_l = 1.0 / (l0 * f0 + l1 * f1 + lt * ft)
            ga[j] = f0 * inv_l
            gb[j] = f1 * inv_l
            tl[j] = ot * (ft * inv_l)

    send_g = [remote(oall.at[core, hh], oall.at[core, hh], S_G, R_G + hh, partner) for hh in TWO]
    for hh in TWO:
        send_c[hh].wait_recv()
        ln = at(hh, T)
        for j in range(6):
            oall[core, hh, j] = c2[hh, 0, j] * ga[j][:, ln] + c2[hh, 1, j] * gb[j][:, ln] + tl[j][:, ln]
        send_g[hh].start()

    here = me < 4

    @pl.when(here)
    def _():
        local(wo, wo, L_WO).wait()
        att = None
        for hh in TWO:
            send_g[hh].wait_recv()
            for g in TWO:
                o_g = jnp.concatenate([oall[h, hh, 2 * s + g] for s in range(S) for h in TWO], axis=0).astype(BF16)
                part = mm(o_g, wo[g, at(hh, T)])
                att = part if att is None else att + part
        xm = (xb[...].reshape(R, D).astype(F32) + att + bo[...]).astype(BF16).astype(F32)
        for n in range(NCH):
            xm4[n] = xm[:, at(n, CW)]
        h2[...] = norm_rows(xm, g2[...], b2[...])

    def act(i):
        for n in FOUR:
            e = i * 4 + n
            raw[e] = mm(h2[...], jnp.concatenate([wg[e], wu[e]], axis=1))

    def mix(i):
        for n in FOUR:
            e = i * 4 + n
            a, up = raw[e, :, :FS], raw[e, :, FS:]
            ub[e] = (gx[e] * (a * (1.0 / (1.0 + jnp.exp(-a)))) * up).astype(BF16)

    def wait_up(sl, sem):
        for n, w in enumerate((wg, wu)):
            local(w.at[sl], w.at[sl], sem + n).wait()

    wait_up(pl.ds(0, 20), L_GU)

    @pl.when(here)
    def _():
        logits = mm(h2[...], wrt[...])
        for i in FOUR:
            act(i)
        lane_e = lane_iota((R, E)).astype(F32)
        chosen = picks[...]
        gates = jnp.zeros((R, E), F32)
        for k in EIGHT:
            on = jnp.concatenate([rm[s, :, k, :] for s in range(S)], axis=0) == 1
            mk = jnp.where(on, logits, NEG_FILL)
            pk = jnp.exp(mk - jnp.max(mk, axis=1, keepdims=True))
            pk = pk / jnp.sum(pk, axis=1, keepdims=True)
            gates = gates + jnp.where(chosen[:, k:k + 1] == lane_e, pk, 0.0)
        for e in range(E):
            gx[e] = jnp.broadcast_to(gates[:, e:e + 1], (R, 128))

        act(4)

    def down(n, first, count, width):
        u = jnp.concatenate([ub[e] for e in range(first, first + count)], axis=1)
        return mm(u, wd[first:first + count, :, n * CW:n * CW + width].reshape(count * FS, width))

    def rounded(x):
        return x.astype(BF16).astype(F32)

    send_a = [remote(pb.at[n], ab.at[n], S_P, R_P + n, partner) for n in range(NCH)]
    send_b = [remote(s2.at[n, chip], s2.at[n, chip], S_B, R_B + n, peer) for n in range(NCH)]
    send_d = [remote(pb.at[0], db.at[0], S_B, R_B + NCH, diag), remote(pb.at[0], db.at[1], S_B, R_B, peer)]
    send_y = [remote(yb.at[n], yb.at[n], S_P, R_P + n, partner) for n in range(NCH)]

    wait_up(pl.ds(20, 12), L_GU + 2)
    for m in range(3):
        if m < 2:
            down_copy(m, 0, E).wait()

        @pl.when(here)
        def _():
            if m == 0:
                for i in range(5, 8):
                    act(i)
                    mix(i - 5)
                for i in range(3, 8):
                    mix(i)
                part = rounded(down(0, 0, E, 2 * CW))
                pb[0] = part[:, :CW]
                pb[1] = part[:, CW:]
            else:
                for h in TWO:
                    dsum[h] = down(m + 1, h * (E // 2), E // 2, CW)
                pb[m + 1] = rounded(dsum[0] + dsum[1])

        @pl.when(core == 0)
        def _():
            for n in ((0, 1) if m == 0 else (m + 1,)):
                send_a[n].start()
            if m == 0:
                send_d[0].start()

        if m == 0:
            @pl.when(core == 1)
            def _():
                send_d[1].start()

    @pl.when(core == 1)
    def _():
        for n in range(NCH):
            send_a[n].wait_recv()
            s2[n, chip] = ab[n] + pb[n]
            if n > 0:
                send_b[n].start()
        for c in send_d:
            c.wait_recv()
        s2[0, 1 - chip] = db[0] + db[1]
        for n in range(NCH):
            if n > 0:
                send_b[n].wait_recv()
            yb[n] = xm4[n] + (s2[n, 0] + s2[n, 1])
            send_y[n].start()
            hb[:, :, at(n, CW)] = yb[n].astype(BF16).reshape(S, B, CW)
        remote(s2.at[:, chip], s2.at[:, chip], S_B, R_B, peer).wait_send()

    @pl.when(core == 0)
    def _():
        send_d[0].wait_send()
        for n in range(NCH):
            send_y[n].wait_recv()
            hb[:, :, at(n, CW)] = yb[n].astype(BF16).reshape(S, B, CW)

    for ref, snd in ((mlall.at[pl.ds(0, 3)], S_ML), (obuf.at[1 - core], S_O), (c2.at[:, chip, pl.ds(0, 6)], S_C), (oall.at[core], S_G), (pb, S_P)):
        remote(ref, ref, snd, R_ML, partner).wait_send()


def write_kernel(h, tk, tv, h_out, tk_out, tv_out, sem):
    copies = [pltpu.make_async_copy(a, b, sem.at[i]) for i, (a, b) in enumerate(((h, h_out), (tk, tk_out), (tv, tv_out)))]
    for c in copies:
        c.start()
    for c in copies:
        c.wait()


def solution(mesh):
    def layer_steps(x_first, next_emb, k_cache, v_cache, seq_len, ln1_gain, ln1_bias, w_q, b_q, w_k, b_k, w_v, b_v, w_o, b_o, ln2_gain, ln2_bias, w_router, w_gate, w_up, w_down, long_factor, expert_idx, route_mask):
        def row(v):
            return v.reshape(1, -1)

        powers = (np.float32(ROPE_BASE) ** (np.arange(32, dtype=np.float32) * np.float32(2.0) / np.float32(HD))).astype(np.float32)
        base = jnp.asarray(np.tile(powers, 4)[None, :])
        args = (
            x_first, next_emb, jnp.transpose(k_cache, (0, 2, 3, 1)), jnp.transpose(v_cache, (0, 2, 3, 1)), seq_len,
            row(ln1_gain), row(ln1_bias), w_q, row(b_q), w_k, row(b_k), w_v, row(b_v), w_o, row(b_o), row(ln2_gain), row(ln2_bias),
            jnp.transpose(w_router), w_gate, w_up, w_down, row(long_factor), jnp.transpose(expert_idx, (0, 2, 1)), route_mask, base,
        )
        V = pltpu.VMEM
        scratch = [
            V((S, B, D), BF16), V((1, D), F32), V((1, D), F32), V((D, D), BF16), V((1, D), F32), V((D, 512), BF16), V((1, 512), F32),
            V((D, 512), BF16), V((1, 512), F32), V((2, 512, D), BF16), V((1, D), F32), V((1, D), F32), V((1, D), F32), V((E, D), BF16),
            V((E, D, FS), BF16), V((E, D, FS), BF16), V((E, FS, D), BF16), V((1, 32), F32), V((S, 8, B), jnp.int32),
            V((S, B, 8, E), jnp.int32), V((1, 128), F32), pltpu.SMEM((B,), jnp.int32), V((B, KV, HD, T), BF16), V((B, KV, HD, T), BF16),
            V((B, 8, 512), F32), V((S, B, 512), F32), V((S, B, 512), F32), V((B, 2, 32, T), F32), V((B, 2, 32, T), BF16),
            V((2, 8, 128), F32), V((4, 8, 128), F32), V((2, 2, 8, 8, 256), F32), V((2, 8, 8, 256), F32), V((2, 2, 8, 8, 256), F32),
            V((4, 8, 8, 512), F32), V((6, 8, 512), F32), V((6, 8, 512), F32), V((6, 8, 512), F32), V((2, 2, 6, 8, 256), F32),
            V((NCH, R, CW), F32), V((E, R, 128), F32), V((E, R, 2 * FS), F32), V((R, 512), F32), V((2, R, CW), F32), V((R, 8), F32), V((D, E), BF16), V((R, D), BF16), V((E, R, FS), BF16), V((NCH, R, CW), F32),
            V((NCH, R, CW), F32), V((2, R, CW), F32), V((NCH, 2, R, CW), F32), V((NCH, R, CW), F32), V((B, S, KV, HD), F32), V((B, S, KV, HD), F32),
            pltpu.SemaphoreType.DMA((NLOCAL,)), pltpu.SemaphoreType.DMA((NSEND,)), pltpu.SemaphoreType.DMA((NRECV,)),
        ]
        anyspec = pl.BlockSpec(memory_space=pl.ANY)
        outs = [((S, B, D), BF16), ((B, S, KV, HD), BF16), ((B, S, KV, HD), BF16)]
        vmem = pl.BlockSpec(memory_space=pltpu.VMEM)
        parts = pl.pallas_call(
            kernel,
            out_shape=tuple(V(*o) for o in outs),
            in_specs=[anyspec] * len(args),
            out_specs=(vmem,) * 3,
            scratch_shapes=scratch,
            compiler_params=pltpu.CompilerParams(collective_id=0, has_side_effects=True, vmem_limit_bytes=60 * 1024 * 1024),
        )(*args)
        return pl.pallas_call(
            write_kernel,
            out_shape=tuple(jax.ShapeDtypeStruct(*o) for o in outs),
            in_specs=[vmem] * 3,
            out_specs=(anyspec,) * 3,
            scratch_shapes=[pltpu.SemaphoreType.DMA((3,))],
            compiler_params=pltpu.CompilerParams(vmem_limit_bytes=1024 * 1024),
        )(*parts)

    replicated = P()
    in_specs = (P('dp'), P(None, 'dp'), P('dp', 'kv'), P('dp', 'kv'), P('dp')) + (replicated,) * 13 + (P(None, None, 'kv'), P(None, None, 'kv'), P(None, 'kv'), replicated, P(None, 'dp'), P(None, 'dp'))
    out_specs = (P(None, 'dp'), P('dp'), P('dp'))
    return jax.shard_map(layer_steps, mesh=mesh, in_specs=in_specs, out_specs=out_specs, check_vma=False)
```

```python
import functools
import itertools
import math

import jax
import jax.numpy as jnp
import numpy as np
from jax import lax
from jax.experimental import pallas as pl
from jax.experimental.pallas import tpu as pltpu
from jax.sharding import PartitionSpec as P

ROPE_BASE = 10000.0
ROPE_MSCALE = math.sqrt(1.0 + math.log(32.0) / math.log(4096.0))
NORM_EPS = 1e-5
NEG_FILL = -1e30
F32 = jnp.float32
BF16 = jnp.bfloat16

S = 3
B = 16
D = 1024
T = 256
KV = 8
HD = 64
E = 32
FS = 128
R = S * B
NCH = 4
CW = D // NCH

GROUPS = 8
SMALL, PARTS = 8, 4
L_SMALL, L_WQ, L_K, L_V, L_WO, L_GU, L_DN, NLOCAL = itertools.accumulate((SMALL, 2, PARTS, PARTS, 1, PARTS, 2), initial=0)
R_ML, R_O, R_C, R_G, R_P, R_B, NRECV = itertools.accumulate((3, 2, 2, 2, NCH, NCH + 1), initial=0)
S_ML, S_O, S_C, S_G, S_P, S_B, NSEND = range(7)
LN = 128
TWO, FOUR, EIGHT = range(2), range(4), range(8)


def at(i, width=LN):
    return slice(i * width, (i + 1) * width)


def mm(a, b):
    return jnp.dot(a, b, preferred_element_type=F32)


def mm_t(a, b):
    return lax.dot_general(a, b, (((1,), (1,)), ((), ())), preferred_element_type=F32)


def norm_rows(x, gain, bias):
    mean = jnp.mean(x, axis=-1, keepdims=True)
    cen = x - mean
    var = jnp.mean(cen * cen, axis=-1, keepdims=True)
    return (cen * lax.rsqrt(var + NORM_EPS) * gain + bias).astype(BF16)


def lane_iota(shape):
    return lax.broadcasted_iota(jnp.int32, shape, len(shape) - 1)


def kernel(
    x_first, next_emb, k_hbm, v_hbm, seq_hbm, g1_h, b1_h, wq_h, bq_h, wk_h, bk_h, wv_h, bv_h, wo_h, bo_h, g2_h, b2_h,
    wr_h, wg_h, wu_h, wd_h, lf_h, idx_h, rm_h, base_h,
    hb, tkb, tvb,
    xb, g1, b1, wq, bq, wk, bk, wv, bv, wo, bo, g2, b2, wr, wg, wu, wd, lf, idx, rm, base, seq_s, kc, vc,
    qbuf, kbuf, vbuf, sbuf, wbuf, mlb, mlall, obuf, orecv, c2, ex, ga, gb, tl, oall, xm4, gx, raw, qraw, dsum, picks, wrt, h2, ub, pb, ab, db, s2, yb, tkf, tvf,
    lsem, ssem, rsem,
):
    me = lax.axis_index("kv")
    core = me % 2
    chip = me // 2
    partner = me + 1 - 2 * core
    peer = (me + 2) % 4
    diag = (partner + 2) % 4

    def local(src, dst, i):
        return pltpu.make_async_copy(src, dst, lsem.at[i])

    def remote(src, dst, snd, rcv, dev):
        return pltpu.make_async_remote_copy(
            src_ref=src, dst_ref=dst, send_sem=ssem.at[snd], recv_sem=rsem.at[rcv],
            device_id={"kv": dev}, device_id_type=pl.DeviceIdType.MESH)

    small = [
        local(src, dst, L_SMALL + i % SMALL) for i, (src, dst) in enumerate((
            (x_first, xb.at[0]), (next_emb, xb.at[pl.ds(1, S - 1)]), (g1_h, g1), (b1_h, b1), (bq_h, bq), (lf_h, lf), (base_h, base),
            (seq_hbm, seq_s), (bk_h, bk), (bv_h, bv), (bo_h, bo), (g2_h, g2), (b2_h, b2), (wr_h, wr), (idx_h, idx), (rm_h, rm)))
    ]
    first, later = small[:SMALL], small[SMALL:]
    cp_wq = [local(wq_h.at[:, pl.ds(i * 512, 512)], wq.at[:, pl.ds(i * 512, 512)], L_WQ + i) for i in TWO]
    other, own = (1 - core) * 8, core * 8

    def k_part(i):
        sl = pl.ds((other if i < 2 else own) + (i % 2) * 4, 4)
        return local(k_hbm.at[sl], kc.at[sl], L_K + i)

    def v_part(i):
        sl = (pl.ds(other if i < 2 else own, 8), pl.ds((i % 2) * 4, 4))
        return local(v_hbm.at[sl], vc.at[sl], L_V + i)

    cp_k = [k_part(i) for i in FOUR]
    cp_v = [v_part(i) for i in FOUR]
    cp_wkv = [local(wk_h, wk, L_WQ), local(wv_h, wv, L_WQ + 1)]
    cp_wo = [
        local(wo_h.at[pl.ds(kv * 128 + g * 64, 64)], wo.at[g, pl.ds(kv * 64, 64)], L_WO) for kv in range(KV) for g in TWO
    ]

    def up_copy(src, dst, i, sem):
        sl = pl.ds(i * 4, 4)
        return local(src.at[sl], dst.at[sl], sem)

    def down_copy(m, e, n):
        sl = (pl.ds(e, n), pl.ds(0, FS), pl.ds(m * 2 * CW, 2 * CW))
        return local(wd_h.at[sl], wd.at[sl], L_DN + m)

    for c in first + cp_wq + cp_k[:3] + cp_v[:1] + cp_k[3:]:
        c.start()
    bar = pltpu.get_barrier_semaphore()
    for dev in (partner, peer, diag):
        pl.semaphore_signal(bar, inc=1, device_id={"kv": dev}, device_id_type=pl.DeviceIdType.MESH)
    qbuf[:, 6:8, :] = jnp.zeros((B, 2, 512), F32)

    for c in first:
        c.wait()
    for c in cp_v[1:]:
        c.start()

    lane48 = lane_iota((R, 128))
    inv = 1.0 / (jnp.concatenate([lf[...]] * 4, axis=1) * base[...])
    row_b = lax.broadcasted_iota(jnp.int32, (B, 128), 0)
    len_rows = jnp.zeros((B, 128), jnp.int32)
    for b in range(B):
        len_rows = jnp.where(row_b == b, seq_s[b], len_rows)
    angles = jnp.concatenate([(len_rows + s).astype(F32) for s in range(S)], axis=0) * inv
    cosv = jnp.cos(angles) * ROPE_MSCALE
    sinv = jnp.sin(angles) * ROPE_MSCALE
    low_half = (lane48 % HD) < (HD // 2)

    def rope(x, both=False):
        xf = x.astype(BF16).astype(F32)
        up, down_ = pltpu.roll(xf, 96, 1), pltpu.roll(xf, 32, 1)
        plain = (xf * cosv + jnp.where(low_half, -up, down_) * sinv).astype(BF16).astype(F32)
        if not both:
            return plain
        return plain, (pltpu.roll(xf, HD, 1) * cosv + jnp.where(low_half, -down_, up) * sinv).astype(BF16).astype(F32)

    h1 = norm_rows(xb[...].reshape(R, D).astype(F32), g1[...], b1[...])

    left = lane48 < HD

    def put_q(q, p):
        qa, qa_x = rope(q[:, :LN], True)
        qb, qb_x = rope(q[:, LN:], True)
        pair = (jnp.where(left, qa, qb_x) * 0.125, jnp.where(left, qa_x, qb) * 0.125)
        for g in TWO:
            for s in range(S):
                qbuf[:, 2 * s + g, at(p)] = pair[g][at(s, B)]

    cp_wq[0].wait()
    q_lo = mm(h1, wq[:, :512]) + bq[:, :512]
    qraw[...] = q_lo
    cp_wq[1].wait()
    for c in later + cp_wo + cp_wkv:
        c.start()
    q_hi = mm(h1, wq[:, 512:]) + bq[:, 512:]
    for p in FOUR:
        put_q(qraw[:, p * 256:(p + 1) * 256] if p < 2 else q_hi[:, (p - 2) * 256:(p - 1) * 256], p)

    rowq = lax.broadcasted_iota(jnp.int32, (32, T), 0)
    laneq = lane_iota((32, T))
    diag_mask = (rowq // 8) == (laneq // HD)
    pos = laneq + me * T
    lane8 = lane_iota((8, 128))

    def scores(start, i):
        qv = qbuf[start + i]
        for hh in TWO:
            rep = jnp.concatenate([qv[:, at(hh, T)]] * 4, axis=0)
            lhs = jnp.where(diag_mask, rep, 0.0).astype(BF16)
            sbuf[start + i, hh] = mm(lhs, kc[start + i, at(hh, 4)].reshape(256, T))

    def soft(start, i, acc):
        keep = pos < seq_s[start + i]
        for hh in TWO:
            sc = jnp.where(keep, sbuf[start + i, hh], NEG_FILL)
            m = jnp.max(sc, axis=1, keepdims=True)
            w = jnp.where(keep, jnp.exp(sc - m), 0.0)
            l = jnp.sum(w, axis=1, keepdims=True)
            wbuf[start + i, hh] = w.astype(BF16)
            for j in FOUR:
                spot = i * 16 + hh * 4 + j
                acc = jnp.where(lane8 == spot, m[at(j, 8)], acc)
                acc = jnp.where(lane8 == spot + 8, l[at(j, 8)], acc)
        return acc

    left8 = lane8 < HD

    def values(half, i, hh):
        b = half * 8 + i
        pv = mm_t(wbuf[b, hh], vc[b, at(hh, 4)].reshape(256, T))
        obuf[half, hh, i, :, 0:128] = jnp.where(left8, pv[0:8, 0:128], pv[8:16, 0:128])
        obuf[half, hh, i, :, 128:256] = jnp.where(left8, pv[16:24, 128:256], pv[24:32, 128:256])

    send_ml = [
        remote(mlb.at[1 - core], mlall.at[me], S_ML, R_ML, partner), remote(mlb.at[core], mlall.at[me], S_ML, R_ML + 1, peer),
        remote(mlb.at[1 - core], mlall.at[me], S_ML, R_ML + 2, diag),
    ]
    send_o = [remote(obuf.at[1 - core, hh], orecv.at[hh], S_O, R_O + hh, partner) for hh in TWO]
    zero = jnp.zeros((8, 128), F32)

    cp_k[0].wait()
    for i in FOUR:
        scores(other, i)
    cp_k[1].wait()
    for i in FOUR:
        scores(other, 4 + i)
    acc = zero
    for i in FOUR:
        acc = soft(other, i, acc)
    cp_k[2].wait()
    for i in range(GROUPS):
        sem = L_GU + 2 * (i // 5)
        up_copy(wg_h, wg, i, sem).start()
        up_copy(wu_h, wu, i, sem + 1).start()
    for i in FOUR:
        scores(own, i)
    for i in FOUR:
        acc = soft(other, 4 + i, acc)
    mlb[1 - core] = acc
    pl.semaphore_wait(bar, 3)
    send_ml[0].start()
    send_ml[2].start()

    cp_v[0].wait()
    for i in EIGHT:
        values(1 - core, i, 0)
    acc = zero
    for i in FOUR:
        acc = soft(own, i, acc)
    send_o[0].start()
    cp_v[1].wait()
    cp_k[3].wait()
    for i in range(GROUPS):
        down_copy(0, i * 4, 4).start()
    for i in range(GROUPS):
        down_copy(1, i * 4, 4).start()
    for i in EIGHT:
        values(1 - core, i, 1)
    for i in FOUR:
        scores(own, 4 + i)
    send_o[1].start()
    cp_v[2].wait()
    for i in FOUR:
        acc = soft(own, 4 + i, acc)
    mlb[core] = acc
    mlall[me] = acc
    for i in EIGHT:
        values(core, i, 0)
    send_ml[1].start()

    pick = (lane8 // HD)

    def spread(v, i, p):
        return jnp.take_along_axis(v, pick + (i * 16 + 2 * p), axis=1, mode="promise_in_bounds")

    send_c = [remote(c2.at[hh, chip, pl.ds(0, 6)], c2.at[hh, chip, pl.ds(0, 6)], S_C, R_C + hh, peer) for hh in TWO]
    for hh in TWO:
        if hh == 1:
            cp_v[3].wait()
            for i in EIGHT:
                values(core, i, 1)
        else:
            send_ml[0].wait_recv()
            ml_a = mlall[me]
            ml_b = mlall[partner]
            m_ab = jnp.maximum(ml_a, ml_b)
            f_a = jnp.exp(ml_a - m_ab)
            f_b = jnp.exp(ml_b - m_ab)
        send_o[hh].wait_recv()
        for i in EIGHT:
            oa = obuf[core, hh, i]
            ob = orecv[hh, i]
            for p in TWO:
                ln = at(p)
                c2[hh, chip, :, i, ln] = (
                    oa[:, ln] * spread(f_a, i, 2 * hh + p) + ob[:, ln] * spread(f_b, i, 2 * hh + p))
        send_c[hh].start()

    for c in later + cp_wkv:
        c.wait()
    for c in send_ml[1:]:
        c.wait_recv()
    kn = mm(h1, wk[...]) + bk[...]
    vn = (mm(h1, wv[...]) + bv[...]).astype(BF16)
    vn = vn.astype(F32)
    for p in FOUR:
        ln = at(p)
        for val, buf in ((rope(kn[:, ln]), kbuf), (vn[:, ln], vbuf)):
            for s in range(S):
                buf[s, :, ln] = val[at(s, B)]

    def tails():
        for buf, fin, out in ((kbuf, tkf, tkb), (vbuf, tvf, tvb)):
            for p in FOUR:
                for s in range(S):
                    val = buf[s, :, at(p)]
                    fin[:, s, 2 * p, :] = val[:, :HD]
                    fin[:, s, 2 * p + 1, :] = pltpu.roll(val, HD, 1)[:, :HD]
            out[...] = fin[...].astype(BF16)

    rows = pl.ds(pl.multiple_of(core * 8, 8), 8)
    kt = [kbuf[t, rows, :] for t in range(S)]
    vt = [vbuf[t, rows, :] for t in range(S)]
    trip = [(s, g, t) for s in range(S) for g in TWO for t in range(s + 1)]
    prod = jnp.concatenate([qbuf[rows, 2 * s + g, :] * kt[t] for s, g, t in trip], axis=0)
    hi = prod.astype(BF16)
    lo = (prod - hi.astype(F32)).astype(BF16)
    r2 = lax.broadcasted_iota(jnp.int32, (256, 128), 0)
    ones = jnp.where(((r2 % 128) // HD) == (lane_iota((256, 128)) // HD), 1.0, 0.0).astype(BF16)
    tsc = jnp.concatenate(
        [mm(jnp.concatenate([hi[:, at(p)], lo[:, at(p)]], axis=1), ones) for p in FOUR], axis=1)

    ml = [mlall[d] for d in FOUR]
    for ch in TWO:
        a, b_ = ml[2 * ch], ml[2 * ch + 1]
        mc = jnp.maximum(a, b_)
        lc = (pltpu.roll(a, 120, 1) * jnp.exp(a - mc) + pltpu.roll(b_, 120, 1) * jnp.exp(b_ - mc))
        for i in EIGHT:
            for p in FOUR:
                ln = at(p)
                ex[2 * ch, :, i, ln] = spread(mc, i, p)
                ex[2 * ch + 1, :, i, ln] = spread(lc, i, p)

    for s in range(S):
        for g in TWO:
            j = 2 * s + g
            sc = [tsc[at(n, 8)] for n, key in enumerate(trip) if key[:2] == (s, g)]
            mt = functools.reduce(jnp.maximum, sc)
            wt = [jnp.exp(v - mt) for v in sc]
            lt = functools.reduce(jnp.add, wt)
            ot = functools.reduce(jnp.add, [w.astype(BF16).astype(F32) * v for w, v in zip(wt, vt)])
            m0, l0, m1, l1 = ex[0, j], ex[1, j], ex[2, j], ex[3, j]
            top = jnp.maximum(jnp.maximum(m0, m1), mt)
            f0, f1, ft = jnp.exp(m0 - top), jnp.exp(m1 - top), jnp.exp(mt - top)
            inv_l = 1.0 / (l0 * f0 + l1 * f1 + lt * ft)
            ga[j] = f0 * inv_l
            gb[j] = f1 * inv_l
            tl[j] = ot * (ft * inv_l)

    send_g = [remote(oall.at[core, hh], oall.at[core, hh], S_G, R_G + hh, partner) for hh in TWO]
    for hh in TWO:
        send_c[hh].wait_recv()
        ln = at(hh, T)
        for j in range(6):
            oall[core, hh, j] = c2[hh, 0, j] * ga[j][:, ln] + c2[hh, 1, j] * gb[j][:, ln] + tl[j][:, ln]
        send_g[hh].start()

    eye = jnp.where(lax.broadcasted_iota(jnp.int32, (B, B), 0) == lane_iota((B, B)), 1.0, 0.0)
    picks[...] = jnp.concatenate([mm_t(eye, idx[s].astype(F32)) for s in range(S)], axis=0)

    eye_e = jnp.where(lax.broadcasted_iota(jnp.int32, (E, E), 0) == lane_iota((E, E)), 1.0, 0.0).astype(BF16)
    wrt[...] = lax.dot_general(wr[...], eye_e, (((0,), (0,)), ((), ())), preferred_element_type=F32).astype(BF16)

    here = me < 4

    @pl.when(here)
    def _():
        local(wo, wo, L_WO).wait()
        att = None
        for hh in TWO:
            send_g[hh].wait_recv()
            for g in TWO:
                o_g = jnp.concatenate([oall[h, hh, 2 * s + g] for s in range(S) for h in TWO], axis=0).astype(BF16)
                part = mm(o_g, wo[g, at(hh, T)])
                att = part if att is None else att + part
        xm = (xb[...].reshape(R, D).astype(F32) + att + bo[...]).astype(BF16).astype(F32)
        for n in range(NCH):
            xm4[n] = xm[:, at(n, CW)]
        h2[...] = norm_rows(xm, g2[...], b2[...])

    def act(i):
        for n in FOUR:
            e = i * 4 + n
            raw[e] = mm(h2[...], jnp.concatenate([wg[e], wu[e]], axis=1))

    def mix(i):
        for n in FOUR:
            e = i * 4 + n
            a, up = raw[e, :, :FS], raw[e, :, FS:]
            ub[e] = (gx[e] * (a * (1.0 / (1.0 + jnp.exp(-a)))) * up).astype(BF16)

    def wait_up(sl, sem):
        for n, w in enumerate((wg, wu)):
            local(w.at[sl], w.at[sl], sem + n).wait()

    wait_up(pl.ds(0, 20), L_GU)

    @pl.when(here)
    def _():
        logits = mm(h2[...], wrt[...])
        for i in FOUR:
            act(i)
        lane_e = lane_iota((R, E)).astype(F32)
        chosen = picks[...]
        gates = jnp.zeros((R, E), F32)
        for k in EIGHT:
            on = jnp.concatenate([rm[s, :, k, :] for s in range(S)], axis=0) == 1
            mk = jnp.where(on, logits, NEG_FILL)
            pk = jnp.exp(mk - jnp.max(mk, axis=1, keepdims=True))
            pk = pk / jnp.sum(pk, axis=1, keepdims=True)
            gates = gates + jnp.where(chosen[:, k:k + 1] == lane_e, pk, 0.0)
        for e in range(E):
            gx[e] = jnp.broadcast_to(gates[:, e:e + 1], (R, 128))

        act(4)

    def down(n, first, count, width):
        u = jnp.concatenate([ub[e] for e in range(first, first + count)], axis=1)
        return mm(u, wd[first:first + count, :, n * CW:n * CW + width].reshape(count * FS, width))

    def rounded(x):
        return x.astype(BF16).astype(F32)

    send_a = [remote(pb.at[n], ab.at[n], S_P, R_P + n, partner) for n in range(NCH)]
    send_b = [remote(s2.at[n, chip], s2.at[n, chip], S_B, R_B + n, peer) for n in range(NCH)]
    send_d = [remote(pb.at[0], db.at[0], S_B, R_B + NCH, diag), remote(pb.at[0], db.at[1], S_B, R_B, peer)]
    send_y = [remote(yb.at[n], yb.at[n], S_P, R_P + n, partner) for n in range(NCH)]

    wait_up(pl.ds(20, 12), L_GU + 2)

    @pl.when(here)
    def _():
        for i in range(5, 8):
            act(i)
            mix(i - 5)
        for i in range(3, 7):
            mix(i)

    for m in range(3):
        if m < 2:
            down_copy(m, 0, E).wait()

        @pl.when(here)
        def _():
            if m == 0:
                mix(7)
                part = rounded(down(0, 0, E, 2 * CW))
                pb[0] = part[:, :CW]
                pb[1] = part[:, CW:]
            else:
                for h in TWO:
                    dsum[h] = down(m + 1, h * (E // 2), E // 2, CW)
                pb[m + 1] = rounded(dsum[0] + dsum[1])

        @pl.when(core == 0)
        def _():
            for n in ((0, 1) if m == 0 else (m + 1,)):
                send_a[n].start()
            if m == 0:
                send_d[0].start()

        if m == 0:
            @pl.when(core == 1)
            def _():
                send_d[1].start()

    @pl.when(core == 1)
    def _():
        for n in range(NCH):
            send_a[n].wait_recv()
            s2[n, chip] = ab[n] + pb[n]
            if n > 0:
                send_b[n].start()
        tails()
        for c in send_d:
            c.wait_recv()
        s2[0, 1 - chip] = db[0] + db[1]
        for n in range(NCH):
            if n > 0:
                send_b[n].wait_recv()
            yb[n] = xm4[n] + (s2[n, 0] + s2[n, 1])
            send_y[n].start()
            hb[:, :, at(n, CW)] = yb[n].astype(BF16).reshape(S, B, CW)
        remote(s2.at[:, chip], s2.at[:, chip], S_B, R_B, peer).wait_send()

    @pl.when(core == 0)
    def _():
        tails()
        send_d[0].wait_send()
        for n in range(NCH):
            send_y[n].wait_recv()
            hb[:, :, at(n, CW)] = yb[n].astype(BF16).reshape(S, B, CW)

    for ref, snd in ((mlall.at[pl.ds(0, 3)], S_ML), (obuf.at[1 - core], S_O), (c2.at[:, chip, pl.ds(0, 6)], S_C), (oall.at[core], S_G), (pb, S_P)):
        remote(ref, ref, snd, R_ML, partner).wait_send()


def write_kernel(h, tk, tv, h_out, tk_out, tv_out, sem):
    copies = [pltpu.make_async_copy(a, b, sem.at[i]) for i, (a, b) in enumerate(((h, h_out), (tk, tk_out), (tv, tv_out)))]
    for c in copies:
        c.start()
    for c in copies:
        c.wait()


def solution(mesh):
    def layer_steps(x_first, next_emb, k_cache, v_cache, seq_len, ln1_gain, ln1_bias, w_q, b_q, w_k, b_k, w_v, b_v, w_o, b_o, ln2_gain, ln2_bias, w_router, w_gate, w_up, w_down, long_factor, expert_idx, route_mask):
        def row(v):
            return v.reshape(1, -1)

        powers = (np.float32(ROPE_BASE) ** (np.arange(32, dtype=np.float32) * np.float32(2.0) / np.float32(HD))).astype(np.float32)
        base = jnp.asarray(np.tile(powers, 4)[None, :])
        args = (
            x_first, next_emb, jnp.transpose(k_cache, (0, 2, 3, 1)), jnp.transpose(v_cache, (0, 2, 3, 1)), seq_len,
            row(ln1_gain), row(ln1_bias), w_q, row(b_q), w_k, row(b_k), w_v, row(b_v), w_o, row(b_o), row(ln2_gain), row(ln2_bias),
            jnp.transpose(w_router), w_gate, w_up, w_down, row(long_factor), jnp.transpose(expert_idx, (0, 2, 1)), route_mask, base,
        )
        V = pltpu.VMEM
        scratch = [
            V((S, B, D), BF16), V((1, D), F32), V((1, D), F32), V((D, D), BF16), V((1, D), F32), V((D, 512), BF16), V((1, 512), F32),
            V((D, 512), BF16), V((1, 512), F32), V((2, 512, D), BF16), V((1, D), F32), V((1, D), F32), V((1, D), F32), V((E, D), BF16),
            V((E, D, FS), BF16), V((E, D, FS), BF16), V((E, FS, D), BF16), V((1, 32), F32), V((S, 8, B), jnp.int32),
            V((S, B, 8, E), jnp.int32), V((1, 128), F32), pltpu.SMEM((B,), jnp.int32), V((B, KV, HD, T), BF16), V((B, KV, HD, T), BF16),
            V((B, 8, 512), F32), V((S, B, 512), F32), V((S, B, 512), F32), V((B, 2, 32, T), F32), V((B, 2, 32, T), BF16),
            V((2, 8, 128), F32), V((4, 8, 128), F32), V((2, 2, 8, 8, 256), F32), V((2, 8, 8, 256), F32), V((2, 2, 8, 8, 256), F32),
            V((4, 8, 8, 512), F32), V((6, 8, 512), F32), V((6, 8, 512), F32), V((6, 8, 512), F32), V((2, 2, 6, 8, 256), F32),
            V((NCH, R, CW), F32), V((E, R, 128), F32), V((E, R, 2 * FS), F32), V((R, 512), F32), V((2, R, CW), F32), V((R, 8), F32), V((D, E), BF16), V((R, D), BF16), V((E, R, FS), BF16), V((NCH, R, CW), F32),
            V((NCH, R, CW), F32), V((2, R, CW), F32), V((NCH, 2, R, CW), F32), V((NCH, R, CW), F32), V((B, S, KV, HD), F32), V((B, S, KV, HD), F32),
            pltpu.SemaphoreType.DMA((NLOCAL,)), pltpu.SemaphoreType.DMA((NSEND,)), pltpu.SemaphoreType.DMA((NRECV,)),
        ]
        anyspec = pl.BlockSpec(memory_space=pl.ANY)
        outs = [((S, B, D), BF16), ((B, S, KV, HD), BF16), ((B, S, KV, HD), BF16)]
        vmem = pl.BlockSpec(memory_space=pltpu.VMEM)
        parts = pl.pallas_call(
            kernel,
            out_shape=tuple(V(*o) for o in outs),
            in_specs=[anyspec] * len(args),
            out_specs=(vmem,) * 3,
            scratch_shapes=scratch,
            compiler_params=pltpu.CompilerParams(collective_id=0, has_side_effects=True, vmem_limit_bytes=60 * 1024 * 1024),
        )(*args)
        return pl.pallas_call(
            write_kernel,
            out_shape=tuple(jax.ShapeDtypeStruct(*o) for o in outs),
            in_specs=[vmem] * 3,
            out_specs=(anyspec,) * 3,
            scratch_shapes=[pltpu.SemaphoreType.DMA((3,))],
            compiler_params=pltpu.CompilerParams(vmem_limit_bytes=1024 * 1024),
        )(*parts)

    replicated = P()
    in_specs = (P('dp'), P(None, 'dp'), P('dp', 'kv'), P('dp', 'kv'), P('dp')) + (replicated,) * 13 + (P(None, None, 'kv'), P(None, None, 'kv'), P(None, 'kv'), replicated, P(None, 'dp'), P(None, 'dp'))
    out_specs = (P(None, 'dp'), P('dp'), P('dp'))
    return jax.shard_map(layer_steps, mesh=mesh, in_specs=in_specs, out_specs=out_specs, check_vma=False)
```

```python
import functools
import itertools
import math

import jax
import jax.numpy as jnp
import numpy as np
from jax import lax
from jax.experimental import pallas as pl
from jax.experimental.pallas import tpu as pltpu
from jax.sharding import PartitionSpec as P

ROPE_BASE = 10000.0
ROPE_MSCALE = math.sqrt(1.0 + math.log(32.0) / math.log(4096.0))
NORM_EPS = 1e-5
NEG_FILL = -1e30
F32 = jnp.float32
BF16 = jnp.bfloat16

S = 3
B = 16
D = 1024
T = 256
KV = 8
HD = 64
E = 32
FS = 128
R = S * B
NCH = 4
CW = D // NCH
LAST = NCH - 1

GROUPS = 8
SMALL, PARTS = 8, 4
L_SMALL, L_WQ, L_K, L_V, L_WO, L_GU, L_DN, NLOCAL = itertools.accumulate((SMALL, 2, PARTS, PARTS, 1, PARTS, 2), initial=0)
R_ML, R_O, R_C, R_G, R_P, R_B, NRECV = itertools.accumulate((3, 2, 2, 2, NCH, NCH + 1), initial=0)
S_ML, S_O, S_C, S_G, S_P, S_B, NSEND = range(7)
LN = 128
TWO, FOUR, EIGHT = range(2), range(4), range(8)


def at(i, width=LN):
    return slice(i * width, (i + 1) * width)


def mm(a, b):
    return jnp.dot(a, b, preferred_element_type=F32)


def mm_t(a, b):
    return lax.dot_general(a, b, (((1,), (1,)), ((), ())), preferred_element_type=F32)


def norm_rows(x, gain, bias):
    mean = jnp.mean(x, axis=-1, keepdims=True)
    cen = x - mean
    var = jnp.mean(cen * cen, axis=-1, keepdims=True)
    return (cen * lax.rsqrt(var + NORM_EPS) * gain + bias).astype(BF16)


def lane_iota(shape):
    return lax.broadcasted_iota(jnp.int32, shape, len(shape) - 1)


def kernel(
    x_first, next_emb, k_hbm, v_hbm, seq_hbm, g1_h, b1_h, wq_h, bq_h, wk_h, bk_h, wv_h, bv_h, wo_h, bo_h, g2_h, b2_h,
    wr_h, wg_h, wu_h, wd_h, lf_h, idx_h, rm_h, base_h,
    hb, tkb, tvb,
    xb, g1, b1, wq, bq, wk, bk, wv, bv, wo, bo, g2, b2, wr, wg, wu, wd, lf, idx, rm, base, seq_s, kc, vc,
    qbuf, kbuf, vbuf, sbuf, wbuf, mlb, mlall, obuf, orecv, c2, ex, ga, gb, tl, oall, xm4, gx, raw, qraw, dsum, picks, wrt, h2, ub, pb, ab, db, s2, yb, tkf, tvf,
    lsem, ssem, rsem,
):
    me = lax.axis_index("kv")
    core = me % 2
    chip = me // 2
    partner = me + 1 - 2 * core
    peer = (me + 2) % 4
    diag = (partner + 2) % 4

    def local(src, dst, i):
        return pltpu.make_async_copy(src, dst, lsem.at[i])

    def remote(src, dst, snd, rcv, dev):
        return pltpu.make_async_remote_copy(
            src_ref=src, dst_ref=dst, send_sem=ssem.at[snd], recv_sem=rsem.at[rcv],
            device_id={"kv": dev}, device_id_type=pl.DeviceIdType.MESH)

    small = [
        local(src, dst, L_SMALL + i % SMALL) for i, (src, dst) in enumerate((
            (x_first, xb.at[0]), (next_emb, xb.at[pl.ds(1, S - 1)]), (g1_h, g1), (b1_h, b1), (bq_h, bq), (lf_h, lf), (base_h, base),
            (seq_hbm, seq_s), (bk_h, bk), (bv_h, bv), (bo_h, bo), (g2_h, g2), (b2_h, b2), (wr_h, wr), (idx_h, idx), (rm_h, rm)))
    ]
    first, later = small[:SMALL], small[SMALL:]
    cp_wq = [local(wq_h.at[:, pl.ds(i * 512, 512)], wq.at[:, pl.ds(i * 512, 512)], L_WQ + i) for i in TWO]
    other, own = (1 - core) * 8, core * 8

    def k_part(i):
        sl = pl.ds((other if i < 2 else own) + (i % 2) * 4, 4)
        return local(k_hbm.at[sl], kc.at[sl], L_K + i)

    def v_part(i):
        sl = (pl.ds(other if i < 2 else own, 8), pl.ds((i % 2) * 4, 4))
        return local(v_hbm.at[sl], vc.at[sl], L_V + i)

    cp_k = [k_part(i) for i in FOUR]
    cp_v = [v_part(i) for i in FOUR]
    cp_wkv = [local(wk_h, wk, L_WQ), local(wv_h, wv, L_WQ + 1)]
    cp_wo = [
        local(wo_h.at[pl.ds(kv * 128 + g * 64, 64)], wo.at[g, pl.ds(kv * 64, 64)], L_WO) for kv in range(KV) for g in TWO
    ]

    def up_copy(src, dst, i, sem):
        sl = pl.ds(i * 4, 4)
        return local(src.at[sl], dst.at[sl], sem)

    def down_copy(m, e, n):
        sl = (pl.ds(e, n), pl.ds(0, FS), pl.ds(m * 2 * CW, 2 * CW))
        return local(wd_h.at[sl], wd.at[sl], L_DN + m)

    for c in first + cp_wq + cp_k[:3] + cp_v[:1] + cp_k[3:]:
        c.start()
    bar = pltpu.get_barrier_semaphore()
    for dev in (partner, peer, diag):
        pl.semaphore_signal(bar, inc=1, device_id={"kv": dev}, device_id_type=pl.DeviceIdType.MESH)
    qbuf[:, 6:8, :] = jnp.zeros((B, 2, 512), F32)

    for c in first:
        c.wait()
    for c in cp_v[1:]:
        c.start()

    lane48 = lane_iota((R, 128))
    inv = 1.0 / (jnp.concatenate([lf[...]] * 4, axis=1) * base[...])
    row_b = lax.broadcasted_iota(jnp.int32, (B, 128), 0)
    len_rows = jnp.zeros((B, 128), jnp.int32)
    for b in range(B):
        len_rows = jnp.where(row_b == b, seq_s[b], len_rows)
    angles = jnp.concatenate([(len_rows + s).astype(F32) for s in range(S)], axis=0) * inv
    cosv = jnp.cos(angles) * ROPE_MSCALE
    sinv = jnp.sin(angles) * ROPE_MSCALE
    low_half = (lane48 % HD) < (HD // 2)

    def rope(x, both=False):
        xf = x.astype(BF16).astype(F32)
        up, down_ = pltpu.roll(xf, 96, 1), pltpu.roll(xf, 32, 1)
        plain = (xf * cosv + jnp.where(low_half, -up, down_) * sinv).astype(BF16).astype(F32)
        if not both:
            return plain
        return plain, (pltpu.roll(xf, HD, 1) * cosv + jnp.where(low_half, -down_, up) * sinv).astype(BF16).astype(F32)

    h1 = norm_rows(xb[...].reshape(R, D).astype(F32), g1[...], b1[...])

    left = lane48 < HD

    def put_q(q, p):
        qa, qa_x = rope(q[:, :LN], True)
        qb, qb_x = rope(q[:, LN:], True)
        pair = (jnp.where(left, qa, qb_x) * 0.125, jnp.where(left, qa_x, qb) * 0.125)
        for g in TWO:
            for s in range(S):
                qbuf[:, 2 * s + g, at(p)] = pair[g][at(s, B)]

    cp_wq[0].wait()
    q_lo = mm(h1, wq[:, :512]) + bq[:, :512]
    qraw[...] = q_lo
    cp_wq[1].wait()
    for c in later + cp_wo + cp_wkv:
        c.start()
    q_hi = mm(h1, wq[:, 512:]) + bq[:, 512:]
    for p in FOUR:
        put_q(qraw[:, p * 256:(p + 1) * 256] if p < 2 else q_hi[:, (p - 2) * 256:(p - 1) * 256], p)

    rowq = lax.broadcasted_iota(jnp.int32, (32, T), 0)
    laneq = lane_iota((32, T))
    diag_mask = (rowq // 8) == (laneq // HD)
    pos = laneq + me * T
    lane8 = lane_iota((8, 128))

    def scores(start, i):
        qv = qbuf[start + i]
        for hh in TWO:
            rep = jnp.concatenate([qv[:, at(hh, T)]] * 4, axis=0)
            lhs = jnp.where(diag_mask, rep, 0.0).astype(BF16)
            sbuf[start + i, hh] = mm(lhs, kc[start + i, at(hh, 4)].reshape(256, T))

    def soft(start, i, acc):
        keep = pos < seq_s[start + i]
        for hh in TWO:
            sc = jnp.where(keep, sbuf[start + i, hh], NEG_FILL)
            m = jnp.max(sc, axis=1, keepdims=True)
            w = jnp.where(keep, jnp.exp(sc - m), 0.0)
            l = jnp.sum(w, axis=1, keepdims=True)
            wbuf[start + i, hh] = w.astype(BF16)
            for j in FOUR:
                spot = i * 16 + hh * 4 + j
                acc = jnp.where(lane8 == spot, m[at(j, 8)], acc)
                acc = jnp.where(lane8 == spot + 8, l[at(j, 8)], acc)
        return acc

    left8 = lane8 < HD

    def values(half, i, hh):
        b = half * 8 + i
        pv = mm_t(wbuf[b, hh], vc[b, at(hh, 4)].reshape(256, T))
        obuf[half, hh, i, :, 0:128] = jnp.where(left8, pv[0:8, 0:128], pv[8:16, 0:128])
        obuf[half, hh, i, :, 128:256] = jnp.where(left8, pv[16:24, 128:256], pv[24:32, 128:256])

    send_ml = [
        remote(mlb.at[1 - core], mlall.at[me], S_ML, R_ML, partner), remote(mlb.at[core], mlall.at[me], S_ML, R_ML + 1, peer),
        remote(mlb.at[1 - core], mlall.at[me], S_ML, R_ML + 2, diag),
    ]
    send_o = [remote(obuf.at[1 - core, hh], orecv.at[hh], S_O, R_O + hh, partner) for hh in TWO]
    zero = jnp.zeros((8, 128), F32)

    cp_k[0].wait()
    for i in FOUR:
        scores(other, i)
    cp_k[1].wait()
    for i in FOUR:
        scores(other, 4 + i)
    acc = zero
    for i in FOUR:
        acc = soft(other, i, acc)
    cp_k[2].wait()
    for i in range(GROUPS):
        sem = L_GU + 2 * (i // 5)
        up_copy(wg_h, wg, i, sem).start()
        up_copy(wu_h, wu, i, sem + 1).start()
    for i in FOUR:
        scores(own, i)
    for i in FOUR:
        acc = soft(other, 4 + i, acc)
    mlb[1 - core] = acc
    pl.semaphore_wait(bar, 3)
    send_ml[0].start()
    send_ml[2].start()

    cp_v[0].wait()
    for i in EIGHT:
        values(1 - core, i, 0)
    acc = zero
    for i in FOUR:
        acc = soft(own, i, acc)
    send_o[0].start()
    cp_k[3].wait()
    for i in FOUR:
        scores(own, 4 + i)
    cp_v[1].wait()
    for m in TWO:
        for i in range(GROUPS):
            down_copy(m, i * 4, 4).start()
    for i in EIGHT:
        values(1 - core, i, 1)
    for i in FOUR:
        acc = soft(own, 4 + i, acc)
    mlb[core] = acc
    mlall[me] = acc
    send_o[1].start()
    send_ml[1].start()
    cp_v[2].wait()
    for i in EIGHT:
        values(core, i, 0)

    pick = (lane8 // HD)

    def spread(v, i, p):
        return jnp.take_along_axis(v, pick + (i * 16 + 2 * p), axis=1, mode="promise_in_bounds")

    send_c = [remote(c2.at[hh, chip, pl.ds(0, 6)], c2.at[hh, chip, pl.ds(0, 6)], S_C, R_C + hh, peer) for hh in TWO]
    for hh in TWO:
        if hh == 1:
            cp_v[3].wait()
            for i in EIGHT:
                values(core, i, 1)
        else:
            send_ml[0].wait_recv()
            ml_a = mlall[me]
            ml_b = mlall[partner]
            m_ab = jnp.maximum(ml_a, ml_b)
            f_a = jnp.exp(ml_a - m_ab)
            f_b = jnp.exp(ml_b - m_ab)
        send_o[hh].wait_recv()
        for i in EIGHT:
            oa = obuf[core, hh, i]
            ob = orecv[hh, i]
            for p in TWO:
                ln = at(p)
                c2[hh, chip, :, i, ln] = (
                    oa[:, ln] * spread(f_a, i, 2 * hh + p) + ob[:, ln] * spread(f_b, i, 2 * hh + p))
        send_c[hh].start()

    for c in later + cp_wkv:
        c.wait()
    for c in send_ml[1:]:
        c.wait_recv()
    kn = mm(h1, wk[...]) + bk[...]
    vn = (mm(h1, wv[...]) + bv[...]).astype(BF16)
    vn = vn.astype(F32)
    for p in FOUR:
        ln = at(p)
        for val, buf in ((rope(kn[:, ln]), kbuf), (vn[:, ln], vbuf)):
            for s in range(S):
                buf[s, :, ln] = val[at(s, B)]

    def tails():
        for buf, fin, out in ((kbuf, tkf, tkb), (vbuf, tvf, tvb)):
            for p in FOUR:
                for s in range(S):
                    val = buf[s, :, at(p)]
                    fin[:, s, 2 * p, :] = val[:, :HD]
                    fin[:, s, 2 * p + 1, :] = pltpu.roll(val, HD, 1)[:, :HD]
            out[...] = fin[...].astype(BF16)

    rows = pl.ds(pl.multiple_of(core * 8, 8), 8)
    kt = [kbuf[t, rows, :] for t in range(S)]
    vt = [vbuf[t, rows, :] for t in range(S)]
    trip = [(s, g, t) for s in range(S) for g in TWO for t in range(s + 1)]
    prod = jnp.concatenate([qbuf[rows, 2 * s + g, :] * kt[t] for s, g, t in trip], axis=0)
    hi = prod.astype(BF16)
    lo = (prod - hi.astype(F32)).astype(BF16)
    r2 = lax.broadcasted_iota(jnp.int32, (256, 128), 0)
    ones = jnp.where(((r2 % 128) // HD) == (lane_iota((256, 128)) // HD), 1.0, 0.0).astype(BF16)
    tsc = jnp.concatenate(
        [mm(jnp.concatenate([hi[:, at(p)], lo[:, at(p)]], axis=1), ones) for p in FOUR], axis=1)

    ml = [mlall[d] for d in FOUR]
    for ch in TWO:
        a, b_ = ml[2 * ch], ml[2 * ch + 1]
        mc = jnp.maximum(a, b_)
        lc = (pltpu.roll(a, 120, 1) * jnp.exp(a - mc) + pltpu.roll(b_, 120, 1) * jnp.exp(b_ - mc))
        for i in EIGHT:
            for p in FOUR:
                ln = at(p)
                ex[2 * ch, :, i, ln] = spread(mc, i, p)
                ex[2 * ch + 1, :, i, ln] = spread(lc, i, p)

    for s in range(S):
        for g in TWO:
            j = 2 * s + g
            sc = [tsc[at(n, 8)] for n, key in enumerate(trip) if key[:2] == (s, g)]
            mt = functools.reduce(jnp.maximum, sc)
            wt = [jnp.exp(v - mt) for v in sc]
            lt = functools.reduce(jnp.add, wt)
            ot = functools.reduce(jnp.add, [w.astype(BF16).astype(F32) * v for w, v in zip(wt, vt)])
            m0, l0, m1, l1 = ex[0, j], ex[1, j], ex[2, j], ex[3, j]
            top = jnp.maximum(jnp.maximum(m0, m1), mt)
            f0, f1, ft = jnp.exp(m0 - top), jnp.exp(m1 - top), jnp.exp(mt - top)
            inv_l = 1.0 / (l0 * f0 + l1 * f1 + lt * ft)
            ga[j] = f0 * inv_l
            gb[j] = f1 * inv_l
            tl[j] = ot * (ft * inv_l)

    send_g = [remote(oall.at[core, hh], oall.at[core, hh], S_G, R_G + hh, partner) for hh in TWO]
    for hh in TWO:
        send_c[hh].wait_recv()
        ln = at(hh, T)
        for j in range(6):
            oall[core, hh, j] = c2[hh, 0, j] * ga[j][:, ln] + c2[hh, 1, j] * gb[j][:, ln] + tl[j][:, ln]
        send_g[hh].start()

    eye = jnp.where(lax.broadcasted_iota(jnp.int32, (B, B), 0) == lane_iota((B, B)), 1.0, 0.0)
    picks[...] = jnp.concatenate([mm_t(eye, idx[s].astype(F32)) for s in range(S)], axis=0)

    eye_e = jnp.where(lax.broadcasted_iota(jnp.int32, (E, E), 0) == lane_iota((E, E)), 1.0, 0.0).astype(BF16)
    wrt[...] = lax.dot_general(wr[...], eye_e, (((0,), (0,)), ((), ())), preferred_element_type=F32).astype(BF16)

    here = me < 4

    @pl.when(here)
    def _():
        local(wo, wo, L_WO).wait()
        att = None
        for hh in TWO:
            send_g[hh].wait_recv()
            for g in TWO:
                o_g = jnp.concatenate([oall[h, hh, 2 * s + g] for s in range(S) for h in TWO], axis=0).astype(BF16)
                part = mm(o_g, wo[g, at(hh, T)])
                att = part if att is None else att + part
        xm = (xb[...].reshape(R, D).astype(F32) + att + bo[...]).astype(BF16).astype(F32)
        for n in range(NCH):
            xm4[n] = xm[:, at(n, CW)]
        h2[...] = norm_rows(xm, g2[...], b2[...])

    def act(i):
        for n in FOUR:
            e = i * 4 + n
            raw[e] = mm(h2[...], jnp.concatenate([wg[e], wu[e]], axis=1))

    def mix(i):
        for n in FOUR:
            e = i * 4 + n
            a, up = raw[e, :, :FS], raw[e, :, FS:]
            ub[e] = (gx[e] * (a * (1.0 / (1.0 + jnp.exp(-a)))) * up).astype(BF16)

    def wait_up(sl, sem):
        for n, w in enumerate((wg, wu)):
            local(w.at[sl], w.at[sl], sem + n).wait()

    wait_up(pl.ds(0, 20), L_GU)

    @pl.when(here)
    def _():
        logits = mm(h2[...], wrt[...])
        for i in FOUR:
            act(i)
        lane_e = lane_iota((R, E)).astype(F32)
        chosen = picks[...]
        gates = jnp.zeros((R, E), F32)
        for k in EIGHT:
            on = jnp.concatenate([rm[s, :, k, :] for s in range(S)], axis=0) == 1
            mk = jnp.where(on, logits, NEG_FILL)
            pk = jnp.exp(mk - jnp.max(mk, axis=1, keepdims=True))
            pk = pk / jnp.sum(pk, axis=1, keepdims=True)
            gates = gates + jnp.where(chosen[:, k:k + 1] == lane_e, pk, 0.0)
        for e in range(E):
            gx[e] = jnp.broadcast_to(gates[:, e:e + 1], (R, 128))

        act(4)

    def down(n, first, count, width):
        u = jnp.concatenate([ub[e] for e in range(first, first + count)], axis=1)
        return mm(u, wd[first:first + count, :, n * CW:n * CW + width].reshape(count * FS, width))

    def rounded(x):
        return x.astype(BF16).astype(F32)

    send_a = [remote(pb.at[n], ab.at[n], S_P, R_P + n, partner) for n in range(NCH)]
    send_b = [remote(s2.at[n, chip], s2.at[n, chip], S_B, R_B + n, peer) for n in range(NCH)]
    send_d = [remote(pb.at[0], db.at[0], S_B, R_B + NCH, diag), remote(pb.at[0], db.at[1], S_B, R_B, peer)]
    send_last = [
        remote(s2.at[LAST, chip], s2.at[LAST, chip], S_B, R_B + LAST, diag),
        remote(s2.at[LAST, chip], s2.at[LAST, chip], S_B, R_B + LAST - 1, partner),
    ]
    send_y = [remote(yb.at[n], yb.at[n], S_P, R_P + n, partner) for n in range(NCH)]

    wait_up(pl.ds(20, 12), L_GU + 2)

    @pl.when(here)
    def _():
        for i in range(5, 8):
            act(i)
            mix(i - 5)
        for i in range(3, 7):
            mix(i)

    for m in range(3):
        if m < 2:
            down_copy(m, 0, E).wait()

        @pl.when(here)
        def _():
            if m == 0:
                mix(7)
                part = rounded(down(0, 0, E, 2 * CW))
                pb[0] = part[:, :CW]
                pb[1] = part[:, CW:]
            else:
                for h in TWO:
                    dsum[h] = down(m + 1, h * (E // 2), E // 2, CW)
                pb[m + 1] = rounded(dsum[0] + dsum[1])

        @pl.when(core == 0)
        def _():
            for n in ((0, 1) if m == 0 else (m + 1,)):
                send_a[n].start()
            if m == 0:
                send_d[0].start()

        @pl.when(core == 1)
        def _():
            if m == 0:
                send_d[1].start()
            for n in ((), (0, 1), (2, LAST))[m]:
                send_a[n].wait_recv()
                s2[n, chip] = ab[n] + pb[n]
                if n == LAST:
                    for c in send_last:
                        c.start()
                if n > 0:
                    send_b[n].start()

    def finish(n):
        yb[n] = xm4[n] + (s2[n, 0] + s2[n, 1])

    def put(n):
        hb[:, :, at(n, CW)] = yb[n].astype(BF16).reshape(S, B, CW)

    @pl.when(core == 1)
    def _():
        tails()
        for c in send_d:
            c.wait_recv()
        s2[0, 1 - chip] = db[0] + db[1]
        for n in range(NCH):
            if n > 0:
                send_b[n].wait_recv()
            finish(n)
            if n < LAST:
                send_y[n].start()
            put(n)
        for ref, snd in ((s2.at[:, chip], S_B), (s2.at[pl.ds(0, 2), chip], S_B), (yb.at[pl.ds(0, LAST)], S_P)):
            remote(ref, ref, snd, R_B, peer).wait_send()

    @pl.when(core == 0)
    def _():
        tails()
        send_d[0].wait_send()
        remote(pb, pb, S_P, R_B, peer).wait_send()
        for n in range(LAST):
            send_y[n].wait_recv()
            put(n)
        for c in send_last:
            c.wait_recv()
        finish(LAST)
        put(LAST)

    for ref, snd in ((mlall.at[pl.ds(0, 3)], S_ML), (obuf.at[1 - core], S_O), (c2.at[:, chip, pl.ds(0, 6)], S_C), (oall.at[core], S_G)):
        remote(ref, ref, snd, R_ML, partner).wait_send()


def write_kernel(h, tk, tv, h_out, tk_out, tv_out, sem):
    copies = [pltpu.make_async_copy(a, b, sem.at[i]) for i, (a, b) in enumerate(((h, h_out), (tk, tk_out), (tv, tv_out)))]
    for c in copies:
        c.start()
    for c in copies:
        c.wait()


def solution(mesh):
    def layer_steps(x_first, next_emb, k_cache, v_cache, seq_len, ln1_gain, ln1_bias, w_q, b_q, w_k, b_k, w_v, b_v, w_o, b_o, ln2_gain, ln2_bias, w_router, w_gate, w_up, w_down, long_factor, expert_idx, route_mask):
        def row(v):
            return v.reshape(1, -1)

        powers = (np.float32(ROPE_BASE) ** (np.arange(32, dtype=np.float32) * np.float32(2.0) / np.float32(HD))).astype(np.float32)
        base = jnp.asarray(np.tile(powers, 4)[None, :])
        args = (
            x_first, next_emb, jnp.transpose(k_cache, (0, 2, 3, 1)), jnp.transpose(v_cache, (0, 2, 3, 1)), seq_len,
            row(ln1_gain), row(ln1_bias), w_q, row(b_q), w_k, row(b_k), w_v, row(b_v), w_o, row(b_o), row(ln2_gain), row(ln2_bias),
            jnp.transpose(w_router), w_gate, w_up, w_down, row(long_factor), jnp.transpose(expert_idx, (0, 2, 1)), route_mask, base,
        )
        V = pltpu.VMEM
        scratch = [
            V((S, B, D), BF16), V((1, D), F32), V((1, D), F32), V((D, D), BF16), V((1, D), F32), V((D, 512), BF16), V((1, 512), F32),
            V((D, 512), BF16), V((1, 512), F32), V((2, 512, D), BF16), V((1, D), F32), V((1, D), F32), V((1, D), F32), V((E, D), BF16),
            V((E, D, FS), BF16), V((E, D, FS), BF16), V((E, FS, D), BF16), V((1, 32), F32), V((S, 8, B), jnp.int32),
            V((S, B, 8, E), jnp.int32), V((1, 128), F32), pltpu.SMEM((B,), jnp.int32), V((B, KV, HD, T), BF16), V((B, KV, HD, T), BF16),
            V((B, 8, 512), F32), V((S, B, 512), F32), V((S, B, 512), F32), V((B, 2, 32, T), F32), V((B, 2, 32, T), BF16),
            V((2, 8, 128), F32), V((4, 8, 128), F32), V((2, 2, 8, 8, 256), F32), V((2, 8, 8, 256), F32), V((2, 2, 8, 8, 256), F32),
            V((4, 8, 8, 512), F32), V((6, 8, 512), F32), V((6, 8, 512), F32), V((6, 8, 512), F32), V((2, 2, 6, 8, 256), F32),
            V((NCH, R, CW), F32), V((E, R, 128), F32), V((E, R, 2 * FS), F32), V((R, 512), F32), V((2, R, CW), F32), V((R, 8), F32), V((D, E), BF16), V((R, D), BF16), V((E, R, FS), BF16), V((NCH, R, CW), F32),
            V((NCH, R, CW), F32), V((2, R, CW), F32), V((NCH, 2, R, CW), F32), V((NCH, R, CW), F32), V((B, S, KV, HD), F32), V((B, S, KV, HD), F32),
            pltpu.SemaphoreType.DMA((NLOCAL,)), pltpu.SemaphoreType.DMA((NSEND,)), pltpu.SemaphoreType.DMA((NRECV,)),
        ]
        anyspec = pl.BlockSpec(memory_space=pl.ANY)
        outs = [((S, B, D), BF16), ((B, S, KV, HD), BF16), ((B, S, KV, HD), BF16)]
        vmem = pl.BlockSpec(memory_space=pltpu.VMEM)
        parts = pl.pallas_call(
            kernel,
            out_shape=tuple(V(*o) for o in outs),
            in_specs=[anyspec] * len(args),
            out_specs=(vmem,) * 3,
            scratch_shapes=scratch,
            compiler_params=pltpu.CompilerParams(collective_id=0, has_side_effects=True, vmem_limit_bytes=60 * 1024 * 1024),
        )(*args)
        return pl.pallas_call(
            write_kernel,
            out_shape=tuple(jax.ShapeDtypeStruct(*o) for o in outs),
            in_specs=[vmem] * 3,
            out_specs=(anyspec,) * 3,
            scratch_shapes=[pltpu.SemaphoreType.DMA((3,))],
            compiler_params=pltpu.CompilerParams(vmem_limit_bytes=1024 * 1024),
        )(*parts)

    replicated = P()
    in_specs = (P('dp'), P(None, 'dp'), P('dp', 'kv'), P('dp', 'kv'), P('dp')) + (replicated,) * 13 + (P(None, None, 'kv'), P(None, None, 'kv'), P(None, 'kv'), replicated, P(None, 'dp'), P(None, 'dp'))
    out_specs = (P(None, 'dp'), P('dp'), P('dp'))
    return jax.shard_map(layer_steps, mesh=mesh, in_specs=in_specs, out_specs=out_specs, check_vma=False)
```

```python
import functools
import itertools
import math

import jax
import jax.numpy as jnp
import numpy as np
from jax import lax
from jax.experimental import pallas as pl
from jax.experimental.pallas import tpu as pltpu
from jax.sharding import PartitionSpec as P

ROPE_BASE = 10000.0
ROPE_MSCALE = math.sqrt(1.0 + math.log(32.0) / math.log(4096.0))
NORM_EPS = 1e-5
NEG_FILL = -1e30
F32 = jnp.float32
BF16 = jnp.bfloat16

S = 3
B = 16
D = 1024
T = 256
KV = 8
HD = 64
E = 32
FS = 128
R = S * B
NCH = 4
CW = D // NCH
LAST = NCH - 1

GROUPS = 8
SMALL, PARTS = 8, 4
L_SMALL, L_WQ, L_K, L_V, L_WO, L_GU, L_DN, NLOCAL = itertools.accumulate((SMALL, 2, PARTS, PARTS, 1, PARTS, 3), initial=0)
R_ML, R_O, R_C, R_G, R_P, R_B, NRECV = itertools.accumulate((3, 2, 2, 2, NCH, NCH + 1), initial=0)
S_ML, S_O, S_C, S_G, S_P, S_B, NSEND = range(7)
LN = 128
TWO, FOUR, EIGHT = range(2), range(4), range(8)


def at(i, width=LN):
    return slice(i * width, (i + 1) * width)


def mm(a, b):
    return jnp.dot(a, b, preferred_element_type=F32)


def mm_t(a, b):
    return lax.dot_general(a, b, (((1,), (1,)), ((), ())), preferred_element_type=F32)


def norm_rows(x, gain, bias):
    mean = jnp.mean(x, axis=-1, keepdims=True)
    cen = x - mean
    var = jnp.mean(cen * cen, axis=-1, keepdims=True)
    return (cen * lax.rsqrt(var + NORM_EPS) * gain + bias).astype(BF16)


def lane_iota(shape):
    return lax.broadcasted_iota(jnp.int32, shape, len(shape) - 1)


def kernel(
    x_first, next_emb, k_hbm, v_hbm, seq_hbm, g1_h, b1_h, wq_h, bq_h, wk_h, bk_h, wv_h, bv_h, wo_h, bo_h, g2_h, b2_h,
    wr_h, wg_h, wu_h, wd_h, lf_h, idx_h, rm_h, base_h,
    hb, tkb, tvb,
    xb, g1, b1, wq, bq, wk, bk, wv, bv, wo, bo, g2, b2, wr, wg, wu, wd, lf, idx, rm, base, seq_s, kc, vc,
    qbuf, kbuf, vbuf, sbuf, wbuf, mlb, mlall, obuf, orecv, c2, ex, ga, gb, tl, oall, xm4, gx, raw, qraw, dsum, picks, wrt, h2, ub, pb, ab, db, s2, yb, tkf, tvf,
    lsem, ssem, rsem,
):
    me = lax.axis_index("kv")
    core = me % 2
    chip = me // 2
    partner = me + 1 - 2 * core
    peer = (me + 2) % 4
    diag = (partner + 2) % 4

    def local(src, dst, i):
        return pltpu.make_async_copy(src, dst, lsem.at[i])

    def remote(src, dst, snd, rcv, dev):
        return pltpu.make_async_remote_copy(
            src_ref=src, dst_ref=dst, send_sem=ssem.at[snd], recv_sem=rsem.at[rcv],
            device_id={"kv": dev}, device_id_type=pl.DeviceIdType.MESH)

    small = [
        local(src, dst, L_SMALL + i % SMALL) for i, (src, dst) in enumerate((
            (x_first, xb.at[0]), (next_emb, xb.at[pl.ds(1, S - 1)]), (g1_h, g1), (b1_h, b1), (bq_h, bq), (lf_h, lf), (base_h, base),
            (seq_hbm, seq_s), (bk_h, bk), (bv_h, bv), (bo_h, bo), (g2_h, g2), (b2_h, b2), (wr_h, wr), (idx_h, idx), (rm_h, rm)))
    ]
    first, later = small[:SMALL], small[SMALL:]
    cp_wq = [local(wq_h.at[:, pl.ds(i * 512, 512)], wq.at[:, pl.ds(i * 512, 512)], L_WQ + i) for i in TWO]
    other, own = (1 - core) * 8, core * 8

    def k_part(i):
        sl = pl.ds((other if i < 2 else own) + (i % 2) * 4, 4)
        return local(k_hbm.at[sl], kc.at[sl], L_K + i)

    def v_part(i):
        sl = (pl.ds(other if i < 2 else own, 8), pl.ds((i % 2) * 4, 4))
        return local(v_hbm.at[sl], vc.at[sl], L_V + i)

    cp_k = [k_part(i) for i in FOUR]
    cp_v = [v_part(i) for i in FOUR]
    cp_wkv = [local(wk_h, wk, L_WQ), local(wv_h, wv, L_WQ + 1)]
    cp_wo = [
        local(wo_h.at[pl.ds(kv * 128 + g * 64, 64)], wo.at[g, pl.ds(kv * 64, 64)], L_WO) for kv in range(KV) for g in TWO
    ]

    def up_copy(src, dst, i, sem):
        sl = pl.ds(i * 4, 4)
        return local(src.at[sl], dst.at[sl], sem)

    def down_copy(m, e, n):
        sl = (pl.ds(e, n), pl.ds(0, FS), pl.ds(0, 2 * CW) if m == 0 else pl.ds((m + 1) * CW, CW))
        return local(wd_h.at[sl], wd.at[sl], L_DN + m)

    for c in first + cp_wq + cp_k[:3] + cp_v[:1] + cp_k[3:]:
        c.start()
    bar = pltpu.get_barrier_semaphore()
    for dev in (partner, peer, diag):
        pl.semaphore_signal(bar, inc=1, device_id={"kv": dev}, device_id_type=pl.DeviceIdType.MESH)
    qbuf[:, 6:8, :] = jnp.zeros((B, 2, 512), F32)

    for c in first:
        c.wait()
    for c in cp_v[1:]:
        c.start()

    lane48 = lane_iota((R, 128))
    inv = 1.0 / (jnp.concatenate([lf[...]] * 4, axis=1) * base[...])
    row_b = lax.broadcasted_iota(jnp.int32, (B, 128), 0)
    len_rows = jnp.zeros((B, 128), jnp.int32)
    for b in range(B):
        len_rows = jnp.where(row_b == b, seq_s[b], len_rows)
    angles = jnp.concatenate([(len_rows + s).astype(F32) for s in range(S)], axis=0) * inv
    cosv = jnp.cos(angles) * ROPE_MSCALE
    sinv = jnp.sin(angles) * ROPE_MSCALE
    low_half = (lane48 % HD) < (HD // 2)

    def rope(x, both=False):
        xf = x.astype(BF16).astype(F32)
        up, down_ = pltpu.roll(xf, 96, 1), pltpu.roll(xf, 32, 1)
        plain = (xf * cosv + jnp.where(low_half, -up, down_) * sinv).astype(BF16).astype(F32)
        if not both:
            return plain
        return plain, (pltpu.roll(xf, HD, 1) * cosv + jnp.where(low_half, -down_, up) * sinv).astype(BF16).astype(F32)

    h1 = norm_rows(xb[...].reshape(R, D).astype(F32), g1[...], b1[...])

    left = lane48 < HD

    def put_q(q, p):
        qa, qa_x = rope(q[:, :LN], True)
        qb, qb_x = rope(q[:, LN:], True)
        pair = (jnp.where(left, qa, qb_x) * 0.125, jnp.where(left, qa_x, qb) * 0.125)
        for g in TWO:
            for s in range(S):
                qbuf[:, 2 * s + g, at(p)] = pair[g][at(s, B)]

    cp_wq[0].wait()
    q_lo = mm(h1, wq[:, :512]) + bq[:, :512]
    qraw[...] = q_lo
    cp_wq[1].wait()
    for c in later + cp_wo + cp_wkv:
        c.start()
    q_hi = mm(h1, wq[:, 512:]) + bq[:, 512:]
    for p in FOUR:
        put_q(qraw[:, p * 256:(p + 1) * 256] if p < 2 else q_hi[:, (p - 2) * 256:(p - 1) * 256], p)

    rowq = lax.broadcasted_iota(jnp.int32, (32, T), 0)
    laneq = lane_iota((32, T))
    diag_mask = (rowq // 8) == (laneq // HD)
    pos = laneq + me * T
    lane8 = lane_iota((8, 128))

    def scores(start, i):
        qv = qbuf[start + i]
        for hh in TWO:
            rep = jnp.concatenate([qv[:, at(hh, T)]] * 4, axis=0)
            lhs = jnp.where(diag_mask, rep, 0.0).astype(BF16)
            sbuf[start + i, hh] = mm(lhs, kc[start + i, at(hh, 4)].reshape(256, T))

    def soft(start, i, acc):
        keep = pos < seq_s[start + i]
        for hh in TWO:
            sc = jnp.where(keep, sbuf[start + i, hh], NEG_FILL)
            m = jnp.max(sc, axis=1, keepdims=True)
            w = jnp.where(keep, jnp.exp(sc - m), 0.0)
            l = jnp.sum(w, axis=1, keepdims=True)
            wbuf[start + i, hh] = w.astype(BF16)
            for j in FOUR:
                spot = i * 16 + hh * 4 + j
                acc = jnp.where(lane8 == spot, m[at(j, 8)], acc)
                acc = jnp.where(lane8 == spot + 8, l[at(j, 8)], acc)
        return acc

    left8 = lane8 < HD

    def values(half, i, hh):
        b = half * 8 + i
        pv = mm_t(wbuf[b, hh], vc[b, at(hh, 4)].reshape(256, T))
        obuf[half, hh, i, :, 0:128] = jnp.where(left8, pv[0:8, 0:128], pv[8:16, 0:128])
        obuf[half, hh, i, :, 128:256] = jnp.where(left8, pv[16:24, 128:256], pv[24:32, 128:256])

    send_ml = [
        remote(mlb.at[1 - core], mlall.at[me], S_ML, R_ML, partner), remote(mlb.at[core], mlall.at[me], S_ML, R_ML + 1, peer),
        remote(mlb.at[1 - core], mlall.at[me], S_ML, R_ML + 2, diag),
    ]
    send_o = [remote(obuf.at[1 - core, hh], orecv.at[hh], S_O, R_O + hh, partner) for hh in TWO]
    zero = jnp.zeros((8, 128), F32)

    cp_k[0].wait()
    for i in FOUR:
        scores(other, i)
    cp_k[1].wait()
    for i in FOUR:
        scores(other, 4 + i)
    acc = zero
    for i in FOUR:
        acc = soft(other, i, acc)
    cp_k[2].wait()
    for i in range(GROUPS):
        sem = L_GU + 2 * (i // 5)
        up_copy(wg_h, wg, i, sem).start()
        up_copy(wu_h, wu, i, sem + 1).start()
    for i in FOUR:
        scores(own, i)
    for i in FOUR:
        acc = soft(other, 4 + i, acc)
    mlb[1 - core] = acc
    pl.semaphore_wait(bar, 3)
    send_ml[0].start()
    send_ml[2].start()

    cp_v[0].wait()
    for i in EIGHT:
        values(1 - core, i, 0)
    acc = zero
    for i in FOUR:
        acc = soft(own, i, acc)
    send_o[0].start()
    cp_k[3].wait()
    for i in FOUR:
        scores(own, 4 + i)
    cp_v[1].wait()
    for m in range(3):
        for i in range(GROUPS):
            down_copy(m, i * 4, 4).start()
    for i in EIGHT:
        values(1 - core, i, 1)
    for i in FOUR:
        acc = soft(own, 4 + i, acc)
    mlb[core] = acc
    mlall[me] = acc
    send_o[1].start()
    send_ml[1].start()
    cp_v[2].wait()
    for i in EIGHT:
        values(core, i, 0)

    pick = (lane8 // HD)

    def spread(v, i, p):
        return jnp.take_along_axis(v, pick + (i * 16 + 2 * p), axis=1, mode="promise_in_bounds")

    send_c = [remote(c2.at[hh, chip, pl.ds(0, 6)], c2.at[hh, chip, pl.ds(0, 6)], S_C, R_C + hh, peer) for hh in TWO]
    for hh in TWO:
        if hh == 1:
            cp_v[3].wait()
            for i in EIGHT:
                values(core, i, 1)
        else:
            send_ml[0].wait_recv()
            ml_a = mlall[me]
            ml_b = mlall[partner]
            m_ab = jnp.maximum(ml_a, ml_b)
            f_a = jnp.exp(ml_a - m_ab)
            f_b = jnp.exp(ml_b - m_ab)
        send_o[hh].wait_recv()
        for i in EIGHT:
            oa = obuf[core, hh, i]
            ob = orecv[hh, i]
            for p in TWO:
                ln = at(p)
                c2[hh, chip, :, i, ln] = (
                    oa[:, ln] * spread(f_a, i, 2 * hh + p) + ob[:, ln] * spread(f_b, i, 2 * hh + p))
        send_c[hh].start()

    for c in later + cp_wkv:
        c.wait()
    for c in send_ml[1:]:
        c.wait_recv()
    kn = mm(h1, wk[...]) + bk[...]
    vn = (mm(h1, wv[...]) + bv[...]).astype(BF16)
    vn = vn.astype(F32)
    for p in FOUR:
        ln = at(p)
        for val, buf in ((rope(kn[:, ln]), kbuf), (vn[:, ln], vbuf)):
            for s in range(S):
                buf[s, :, ln] = val[at(s, B)]

    def tails():
        for buf, fin, out in ((kbuf, tkf, tkb), (vbuf, tvf, tvb)):
            for p in FOUR:
                for s in range(S):
                    val = buf[s, :, at(p)]
                    fin[:, s, 2 * p, :] = val[:, :HD]
                    fin[:, s, 2 * p + 1, :] = pltpu.roll(val, HD, 1)[:, :HD]
            out[...] = fin[...].astype(BF16)

    rows = pl.ds(pl.multiple_of(core * 8, 8), 8)
    kt = [kbuf[t, rows, :] for t in range(S)]
    vt = [vbuf[t, rows, :] for t in range(S)]
    trip = [(s, g, t) for s in range(S) for g in TWO for t in range(s + 1)]
    prod = jnp.concatenate([qbuf[rows, 2 * s + g, :] * kt[t] for s, g, t in trip], axis=0)
    hi = prod.astype(BF16)
    lo = (prod - hi.astype(F32)).astype(BF16)
    r2 = lax.broadcasted_iota(jnp.int32, (256, 128), 0)
    ones = jnp.where(((r2 % 128) // HD) == (lane_iota((256, 128)) // HD), 1.0, 0.0).astype(BF16)
    tsc = jnp.concatenate(
        [mm(jnp.concatenate([hi[:, at(p)], lo[:, at(p)]], axis=1), ones) for p in FOUR], axis=1)

    ml = [mlall[d] for d in FOUR]
    for ch in TWO:
        a, b_ = ml[2 * ch], ml[2 * ch + 1]
        mc = jnp.maximum(a, b_)
        lc = (pltpu.roll(a, 120, 1) * jnp.exp(a - mc) + pltpu.roll(b_, 120, 1) * jnp.exp(b_ - mc))
        for i in EIGHT:
            for p in FOUR:
                ln = at(p)
                ex[2 * ch, :, i, ln] = spread(mc, i, p)
                ex[2 * ch + 1, :, i, ln] = spread(lc, i, p)

    for s in range(S):
        for g in TWO:
            j = 2 * s + g
            sc = [tsc[at(n, 8)] for n, key in enumerate(trip) if key[:2] == (s, g)]
            mt = functools.reduce(jnp.maximum, sc)
            wt = [jnp.exp(v - mt) for v in sc]
            lt = functools.reduce(jnp.add, wt)
            ot = functools.reduce(jnp.add, [w.astype(BF16).astype(F32) * v for w, v in zip(wt, vt)])
            m0, l0, m1, l1 = ex[0, j], ex[1, j], ex[2, j], ex[3, j]
            top = jnp.maximum(jnp.maximum(m0, m1), mt)
            f0, f1, ft = jnp.exp(m0 - top), jnp.exp(m1 - top), jnp.exp(mt - top)
            inv_l = 1.0 / (l0 * f0 + l1 * f1 + lt * ft)
            ga[j] = f0 * inv_l
            gb[j] = f1 * inv_l
            tl[j] = ot * (ft * inv_l)

    send_g = [remote(oall.at[core, hh], oall.at[core, hh], S_G, R_G + hh, partner) for hh in TWO]
    for hh in TWO:
        send_c[hh].wait_recv()
        ln = at(hh, T)
        for j in range(6):
            oall[core, hh, j] = c2[hh, 0, j] * ga[j][:, ln] + c2[hh, 1, j] * gb[j][:, ln] + tl[j][:, ln]
        send_g[hh].start()

    eye = jnp.where(lax.broadcasted_iota(jnp.int32, (B, B), 0) == lane_iota((B, B)), 1.0, 0.0)
    picks[...] = jnp.concatenate([mm_t(eye, idx[s].astype(F32)) for s in range(S)], axis=0)

    eye_e = jnp.where(lax.broadcasted_iota(jnp.int32, (E, E), 0) == lane_iota((E, E)), 1.0, 0.0).astype(BF16)
    wrt[...] = lax.dot_general(wr[...], eye_e, (((0,), (0,)), ((), ())), preferred_element_type=F32).astype(BF16)

    here = me < 4

    @pl.when(here)
    def _():
        local(wo, wo, L_WO).wait()
        att = None
        for hh in TWO:
            send_g[hh].wait_recv()
            for g in TWO:
                o_g = jnp.concatenate([oall[h, hh, 2 * s + g] for s in range(S) for h in TWO], axis=0).astype(BF16)
                part = mm(o_g, wo[g, at(hh, T)])
                att = part if att is None else att + part
        xm = (xb[...].reshape(R, D).astype(F32) + att + bo[...]).astype(BF16).astype(F32)
        for n in range(NCH):
            xm4[n] = xm[:, at(n, CW)]
        h2[...] = norm_rows(xm, g2[...], b2[...])

    def act(i):
        for n in FOUR:
            e = i * 4 + n
            raw[e] = mm(h2[...], jnp.concatenate([wg[e], wu[e]], axis=1))

    def mix(i):
        for n in FOUR:
            e = i * 4 + n
            a, up = raw[e, :, :FS], raw[e, :, FS:]
            ub[e] = (gx[e] * (a * (1.0 / (1.0 + jnp.exp(-a)))) * up).astype(BF16)

    def wait_up(sl, sem):
        for n, w in enumerate((wg, wu)):
            local(w.at[sl], w.at[sl], sem + n).wait()

    wait_up(pl.ds(0, 20), L_GU)

    @pl.when(here)
    def _():
        logits = mm(h2[...], wrt[...])
        for i in FOUR:
            act(i)
        lane_e = lane_iota((R, E)).astype(F32)
        chosen = picks[...]
        gates = jnp.zeros((R, E), F32)
        for k in EIGHT:
            on = jnp.concatenate([rm[s, :, k, :] for s in range(S)], axis=0) == 1
            mk = jnp.where(on, logits, NEG_FILL)
            pk = jnp.exp(mk - jnp.max(mk, axis=1, keepdims=True))
            pk = pk / jnp.sum(pk, axis=1, keepdims=True)
            gates = gates + jnp.where(chosen[:, k:k + 1] == lane_e, pk, 0.0)
        for e in range(E):
            gx[e] = jnp.broadcast_to(gates[:, e:e + 1], (R, 128))

        act(4)

    def down(n, first, count, width):
        u = jnp.concatenate([ub[e] for e in range(first, first + count)], axis=1)
        return mm(u, wd[first:first + count, :, n * CW:n * CW + width].reshape(count * FS, width))

    def rounded(x):
        return x.astype(BF16).astype(F32)

    send_a = [remote(pb.at[n], ab.at[n], S_P, R_P + n, partner) for n in range(NCH)]
    send_b = [remote(s2.at[n, chip], s2.at[n, chip], S_B, R_B + n, peer) for n in range(NCH)]
    send_d = [remote(pb.at[0], db.at[0], S_B, R_B + NCH, diag), remote(pb.at[0], db.at[1], S_B, R_B, peer)]
    send_last = [
        remote(s2.at[LAST, chip], s2.at[LAST, chip], S_B, R_B + LAST, diag),
        remote(s2.at[LAST, chip], s2.at[LAST, chip], S_B, R_B + LAST - 1, partner),
    ]
    send_y = [remote(yb.at[n], yb.at[n], S_P, R_P + n, partner) for n in range(NCH)]

    wait_up(pl.ds(20, 12), L_GU + 2)

    @pl.when(here)
    def _():
        for i in range(5, 8):
            act(i)
            mix(i - 5)
        for i in range(3, 7):
            mix(i)

    for m in range(3):
        down_copy(m, 0, E).wait()

        @pl.when(here)
        def _():
            if m == 0:
                mix(7)
                part = rounded(down(0, 0, E, 2 * CW))
                pb[0] = part[:, :CW]
                pb[1] = part[:, CW:]
            else:
                for h in TWO:
                    dsum[h] = down(m + 1, h * (E // 2), E // 2, CW)
                pb[m + 1] = rounded(dsum[0] + dsum[1])

        @pl.when(core == 0)
        def _():
            for n in ((0, 1) if m == 0 else (m + 1,)):
                send_a[n].start()
            if m == 0:
                send_d[0].start()

        @pl.when(core == 1)
        def _():
            if m == 0:
                send_d[1].start()
            for n in ((), (0, 1), (2, LAST))[m]:
                send_a[n].wait_recv()
                s2[n, chip] = ab[n] + pb[n]
                if n == LAST:
                    for c in send_last:
                        c.start()
                if n > 0:
                    send_b[n].start()

    def finish(n):
        yb[n] = xm4[n] + (s2[n, 0] + s2[n, 1])

    def put(n):
        hb[:, :, at(n, CW)] = yb[n].astype(BF16).reshape(S, B, CW)

    @pl.when(core == 1)
    def _():
        tails()
        for c in send_d:
            c.wait_recv()
        s2[0, 1 - chip] = db[0] + db[1]
        for n in range(NCH):
            if n > 0:
                send_b[n].wait_recv()
            finish(n)
            if n < LAST:
                send_y[n].start()
            put(n)
        for ref, snd in ((s2.at[:, chip], S_B), (s2.at[pl.ds(0, 2), chip], S_B), (yb.at[pl.ds(0, LAST)], S_P)):
            remote(ref, ref, snd, R_B, peer).wait_send()

    @pl.when(core == 0)
    def _():
        tails()
        send_d[0].wait_send()
        remote(pb, pb, S_P, R_B, peer).wait_send()
        for n in range(LAST):
            send_y[n].wait_recv()
            put(n)
        for c in send_last:
            c.wait_recv()
        finish(LAST)
        put(LAST)

    for ref, snd in ((mlall.at[pl.ds(0, 3)], S_ML), (obuf.at[1 - core], S_O), (c2.at[:, chip, pl.ds(0, 6)], S_C), (oall.at[core], S_G)):
        remote(ref, ref, snd, R_ML, partner).wait_send()


def write_kernel(h, tk, tv, h_out, tk_out, tv_out, sem):
    copies = [pltpu.make_async_copy(a, b, sem.at[i]) for i, (a, b) in enumerate(((h, h_out), (tk, tk_out), (tv, tv_out)))]
    for c in copies:
        c.start()
    for c in copies:
        c.wait()


def solution(mesh):
    def layer_steps(x_first, next_emb, k_cache, v_cache, seq_len, ln1_gain, ln1_bias, w_q, b_q, w_k, b_k, w_v, b_v, w_o, b_o, ln2_gain, ln2_bias, w_router, w_gate, w_up, w_down, long_factor, expert_idx, route_mask):
        def row(v):
            return v.reshape(1, -1)

        powers = (np.float32(ROPE_BASE) ** (np.arange(32, dtype=np.float32) * np.float32(2.0) / np.float32(HD))).astype(np.float32)
        base = jnp.asarray(np.tile(powers, 4)[None, :])
        args = (
            x_first, next_emb, jnp.transpose(k_cache, (0, 2, 3, 1)), jnp.transpose(v_cache, (0, 2, 3, 1)), seq_len,
            row(ln1_gain), row(ln1_bias), w_q, row(b_q), w_k, row(b_k), w_v, row(b_v), w_o, row(b_o), row(ln2_gain), row(ln2_bias),
            jnp.transpose(w_router), w_gate, w_up, w_down, row(long_factor), jnp.transpose(expert_idx, (0, 2, 1)), route_mask, base,
        )
        V = pltpu.VMEM
        scratch = [
            V((S, B, D), BF16), V((1, D), F32), V((1, D), F32), V((D, D), BF16), V((1, D), F32), V((D, 512), BF16), V((1, 512), F32),
            V((D, 512), BF16), V((1, 512), F32), V((2, 512, D), BF16), V((1, D), F32), V((1, D), F32), V((1, D), F32), V((E, D), BF16),
            V((E, D, FS), BF16), V((E, D, FS), BF16), V((E, FS, D), BF16), V((1, 32), F32), V((S, 8, B), jnp.int32),
            V((S, B, 8, E), jnp.int32), V((1, 128), F32), pltpu.SMEM((B,), jnp.int32), V((B, KV, HD, T), BF16), V((B, KV, HD, T), BF16),
            V((B, 8, 512), F32), V((S, B, 512), F32), V((S, B, 512), F32), V((B, 2, 32, T), F32), V((B, 2, 32, T), BF16),
            V((2, 8, 128), F32), V((4, 8, 128), F32), V((2, 2, 8, 8, 256), F32), V((2, 8, 8, 256), F32), V((2, 2, 8, 8, 256), F32),
            V((4, 8, 8, 512), F32), V((6, 8, 512), F32), V((6, 8, 512), F32), V((6, 8, 512), F32), V((2, 2, 6, 8, 256), F32),
            V((NCH, R, CW), F32), V((E, R, 128), F32), V((E, R, 2 * FS), F32), V((R, 512), F32), V((2, R, CW), F32), V((R, 8), F32), V((D, E), BF16), V((R, D), BF16), V((E, R, FS), BF16), V((NCH, R, CW), F32),
            V((NCH, R, CW), F32), V((2, R, CW), F32), V((NCH, 2, R, CW), F32), V((NCH, R, CW), F32), V((B, S, KV, HD), F32), V((B, S, KV, HD), F32),
            pltpu.SemaphoreType.DMA((NLOCAL,)), pltpu.SemaphoreType.DMA((NSEND,)), pltpu.SemaphoreType.DMA((NRECV,)),
        ]
        anyspec = pl.BlockSpec(memory_space=pl.ANY)
        outs = [((S, B, D), BF16), ((B, S, KV, HD), BF16), ((B, S, KV, HD), BF16)]
        vmem = pl.BlockSpec(memory_space=pltpu.VMEM)
        parts = pl.pallas_call(
            kernel,
            out_shape=tuple(V(*o) for o in outs),
            in_specs=[anyspec] * len(args),
            out_specs=(vmem,) * 3,
            scratch_shapes=scratch,
            compiler_params=pltpu.CompilerParams(collective_id=0, has_side_effects=True, vmem_limit_bytes=60 * 1024 * 1024),
        )(*args)
        return pl.pallas_call(
            write_kernel,
            out_shape=tuple(jax.ShapeDtypeStruct(*o) for o in outs),
            in_specs=[vmem] * 3,
            out_specs=(anyspec,) * 3,
            scratch_shapes=[pltpu.SemaphoreType.DMA((3,))],
            compiler_params=pltpu.CompilerParams(vmem_limit_bytes=1024 * 1024),
        )(*parts)

    replicated = P()
    in_specs = (P('dp'), P(None, 'dp'), P('dp', 'kv'), P('dp', 'kv'), P('dp')) + (replicated,) * 13 + (P(None, None, 'kv'), P(None, None, 'kv'), P(None, 'kv'), replicated, P(None, 'dp'), P(None, 'dp'))
    out_specs = (P(None, 'dp'), P('dp'), P('dp'))
    return jax.shard_map(layer_steps, mesh=mesh, in_specs=in_specs, out_specs=out_specs, check_vma=False)
```

```python
import functools
import itertools
import math

import jax
import jax.numpy as jnp
import numpy as np
from jax import lax
from jax.experimental import pallas as pl
from jax.experimental.pallas import tpu as pltpu
from jax.sharding import PartitionSpec as P

ROPE_BASE = 10000.0
ROPE_MSCALE = math.sqrt(1.0 + math.log(32.0) / math.log(4096.0))
NORM_EPS = 1e-5
NEG_FILL = -1e30
F32 = jnp.float32
BF16 = jnp.bfloat16

S = 3
B = 16
D = 1024
T = 256
KV = 8
HD = 64
E = 32
FS = 128
R = S * B
NCH = 4
CW = D // NCH
LAST = NCH - 1

GROUPS = 8
SMALL, PARTS = 8, 4
L_SMALL, L_WQ, L_K, L_V, L_WO, L_GU, L_DN, NLOCAL = itertools.accumulate((SMALL, 2, PARTS, PARTS, 1, PARTS, 3), initial=0)
R_ML, R_O, R_C, R_G, R_P, R_B, NRECV = itertools.accumulate((3, 2, 2, 2, NCH, NCH + 1), initial=0)
S_ML, S_O, S_C, S_G, S_P, S_B, NSEND = range(7)
LN = 128
TWO, FOUR, EIGHT = range(2), range(4), range(8)


def at(i, width=LN):
    return slice(i * width, (i + 1) * width)


def mm(a, b):
    return jnp.dot(a, b, preferred_element_type=F32)


def mm_t(a, b):
    return lax.dot_general(a, b, (((1,), (1,)), ((), ())), preferred_element_type=F32)


def norm_rows(x, gain, bias):
    mean = jnp.mean(x, axis=-1, keepdims=True)
    cen = x - mean
    var = jnp.mean(cen * cen, axis=-1, keepdims=True)
    return (cen * lax.rsqrt(var + NORM_EPS) * gain + bias).astype(BF16)


def lane_iota(shape):
    return lax.broadcasted_iota(jnp.int32, shape, len(shape) - 1)


def kernel(
    x_first, next_emb, k_hbm, v_hbm, seq_hbm, g1_h, b1_h, wq_h, bq_h, wk_h, bk_h, wv_h, bv_h, wo_h, bo_h, g2_h, b2_h,
    wr_h, wg_h, wu_h, wd_h, lf_h, idx_h, rm_h, base_h,
    hb, tkb, tvb,
    xb, g1, b1, wq, bq, wk, bk, wv, bv, wo, bo, g2, b2, wr, wg, wu, wd, lf, idx, rm, base, seq_s, kc, vc,
    qbuf, kbuf, vbuf, sbuf, wbuf, mlb, mlall, obuf, orecv, c2, ex, ga, gb, tl, oall, xm4, gx, raw, qraw, dsum, picks, wrt, h2, ub, pb, ab, db, s2, yb, tkf, tvf,
    lsem, ssem, rsem,
):
    me = lax.axis_index("kv")
    core = me % 2
    chip = me // 2
    partner = me + 1 - 2 * core
    peer = (me + 2) % 4
    diag = (partner + 2) % 4

    def local(src, dst, i):
        return pltpu.make_async_copy(src, dst, lsem.at[i])

    def remote(src, dst, snd, rcv, dev):
        return pltpu.make_async_remote_copy(
            src_ref=src, dst_ref=dst, send_sem=ssem.at[snd], recv_sem=rsem.at[rcv],
            device_id={"kv": dev}, device_id_type=pl.DeviceIdType.MESH)

    small = [
        local(src, dst, L_SMALL + i % SMALL) for i, (src, dst) in enumerate((
            (x_first, xb.at[0]), (next_emb, xb.at[pl.ds(1, S - 1)]), (g1_h, g1), (b1_h, b1), (bq_h, bq), (lf_h, lf), (base_h, base),
            (seq_hbm, seq_s), (bk_h, bk), (bv_h, bv), (bo_h, bo), (g2_h, g2), (b2_h, b2), (wr_h, wr), (idx_h, idx), (rm_h, rm)))
    ]
    first, later = small[:SMALL], small[SMALL:]
    cp_wq = [local(wq_h.at[:, pl.ds(i * 512, 512)], wq.at[:, pl.ds(i * 512, 512)], L_WQ + i) for i in TWO]
    other, own = (1 - core) * 8, core * 8

    def k_part(i):
        sl = pl.ds((other if i < 2 else own) + (i % 2) * 4, 4)
        return local(k_hbm.at[sl], kc.at[sl], L_K + i)

    def v_part(i):
        sl = (pl.ds(other if i < 2 else own, 8), pl.ds((i % 2) * 4, 4))
        return local(v_hbm.at[sl], vc.at[sl], L_V + i)

    cp_k = [k_part(i) for i in FOUR]
    cp_v = [v_part(i) for i in FOUR]
    cp_wkv = [local(wk_h, wk, L_WQ), local(wv_h, wv, L_WQ + 1)]
    cp_wo = [
        local(wo_h.at[pl.ds(kv * 128 + g * 64, 64)], wo.at[g, pl.ds(kv * 64, 64)], L_WO) for kv in range(KV) for g in TWO
    ]

    def up_copy(src, dst, i, sem):
        sl = pl.ds(i * 4, 4)
        return local(src.at[sl], dst.at[sl], sem)

    def down_copy(m, e, n):
        sl = (pl.ds(e, n), pl.ds(0, FS), pl.ds(0, 2 * CW) if m == 0 else pl.ds((m + 1) * CW, CW))
        return local(wd_h.at[sl], wd.at[sl], L_DN + m)

    for c in cp_wq[:1] + first + cp_wq[1:] + cp_k[:3] + cp_v[:1] + cp_k[3:]:
        c.start()
    bar = pltpu.get_barrier_semaphore()
    for dev in (partner, peer, diag):
        pl.semaphore_signal(bar, inc=1, device_id={"kv": dev}, device_id_type=pl.DeviceIdType.MESH)
    qbuf[:, 6:8, :] = jnp.zeros((B, 2, 512), F32)

    for c in first:
        c.wait()
    for c in cp_v[1:]:
        c.start()

    lane48 = lane_iota((R, 128))
    inv = 1.0 / (jnp.concatenate([lf[...]] * 4, axis=1) * base[...])
    row_b = lax.broadcasted_iota(jnp.int32, (B, 128), 0)
    len_rows = jnp.zeros((B, 128), jnp.int32)
    for b in range(B):
        len_rows = jnp.where(row_b == b, seq_s[b], len_rows)
    angles = jnp.concatenate([(len_rows + s).astype(F32) for s in range(S)], axis=0) * inv
    cosv = jnp.cos(angles) * ROPE_MSCALE
    sinv = jnp.sin(angles) * ROPE_MSCALE
    low_half = (lane48 % HD) < (HD // 2)

    def rope(x, both=False):
        xf = x.astype(BF16).astype(F32)
        up, down_ = pltpu.roll(xf, 96, 1), pltpu.roll(xf, 32, 1)
        plain = (xf * cosv + jnp.where(low_half, -up, down_) * sinv).astype(BF16).astype(F32)
        if not both:
            return plain
        return plain, (pltpu.roll(xf, HD, 1) * cosv + jnp.where(low_half, -down_, up) * sinv).astype(BF16).astype(F32)

    h1 = norm_rows(xb[...].reshape(R, D).astype(F32), g1[...], b1[...])

    left = lane48 < HD

    def put_q(q, p):
        qa, qa_x = rope(q[:, :LN], True)
        qb, qb_x = rope(q[:, LN:], True)
        pair = (jnp.where(left, qa, qb_x) * 0.125, jnp.where(left, qa_x, qb) * 0.125)
        for g in TWO:
            for s in range(S):
                qbuf[:, 2 * s + g, at(p)] = pair[g][at(s, B)]

    cp_wq[0].wait()
    q_lo = mm(h1, wq[:, :512]) + bq[:, :512]
    qraw[...] = q_lo
    cp_wq[1].wait()
    for c in later + cp_wo + cp_wkv:
        c.start()
    q_hi = mm(h1, wq[:, 512:]) + bq[:, 512:]
    for p in FOUR:
        put_q(qraw[:, p * 256:(p + 1) * 256] if p < 2 else q_hi[:, (p - 2) * 256:(p - 1) * 256], p)

    rowq = lax.broadcasted_iota(jnp.int32, (32, T), 0)
    laneq = lane_iota((32, T))
    diag_mask = (rowq // 8) == (laneq // HD)
    pos = laneq + me * T
    lane8 = lane_iota((8, 128))

    def scores(start, i):
        qv = qbuf[start + i]
        for hh in TWO:
            rep = jnp.concatenate([qv[:, at(hh, T)]] * 4, axis=0)
            lhs = jnp.where(diag_mask, rep, 0.0).astype(BF16)
            sbuf[start + i, hh] = mm(lhs, kc[start + i, at(hh, 4)].reshape(256, T))

    def soft(start, i, acc):
        keep = pos < seq_s[start + i]
        for hh in TWO:
            sc = jnp.where(keep, sbuf[start + i, hh], NEG_FILL)
            m = jnp.max(sc, axis=1, keepdims=True)
            w = jnp.where(keep, jnp.exp(sc - m), 0.0)
            l = jnp.sum(w, axis=1, keepdims=True)
            wbuf[start + i, hh] = w.astype(BF16)
            for j in FOUR:
                spot = i * 16 + hh * 4 + j
                acc = jnp.where(lane8 == spot, m[at(j, 8)], acc)
                acc = jnp.where(lane8 == spot + 8, l[at(j, 8)], acc)
        return acc

    left8 = lane8 < HD

    def values(half, i, hh):
        b = half * 8 + i
        pv = mm_t(wbuf[b, hh], vc[b, at(hh, 4)].reshape(256, T))
        obuf[half, hh, i, :, 0:128] = jnp.where(left8, pv[0:8, 0:128], pv[8:16, 0:128])
        obuf[half, hh, i, :, 128:256] = jnp.where(left8, pv[16:24, 128:256], pv[24:32, 128:256])

    send_ml = [
        remote(mlb.at[1 - core], mlall.at[me], S_ML, R_ML, partner), remote(mlb.at[core], mlall.at[me], S_ML, R_ML + 1, peer),
        remote(mlb.at[1 - core], mlall.at[me], S_ML, R_ML + 2, diag),
    ]
    send_o = [remote(obuf.at[1 - core, hh], orecv.at[hh], S_O, R_O + hh, partner) for hh in TWO]
    zero = jnp.zeros((8, 128), F32)

    cp_k[0].wait()
    for i in FOUR:
        scores(other, i)
    cp_k[1].wait()
    for i in FOUR:
        scores(other, 4 + i)
    acc = zero
    for i in FOUR:
        acc = soft(other, i, acc)
    cp_k[2].wait()
    for i in range(GROUPS):
        sem = L_GU + 2 * (i // 5)
        up_copy(wg_h, wg, i, sem).start()
        up_copy(wu_h, wu, i, sem + 1).start()
    for i in FOUR:
        scores(own, i)
    for i in FOUR:
        acc = soft(other, 4 + i, acc)
    mlb[1 - core] = acc
    pl.semaphore_wait(bar, 3)
    send_ml[0].start()
    send_ml[2].start()

    cp_v[0].wait()
    for i in EIGHT:
        values(1 - core, i, 0)
    acc = zero
    for i in FOUR:
        acc = soft(own, i, acc)
    send_o[0].start()
    cp_k[3].wait()
    for i in FOUR:
        scores(own, 4 + i)
    cp_v[1].wait()
    for m in range(3):
        for i in range(GROUPS):
            down_copy(m, i * 4, 4).start()
    for i in EIGHT:
        values(1 - core, i, 1)
    for i in FOUR:
        acc = soft(own, 4 + i, acc)
    mlb[core] = acc
    mlall[me] = acc
    send_o[1].start()
    send_ml[1].start()
    cp_v[2].wait()
    for i in EIGHT:
        values(core, i, 0)

    pick = (lane8 // HD)

    def spread(v, i, p):
        return jnp.take_along_axis(v, pick + (i * 16 + 2 * p), axis=1, mode="promise_in_bounds")

    send_c = [remote(c2.at[hh, chip, pl.ds(0, 6)], c2.at[hh, chip, pl.ds(0, 6)], S_C, R_C + hh, peer) for hh in TWO]
    for hh in TWO:
        if hh == 1:
            cp_v[3].wait()
            for i in EIGHT:
                values(core, i, 1)
        else:
            send_ml[0].wait_recv()
            ml_a = mlall[me]
            ml_b = mlall[partner]
            m_ab = jnp.maximum(ml_a, ml_b)
            f_a = jnp.exp(ml_a - m_ab)
            f_b = jnp.exp(ml_b - m_ab)
        send_o[hh].wait_recv()
        for i in EIGHT:
            oa = obuf[core, hh, i]
            ob = orecv[hh, i]
            for p in TWO:
                ln = at(p)
                c2[hh, chip, :, i, ln] = (
                    oa[:, ln] * spread(f_a, i, 2 * hh + p) + ob[:, ln] * spread(f_b, i, 2 * hh + p))
        send_c[hh].start()

    for c in later + cp_wkv:
        c.wait()
    for c in send_ml[1:]:
        c.wait_recv()
    kn = mm(h1, wk[...]) + bk[...]
    vn = (mm(h1, wv[...]) + bv[...]).astype(BF16)
    vn = vn.astype(F32)
    for p in FOUR:
        ln = at(p)
        for val, buf in ((rope(kn[:, ln]), kbuf), (vn[:, ln], vbuf)):
            for s in range(S):
                buf[s, :, ln] = val[at(s, B)]

    def tails():
        for buf, fin, out in ((kbuf, tkf, tkb), (vbuf, tvf, tvb)):
            for p in FOUR:
                for s in range(S):
                    val = buf[s, :, at(p)]
                    fin[:, s, 2 * p, :] = val[:, :HD]
                    fin[:, s, 2 * p + 1, :] = pltpu.roll(val, HD, 1)[:, :HD]
            out[...] = fin[...].astype(BF16)

    rows = pl.ds(pl.multiple_of(core * 8, 8), 8)
    kt = [kbuf[t, rows, :] for t in range(S)]
    vt = [vbuf[t, rows, :] for t in range(S)]
    trip = [(s, g, t) for s in range(S) for g in TWO for t in range(s + 1)]
    prod = jnp.concatenate([qbuf[rows, 2 * s + g, :] * kt[t] for s, g, t in trip], axis=0)
    hi = prod.astype(BF16)
    lo = (prod - hi.astype(F32)).astype(BF16)
    r2 = lax.broadcasted_iota(jnp.int32, (256, 128), 0)
    ones = jnp.where(((r2 % 128) // HD) == (lane_iota((256, 128)) // HD), 1.0, 0.0).astype(BF16)
    tsc = jnp.concatenate(
        [mm(jnp.concatenate([hi[:, at(p)], lo[:, at(p)]], axis=1), ones) for p in FOUR], axis=1)

    ml = [mlall[d] for d in FOUR]
    for ch in TWO:
        a, b_ = ml[2 * ch], ml[2 * ch + 1]
        mc = jnp.maximum(a, b_)
        lc = (pltpu.roll(a, 120, 1) * jnp.exp(a - mc) + pltpu.roll(b_, 120, 1) * jnp.exp(b_ - mc))
        for i in EIGHT:
            for p in FOUR:
                ln = at(p)
                ex[2 * ch, :, i, ln] = spread(mc, i, p)
                ex[2 * ch + 1, :, i, ln] = spread(lc, i, p)

    for s in range(S):
        for g in TWO:
            j = 2 * s + g
            sc = [tsc[at(n, 8)] for n, key in enumerate(trip) if key[:2] == (s, g)]
            mt = functools.reduce(jnp.maximum, sc)
            wt = [jnp.exp(v - mt) for v in sc]
            lt = functools.reduce(jnp.add, wt)
            ot = functools.reduce(jnp.add, [w.astype(BF16).astype(F32) * v for w, v in zip(wt, vt)])
            m0, l0, m1, l1 = ex[0, j], ex[1, j], ex[2, j], ex[3, j]
            top = jnp.maximum(jnp.maximum(m0, m1), mt)
            f0, f1, ft = jnp.exp(m0 - top), jnp.exp(m1 - top), jnp.exp(mt - top)
            inv_l = 1.0 / (l0 * f0 + l1 * f1 + lt * ft)
            ga[j] = f0 * inv_l
            gb[j] = f1 * inv_l
            tl[j] = ot * (ft * inv_l)

    send_g = [remote(oall.at[core, hh], oall.at[core, hh], S_G, R_G + hh, partner) for hh in TWO]
    for hh in TWO:
        send_c[hh].wait_recv()
        ln = at(hh, T)
        for j in range(6):
            oall[core, hh, j] = c2[hh, 0, j] * ga[j][:, ln] + c2[hh, 1, j] * gb[j][:, ln] + tl[j][:, ln]
        send_g[hh].start()

    eye = jnp.where(lax.broadcasted_iota(jnp.int32, (B, B), 0) == lane_iota((B, B)), 1.0, 0.0)
    picks[...] = jnp.concatenate([mm_t(eye, idx[s].astype(F32)) for s in range(S)], axis=0)

    eye_e = jnp.where(lax.broadcasted_iota(jnp.int32, (E, E), 0) == lane_iota((E, E)), 1.0, 0.0).astype(BF16)
    wrt[...] = lax.dot_general(wr[...], eye_e, (((0,), (0,)), ((), ())), preferred_element_type=F32).astype(BF16)

    here = me < 4

    @pl.when(here)
    def _():
        local(wo, wo, L_WO).wait()
        att = None
        for hh in TWO:
            send_g[hh].wait_recv()
            for g in TWO:
                o_g = jnp.concatenate([oall[h, hh, 2 * s + g] for s in range(S) for h in TWO], axis=0).astype(BF16)
                part = mm(o_g, wo[g, at(hh, T)])
                att = part if att is None else att + part
        xm = (xb[...].reshape(R, D).astype(F32) + att + bo[...]).astype(BF16).astype(F32)
        for n in range(NCH):
            xm4[n] = xm[:, at(n, CW)]
        h2[...] = norm_rows(xm, g2[...], b2[...])

    def act(i):
        for n in FOUR:
            e = i * 4 + n
            raw[e] = mm(h2[...], jnp.concatenate([wg[e], wu[e]], axis=1))

    def mix(i):
        for n in FOUR:
            e = i * 4 + n
            a, up = raw[e, :, :FS], raw[e, :, FS:]
            ub[e] = (gx[e] * (a * (1.0 / (1.0 + jnp.exp(-a)))) * up).astype(BF16)

    def wait_up(sl, sem):
        for n, w in enumerate((wg, wu)):
            local(w.at[sl], w.at[sl], sem + n).wait()

    wait_up(pl.ds(0, 20), L_GU)

    @pl.when(here)
    def _():
        logits = mm(h2[...], wrt[...])
        for i in FOUR:
            act(i)
        lane_e = lane_iota((R, E)).astype(F32)
        chosen = picks[...]
        gates = jnp.zeros((R, E), F32)
        for k in EIGHT:
            on = jnp.concatenate([rm[s, :, k, :] for s in range(S)], axis=0) == 1
            mk = jnp.where(on, logits, NEG_FILL)
            pk = jnp.exp(mk - jnp.max(mk, axis=1, keepdims=True))
            pk = pk / jnp.sum(pk, axis=1, keepdims=True)
            gates = gates + jnp.where(chosen[:, k:k + 1] == lane_e, pk, 0.0)
        for e in range(E):
            gx[e] = jnp.broadcast_to(gates[:, e:e + 1], (R, 128))

        act(4)

    def down(n, first, count, width):
        u = jnp.concatenate([ub[e] for e in range(first, first + count)], axis=1)
        return mm(u, wd[first:first + count, :, n * CW:n * CW + width].reshape(count * FS, width))

    def rounded(x):
        return x.astype(BF16).astype(F32)

    send_a = [remote(pb.at[n], ab.at[n], S_P, R_P + n, partner) for n in range(NCH)]
    send_b = [remote(s2.at[n, chip], s2.at[n, chip], S_B, R_B + n, peer) for n in range(NCH)]
    send_d = [remote(pb.at[0], db.at[0], S_B, R_B + NCH, diag), remote(pb.at[0], db.at[1], S_B, R_B, peer)]
    send_last = [
        remote(s2.at[LAST, chip], s2.at[LAST, chip], S_B, R_B + LAST, diag),
        remote(s2.at[LAST, chip], s2.at[LAST, chip], S_B, R_B + LAST - 1, partner),
    ]
    send_y = [remote(yb.at[n], yb.at[n], S_P, R_P + n, partner) for n in range(NCH)]

    wait_up(pl.ds(20, 12), L_GU + 2)

    @pl.when(here)
    def _():
        for i in range(5, 8):
            act(i)
            mix(i - 5)
        for i in range(3, 7):
            mix(i)

    for m in range(3):
        down_copy(m, 0, E).wait()

        @pl.when(here)
        def _():
            if m == 0:
                mix(7)
                part = rounded(down(0, 0, E, 2 * CW))
                pb[0] = part[:, :CW]
                pb[1] = part[:, CW:]
            else:
                for h in TWO:
                    dsum[h] = down(m + 1, h * (E // 2), E // 2, CW)
                pb[m + 1] = rounded(dsum[0] + dsum[1])

        @pl.when(core == 0)
        def _():
            for n in ((0, 1) if m == 0 else (m + 1,)):
                send_a[n].start()
            if m == 0:
                send_d[0].start()

        @pl.when(core == 1)
        def _():
            if m == 0:
                send_d[1].start()
            for n in ((), (0, 1), (2, LAST))[m]:
                send_a[n].wait_recv()
                s2[n, chip] = ab[n] + pb[n]
                if n == LAST:
                    for c in send_last:
                        c.start()
                if n > 0:
                    send_b[n].start()

    def finish(n):
        yb[n] = xm4[n] + (s2[n, 0] + s2[n, 1])

    def put(n):
        hb[:, :, at(n, CW)] = yb[n].astype(BF16).reshape(S, B, CW)

    @pl.when(core == 1)
    def _():
        tails()
        for c in send_d:
            c.wait_recv()
        s2[0, 1 - chip] = db[0] + db[1]
        for n in range(NCH):
            if n > 0:
                send_b[n].wait_recv()
            finish(n)
            if n < LAST:
                send_y[n].start()
            put(n)
        for ref, snd in ((s2.at[:, chip], S_B), (s2.at[pl.ds(0, 2), chip], S_B), (yb.at[pl.ds(0, LAST)], S_P)):
            remote(ref, ref, snd, R_B, peer).wait_send()

    @pl.when(core == 0)
    def _():
        tails()
        send_d[0].wait_send()
        remote(pb, pb, S_P, R_B, peer).wait_send()
        for n in range(LAST):
            send_y[n].wait_recv()
            put(n)
        for c in send_last:
            c.wait_recv()
        finish(LAST)
        put(LAST)

    for ref, snd in ((mlall.at[pl.ds(0, 3)], S_ML), (obuf.at[1 - core], S_O), (c2.at[:, chip, pl.ds(0, 6)], S_C), (oall.at[core], S_G)):
        remote(ref, ref, snd, R_ML, partner).wait_send()


def write_kernel(h, tk, tv, h_out, tk_out, tv_out, sem):
    copies = [pltpu.make_async_copy(a, b, sem.at[i]) for i, (a, b) in enumerate(((h, h_out), (tk, tk_out), (tv, tv_out)))]
    for c in copies:
        c.start()
    for c in copies:
        c.wait()


def solution(mesh):
    def layer_steps(x_first, next_emb, k_cache, v_cache, seq_len, ln1_gain, ln1_bias, w_q, b_q, w_k, b_k, w_v, b_v, w_o, b_o, ln2_gain, ln2_bias, w_router, w_gate, w_up, w_down, long_factor, expert_idx, route_mask):
        def row(v):
            return v.reshape(1, -1)

        powers = (np.float32(ROPE_BASE) ** (np.arange(32, dtype=np.float32) * np.float32(2.0) / np.float32(HD))).astype(np.float32)
        base = jnp.asarray(np.tile(powers, 4)[None, :])
        args = (
            x_first, next_emb, jnp.transpose(k_cache, (0, 2, 3, 1)), jnp.transpose(v_cache, (0, 2, 3, 1)), seq_len,
            row(ln1_gain), row(ln1_bias), w_q, row(b_q), w_k, row(b_k), w_v, row(b_v), w_o, row(b_o), row(ln2_gain), row(ln2_bias),
            jnp.transpose(w_router), w_gate, w_up, w_down, row(long_factor), jnp.transpose(expert_idx, (0, 2, 1)), route_mask, base,
        )
        V = pltpu.VMEM
        scratch = [
            V((S, B, D), BF16), V((1, D), F32), V((1, D), F32), V((D, D), BF16), V((1, D), F32), V((D, 512), BF16), V((1, 512), F32),
            V((D, 512), BF16), V((1, 512), F32), V((2, 512, D), BF16), V((1, D), F32), V((1, D), F32), V((1, D), F32), V((E, D), BF16),
            V((E, D, FS), BF16), V((E, D, FS), BF16), V((E, FS, D), BF16), V((1, 32), F32), V((S, 8, B), jnp.int32),
            V((S, B, 8, E), jnp.int32), V((1, 128), F32), pltpu.SMEM((B,), jnp.int32), V((B, KV, HD, T), BF16), V((B, KV, HD, T), BF16),
            V((B, 8, 512), F32), V((S, B, 512), F32), V((S, B, 512), F32), V((B, 2, 32, T), F32), V((B, 2, 32, T), BF16),
            V((2, 8, 128), F32), V((4, 8, 128), F32), V((2, 2, 8, 8, 256), F32), V((2, 8, 8, 256), F32), V((2, 2, 8, 8, 256), F32),
            V((4, 8, 8, 512), F32), V((6, 8, 512), F32), V((6, 8, 512), F32), V((6, 8, 512), F32), V((2, 2, 6, 8, 256), F32),
            V((NCH, R, CW), F32), V((E, R, 128), F32), V((E, R, 2 * FS), F32), V((R, 512), F32), V((2, R, CW), F32), V((R, 8), F32), V((D, E), BF16), V((R, D), BF16), V((E, R, FS), BF16), V((NCH, R, CW), F32),
            V((NCH, R, CW), F32), V((2, R, CW), F32), V((NCH, 2, R, CW), F32), V((NCH, R, CW), F32), V((B, S, KV, HD), F32), V((B, S, KV, HD), F32),
            pltpu.SemaphoreType.DMA((NLOCAL,)), pltpu.SemaphoreType.DMA((NSEND,)), pltpu.SemaphoreType.DMA((NRECV,)),
        ]
        anyspec = pl.BlockSpec(memory_space=pl.ANY)
        outs = [((S, B, D), BF16), ((B, S, KV, HD), BF16), ((B, S, KV, HD), BF16)]
        vmem = pl.BlockSpec(memory_space=pltpu.VMEM)
        parts = pl.pallas_call(
            kernel,
            out_shape=tuple(V(*o) for o in outs),
            in_specs=[anyspec] * len(args),
            out_specs=(vmem,) * 3,
            scratch_shapes=scratch,
            compiler_params=pltpu.CompilerParams(collective_id=0, has_side_effects=True, vmem_limit_bytes=60 * 1024 * 1024),
        )(*args)
        return pl.pallas_call(
            write_kernel,
            out_shape=tuple(jax.ShapeDtypeStruct(*o) for o in outs),
            in_specs=[vmem] * 3,
            out_specs=(anyspec,) * 3,
            scratch_shapes=[pltpu.SemaphoreType.DMA((3,))],
            compiler_params=pltpu.CompilerParams(vmem_limit_bytes=1024 * 1024),
        )(*parts)

    replicated = P()
    in_specs = (P('dp'), P(None, 'dp'), P('dp', 'kv'), P('dp', 'kv'), P('dp')) + (replicated,) * 13 + (P(None, None, 'kv'), P(None, None, 'kv'), P(None, 'kv'), replicated, P(None, 'dp'), P(None, 'dp'))
    out_specs = (P(None, 'dp'), P('dp'), P('dp'))
    return jax.shard_map(layer_steps, mesh=mesh, in_specs=in_specs, out_specs=out_specs, check_vma=False)
```

```python
import functools
import itertools
import math

import jax
import jax.numpy as jnp
import numpy as np
from jax import lax
from jax.experimental import pallas as pl
from jax.experimental.pallas import tpu as pltpu
from jax.sharding import PartitionSpec as P

ROPE_BASE = 10000.0
ROPE_MSCALE = math.sqrt(1.0 + math.log(32.0) / math.log(4096.0))
NORM_EPS = 1e-5
NEG_FILL = -1e30
F32 = jnp.float32
BF16 = jnp.bfloat16

S = 3
B = 16
D = 1024
T = 256
KV = 8
HD = 64
E = 32
FS = 128
R = S * B
NCH = 4
CW = D // NCH
LAST = NCH - 1

GROUPS = 8
SMALL, PARTS = 8, 4
L_SMALL, L_WQ, L_K, L_V, L_WO, L_GU, L_DN, NLOCAL = itertools.accumulate((SMALL, 2, PARTS, PARTS, 1, PARTS, NCH), initial=0)
R_ML, R_O, R_C, R_G, R_P, R_B, NRECV = itertools.accumulate((3, 2, 2, 2, NCH, NCH + 1), initial=0)
S_ML, S_O, S_C, S_G, S_P, S_B, NSEND = range(7)
LN = 128
TWO, FOUR, EIGHT = range(2), range(4), range(8)


def at(i, width=LN):
    return slice(i * width, (i + 1) * width)


def mm(a, b):
    return jnp.dot(a, b, preferred_element_type=F32)


def mm_t(a, b):
    return lax.dot_general(a, b, (((1,), (1,)), ((), ())), preferred_element_type=F32)


def norm_rows(x, gain, bias):
    mean = jnp.mean(x, axis=-1, keepdims=True)
    cen = x - mean
    var = jnp.mean(cen * cen, axis=-1, keepdims=True)
    return (cen * lax.rsqrt(var + NORM_EPS) * gain + bias).astype(BF16)


def lane_iota(shape):
    return lax.broadcasted_iota(jnp.int32, shape, len(shape) - 1)


def kernel(
    x_first, next_emb, k_hbm, v_hbm, seq_hbm, g1_h, b1_h, wq_h, bq_h, wk_h, bk_h, wv_h, bv_h, wo_h, bo_h, g2_h, b2_h,
    wr_h, wg_h, wu_h, wd_h, lf_h, idx_h, rm_h, base_h,
    hb, tkb, tvb,
    xb, g1, b1, wq, bq, wk, bk, wv, bv, wo, bo, g2, b2, wr, wg, wu, wd, lf, idx, rm, base, seq_s, kc, vc,
    qbuf, kbuf, vbuf, sbuf, wbuf, mlb, mlall, obuf, orecv, c2, ex, ga, gb, tl, oall, xm4, gx, raw, qraw, dsum, picks, wrt, h2, ub, pb, ab, db, s2, yb, tkf, tvf,
    lsem, ssem, rsem,
):
    me = lax.axis_index("kv")
    core = me % 2
    chip = me // 2
    partner = me + 1 - 2 * core
    peer = (me + 2) % 4
    diag = (partner + 2) % 4

    def local(src, dst, i):
        return pltpu.make_async_copy(src, dst, lsem.at[i])

    def remote(src, dst, snd, rcv, dev):
        return pltpu.make_async_remote_copy(
            src_ref=src, dst_ref=dst, send_sem=ssem.at[snd], recv_sem=rsem.at[rcv],
            device_id={"kv": dev}, device_id_type=pl.DeviceIdType.MESH)

    small = [
        local(src, dst, L_SMALL + i % SMALL) for i, (src, dst) in enumerate((
            (x_first, xb.at[0]), (next_emb, xb.at[pl.ds(1, S - 1)]), (g1_h, g1), (b1_h, b1), (bq_h, bq), (lf_h, lf), (base_h, base),
            (seq_hbm, seq_s), (bk_h, bk), (bv_h, bv), (bo_h, bo), (g2_h, g2), (b2_h, b2), (wr_h, wr), (idx_h, idx), (rm_h, rm)))
    ]
    first, later = small[:SMALL], small[SMALL:]
    cp_wq = [local(wq_h.at[:, pl.ds(i * 512, 512)], wq.at[:, pl.ds(i * 512, 512)], L_WQ + i) for i in TWO]
    other, own = (1 - core) * 8, core * 8

    def k_part(i):
        sl = pl.ds((other if i < 2 else own) + (i % 2) * 4, 4)
        return local(k_hbm.at[sl], kc.at[sl], L_K + i)

    def v_part(i):
        sl = (pl.ds(other if i < 2 else own, 8), pl.ds((i % 2) * 4, 4))
        return local(v_hbm.at[sl], vc.at[sl], L_V + i)

    cp_k = [k_part(i) for i in FOUR]
    cp_v = [v_part(i) for i in FOUR]
    cp_wkv = [local(wk_h, wk, L_WQ), local(wv_h, wv, L_WQ + 1)]
    cp_wo = [
        local(wo_h.at[pl.ds(kv * 128 + g * 64, 64)], wo.at[g, pl.ds(kv * 64, 64)], L_WO) for kv in range(KV) for g in TWO
    ]

    def up_copy(src, dst, i, sem):
        sl = pl.ds(i * 4, 4)
        return local(src.at[sl], dst.at[sl], sem)

    def down_copy(m, e, n):
        sl = (pl.ds(e, n), pl.ds(0, FS), pl.ds(m * CW, CW))
        return local(wd_h.at[sl], wd.at[sl], L_DN + m)

    for c in first + cp_wq + cp_k[:3] + cp_v[:1] + cp_k[3:]:
        c.start()
    bar = pltpu.get_barrier_semaphore()
    for dev in (partner, peer, diag):
        pl.semaphore_signal(bar, inc=1, device_id={"kv": dev}, device_id_type=pl.DeviceIdType.MESH)
    qbuf[:, 6:8, :] = jnp.zeros((B, 2, 512), F32)

    for c in first:
        c.wait()
    for c in cp_v[1:]:
        c.start()

    lane48 = lane_iota((R, 128))
    inv = 1.0 / (jnp.concatenate([lf[...]] * 4, axis=1) * base[...])
    row_b = lax.broadcasted_iota(jnp.int32, (B, 128), 0)
    len_rows = jnp.zeros((B, 128), jnp.int32)
    for b in range(B):
        len_rows = jnp.where(row_b == b, seq_s[b], len_rows)
    angles = jnp.concatenate([(len_rows + s).astype(F32) for s in range(S)], axis=0) * inv
    cosv = jnp.cos(angles) * ROPE_MSCALE
    sinv = jnp.sin(angles) * ROPE_MSCALE
    low_half = (lane48 % HD) < (HD // 2)

    def rope(x, both=False):
        xf = x.astype(BF16).astype(F32)
        up, down_ = pltpu.roll(xf, 96, 1), pltpu.roll(xf, 32, 1)
        plain = (xf * cosv + jnp.where(low_half, -up, down_) * sinv).astype(BF16).astype(F32)
        if not both:
            return plain
        return plain, (pltpu.roll(xf, HD, 1) * cosv + jnp.where(low_half, -down_, up) * sinv).astype(BF16).astype(F32)

    h1 = norm_rows(xb[...].reshape(R, D).astype(F32), g1[...], b1[...])

    left = lane48 < HD

    def put_q(q, p):
        qa, qa_x = rope(q[:, :LN], True)
        qb, qb_x = rope(q[:, LN:], True)
        pair = (jnp.where(left, qa, qb_x) * 0.125, jnp.where(left, qa_x, qb) * 0.125)
        for g in TWO:
            for s in range(S):
                qbuf[:, 2 * s + g, at(p)] = pair[g][at(s, B)]

    cp_wq[0].wait()
    q_lo = mm(h1, wq[:, :512]) + bq[:, :512]
    qraw[...] = q_lo
    cp_wq[1].wait()
    for c in later + cp_wo + cp_wkv:
        c.start()
    q_hi = mm(h1, wq[:, 512:]) + bq[:, 512:]
    for p in FOUR:
        put_q(qraw[:, p * 256:(p + 1) * 256] if p < 2 else q_hi[:, (p - 2) * 256:(p - 1) * 256], p)

    rowq = lax.broadcasted_iota(jnp.int32, (32, T), 0)
    laneq = lane_iota((32, T))
    diag_mask = (rowq // 8) == (laneq // HD)
    pos = laneq + me * T
    lane8 = lane_iota((8, 128))

    def scores(start, i):
        qv = qbuf[start + i]
        for hh in TWO:
            rep = jnp.concatenate([qv[:, at(hh, T)]] * 4, axis=0)
            lhs = jnp.where(diag_mask, rep, 0.0).astype(BF16)
            sbuf[start + i, hh] = mm(lhs, kc[start + i, at(hh, 4)].reshape(256, T))

    def soft(start, i, acc):
        keep = pos < seq_s[start + i]
        for hh in TWO:
            sc = jnp.where(keep, sbuf[start + i, hh], NEG_FILL)
            m = jnp.max(sc, axis=1, keepdims=True)
            w = jnp.where(keep, jnp.exp(sc - m), 0.0)
            l = jnp.sum(w, axis=1, keepdims=True)
            wbuf[start + i, hh] = w.astype(BF16)
            for j in FOUR:
                spot = i * 16 + hh * 4 + j
                acc = jnp.where(lane8 == spot, m[at(j, 8)], acc)
                acc = jnp.where(lane8 == spot + 8, l[at(j, 8)], acc)
        return acc

    left8 = lane8 < HD

    def values(half, i, hh):
        b = half * 8 + i
        pv = mm_t(wbuf[b, hh], vc[b, at(hh, 4)].reshape(256, T))
        obuf[half, hh, i, :, 0:128] = jnp.where(left8, pv[0:8, 0:128], pv[8:16, 0:128])
        obuf[half, hh, i, :, 128:256] = jnp.where(left8, pv[16:24, 128:256], pv[24:32, 128:256])

    send_ml = [
        remote(mlb.at[1 - core], mlall.at[me], S_ML, R_ML, partner), remote(mlb.at[core], mlall.at[me], S_ML, R_ML + 1, peer),
        remote(mlb.at[1 - core], mlall.at[me], S_ML, R_ML + 2, diag),
    ]
    send_o = [remote(obuf.at[1 - core, hh], orecv.at[hh], S_O, R_O + hh, partner) for hh in TWO]
    zero = jnp.zeros((8, 128), F32)

    cp_k[0].wait()
    for i in FOUR:
        scores(other, i)
    cp_k[1].wait()
    for i in FOUR:
        scores(other, 4 + i)
    acc = zero
    for i in FOUR:
        acc = soft(other, i, acc)
    cp_k[2].wait()
    for i in range(GROUPS):
        sem = L_GU + 2 * (i // 5)
        up_copy(wg_h, wg, i, sem).start()
        up_copy(wu_h, wu, i, sem + 1).start()
    for i in FOUR:
        scores(own, i)
    for i in FOUR:
        acc = soft(other, 4 + i, acc)
    mlb[1 - core] = acc
    pl.semaphore_wait(bar, 3)
    send_ml[0].start()
    send_ml[2].start()

    cp_v[0].wait()
    for i in EIGHT:
        values(1 - core, i, 0)
    acc = zero
    for i in FOUR:
        acc = soft(own, i, acc)
    send_o[0].start()
    cp_k[3].wait()
    for i in FOUR:
        scores(own, 4 + i)
    cp_v[1].wait()
    for m in range(NCH):
        for i in range(GROUPS):
            down_copy(m, i * 4, 4).start()
    for i in EIGHT:
        values(1 - core, i, 1)
    for i in FOUR:
        acc = soft(own, 4 + i, acc)
    mlb[core] = acc
    mlall[me] = acc
    send_o[1].start()
    send_ml[1].start()
    cp_v[2].wait()
    for i in EIGHT:
        values(core, i, 0)

    pick = (lane8 // HD)

    def spread(v, i, p):
        return jnp.take_along_axis(v, pick + (i * 16 + 2 * p), axis=1, mode="promise_in_bounds")

    send_c = [remote(c2.at[hh, chip, pl.ds(0, 6)], c2.at[hh, chip, pl.ds(0, 6)], S_C, R_C + hh, peer) for hh in TWO]
    for hh in TWO:
        if hh == 1:
            cp_v[3].wait()
            for i in EIGHT:
                values(core, i, 1)
        else:
            send_ml[0].wait_recv()
            ml_a = mlall[me]
            ml_b = mlall[partner]
            m_ab = jnp.maximum(ml_a, ml_b)
            f_a = jnp.exp(ml_a - m_ab)
            f_b = jnp.exp(ml_b - m_ab)
        send_o[hh].wait_recv()
        for i in EIGHT:
            oa = obuf[core, hh, i]
            ob = orecv[hh, i]
            for p in TWO:
                ln = at(p)
                c2[hh, chip, :, i, ln] = (
                    oa[:, ln] * spread(f_a, i, 2 * hh + p) + ob[:, ln] * spread(f_b, i, 2 * hh + p))
        send_c[hh].start()

    for c in later + cp_wkv:
        c.wait()
    for c in send_ml[1:]:
        c.wait_recv()
    kn = mm(h1, wk[...]) + bk[...]
    vn = (mm(h1, wv[...]) + bv[...]).astype(BF16)
    vn = vn.astype(F32)
    for p in FOUR:
        ln = at(p)
        for val, buf in ((rope(kn[:, ln]), kbuf), (vn[:, ln], vbuf)):
            for s in range(S):
                buf[s, :, ln] = val[at(s, B)]

    def tails():
        for buf, fin, out in ((kbuf, tkf, tkb), (vbuf, tvf, tvb)):
            for p in FOUR:
                for s in range(S):
                    val = buf[s, :, at(p)]
                    fin[:, s, 2 * p, :] = val[:, :HD]
                    fin[:, s, 2 * p + 1, :] = pltpu.roll(val, HD, 1)[:, :HD]
            out[...] = fin[...].astype(BF16)

    rows = pl.ds(pl.multiple_of(core * 8, 8), 8)
    kt = [kbuf[t, rows, :] for t in range(S)]
    vt = [vbuf[t, rows, :] for t in range(S)]
    trip = [(s, g, t) for s in range(S) for g in TWO for t in range(s + 1)]
    prod = jnp.concatenate([qbuf[rows, 2 * s + g, :] * kt[t] for s, g, t in trip], axis=0)
    hi = prod.astype(BF16)
    lo = (prod - hi.astype(F32)).astype(BF16)
    r2 = lax.broadcasted_iota(jnp.int32, (256, 128), 0)
    ones = jnp.where(((r2 % 128) // HD) == (lane_iota((256, 128)) // HD), 1.0, 0.0).astype(BF16)
    tsc = jnp.concatenate(
        [mm(jnp.concatenate([hi[:, at(p)], lo[:, at(p)]], axis=1), ones) for p in FOUR], axis=1)

    ml = [mlall[d] for d in FOUR]
    for ch in TWO:
        a, b_ = ml[2 * ch], ml[2 * ch + 1]
        mc = jnp.maximum(a, b_)
        lc = (pltpu.roll(a, 120, 1) * jnp.exp(a - mc) + pltpu.roll(b_, 120, 1) * jnp.exp(b_ - mc))
        for i in EIGHT:
            for p in FOUR:
                ln = at(p)
                ex[2 * ch, :, i, ln] = spread(mc, i, p)
                ex[2 * ch + 1, :, i, ln] = spread(lc, i, p)

    for s in range(S):
        for g in TWO:
            j = 2 * s + g
            sc = [tsc[at(n, 8)] for n, key in enumerate(trip) if key[:2] == (s, g)]
            mt = functools.reduce(jnp.maximum, sc)
            wt = [jnp.exp(v - mt) for v in sc]
            lt = functools.reduce(jnp.add, wt)
            ot = functools.reduce(jnp.add, [w.astype(BF16).astype(F32) * v for w, v in zip(wt, vt)])
            m0, l0, m1, l1 = ex[0, j], ex[1, j], ex[2, j], ex[3, j]
            top = jnp.maximum(jnp.maximum(m0, m1), mt)
            f0, f1, ft = jnp.exp(m0 - top), jnp.exp(m1 - top), jnp.exp(mt - top)
            inv_l = 1.0 / (l0 * f0 + l1 * f1 + lt * ft)
            ga[j] = f0 * inv_l
            gb[j] = f1 * inv_l
            tl[j] = ot * (ft * inv_l)

    send_g = [remote(oall.at[core, hh], oall.at[core, hh], S_G, R_G + hh, partner) for hh in TWO]
    for hh in TWO:
        send_c[hh].wait_recv()
        ln = at(hh, T)
        for j in range(6):
            oall[core, hh, j] = c2[hh, 0, j] * ga[j][:, ln] + c2[hh, 1, j] * gb[j][:, ln] + tl[j][:, ln]
        send_g[hh].start()

    eye = jnp.where(lax.broadcasted_iota(jnp.int32, (B, B), 0) == lane_iota((B, B)), 1.0, 0.0)
    picks[...] = jnp.concatenate([mm_t(eye, idx[s].astype(F32)) for s in range(S)], axis=0)

    eye_e = jnp.where(lax.broadcasted_iota(jnp.int32, (E, E), 0) == lane_iota((E, E)), 1.0, 0.0).astype(BF16)
    wrt[...] = lax.dot_general(wr[...], eye_e, (((0,), (0,)), ((), ())), preferred_element_type=F32).astype(BF16)

    here = me < 4

    @pl.when(here)
    def _():
        local(wo, wo, L_WO).wait()
        att = None
        for hh in TWO:
            send_g[hh].wait_recv()
            for g in TWO:
                o_g = jnp.concatenate([oall[h, hh, 2 * s + g] for s in range(S) for h in TWO], axis=0).astype(BF16)
                part = mm(o_g, wo[g, at(hh, T)])
                att = part if att is None else att + part
        xm = (xb[...].reshape(R, D).astype(F32) + att + bo[...]).astype(BF16).astype(F32)
        for n in range(NCH):
            xm4[n] = xm[:, at(n, CW)]
        h2[...] = norm_rows(xm, g2[...], b2[...])

    def act(i):
        for n in FOUR:
            e = i * 4 + n
            raw[e] = mm(h2[...], jnp.concatenate([wg[e], wu[e]], axis=1))

    def mix(i):
        for n in FOUR:
            e = i * 4 + n
            a, up = raw[e, :, :FS], raw[e, :, FS:]
            ub[e] = (gx[e] * (a * (1.0 / (1.0 + jnp.exp(-a)))) * up).astype(BF16)

    def wait_up(sl, sem):
        for n, w in enumerate((wg, wu)):
            local(w.at[sl], w.at[sl], sem + n).wait()

    wait_up(pl.ds(0, 20), L_GU)

    @pl.when(here)
    def _():
        logits = mm(h2[...], wrt[...])
        for i in FOUR:
            act(i)
        lane_e = lane_iota((R, E)).astype(F32)
        chosen = picks[...]
        gates = jnp.zeros((R, E), F32)
        for k in EIGHT:
            on = jnp.concatenate([rm[s, :, k, :] for s in range(S)], axis=0) == 1
            mk = jnp.where(on, logits, NEG_FILL)
            pk = jnp.exp(mk - jnp.max(mk, axis=1, keepdims=True))
            pk = pk / jnp.sum(pk, axis=1, keepdims=True)
            gates = gates + jnp.where(chosen[:, k:k + 1] == lane_e, pk, 0.0)
        for e in range(E):
            gx[e] = jnp.broadcast_to(gates[:, e:e + 1], (R, 128))

        act(4)

    def down(n, first, count, width):
        u = jnp.concatenate([ub[e] for e in range(first, first + count)], axis=1)
        return mm(u, wd[first:first + count, :, n * CW:n * CW + width].reshape(count * FS, width))

    def rounded(x):
        return x.astype(BF16).astype(F32)

    send_a = [remote(pb.at[n], ab.at[n], S_P, R_P + n, partner) for n in range(NCH)]
    send_b = [remote(s2.at[n, chip], s2.at[n, chip], S_B, R_B + n, peer) for n in range(NCH)]
    send_d = [remote(pb.at[0], db.at[0], S_B, R_B + NCH, diag), remote(pb.at[0], db.at[1], S_B, R_B, peer)]
    send_last = [
        remote(s2.at[LAST, chip], s2.at[LAST, chip], S_B, R_B + LAST, diag),
        remote(s2.at[LAST, chip], s2.at[LAST, chip], S_B, R_B + LAST - 1, partner),
    ]
    send_y = [remote(yb.at[n], yb.at[n], S_P, R_P + n, partner) for n in range(NCH)]

    wait_up(pl.ds(20, 12), L_GU + 2)

    @pl.when(here)
    def _():
        for i in range(5, 8):
            act(i)
            mix(i - 5)
        for i in range(3, 7):
            mix(i)

    for m in range(NCH):
        down_copy(m, 0, E).wait()

        @pl.when(here)
        def _():
            if m == 0:
                mix(7)
            for h in TWO:
                dsum[h] = down(m, h * (E // 2), E // 2, CW)
            pb[m] = rounded(dsum[0] + dsum[1])

        @pl.when(core == 0)
        def _():
            send_a[m].start()
            if m == 0:
                send_d[0].start()

        @pl.when(core == 1)
        def _():
            if m == 0:
                send_d[1].start()
            for n in ((), (), (0, 1), (2, LAST))[m]:
                send_a[n].wait_recv()
                s2[n, chip] = ab[n] + pb[n]
                if n == LAST:
                    for c in send_last:
                        c.start()
                if n > 0:
                    send_b[n].start()

    def finish(n):
        yb[n] = xm4[n] + (s2[n, 0] + s2[n, 1])

    def put(n):
        hb[:, :, at(n, CW)] = yb[n].astype(BF16).reshape(S, B, CW)

    @pl.when(core == 1)
    def _():
        tails()
        for c in send_d:
            c.wait_recv()
        s2[0, 1 - chip] = db[0] + db[1]
        for n in range(NCH):
            if n > 0:
                send_b[n].wait_recv()
            finish(n)
            if n < LAST:
                send_y[n].start()
            put(n)
        for ref, snd in ((s2.at[:, chip], S_B), (s2.at[pl.ds(0, 2), chip], S_B), (yb.at[pl.ds(0, LAST)], S_P)):
            remote(ref, ref, snd, R_B, peer).wait_send()

    @pl.when(core == 0)
    def _():
        tails()
        send_d[0].wait_send()
        remote(pb, pb, S_P, R_B, peer).wait_send()
        for n in range(LAST):
            send_y[n].wait_recv()
            put(n)
        for c in send_last:
            c.wait_recv()
        finish(LAST)
        put(LAST)

    for ref, snd in ((mlall.at[pl.ds(0, 3)], S_ML), (obuf.at[1 - core], S_O), (c2.at[:, chip, pl.ds(0, 6)], S_C), (oall.at[core], S_G)):
        remote(ref, ref, snd, R_ML, partner).wait_send()


def write_kernel(h, tk, tv, h_out, tk_out, tv_out, sem):
    copies = [pltpu.make_async_copy(a, b, sem.at[i]) for i, (a, b) in enumerate(((h, h_out), (tk, tk_out), (tv, tv_out)))]
    for c in copies:
        c.start()
    for c in copies:
        c.wait()


def solution(mesh):
    def layer_steps(x_first, next_emb, k_cache, v_cache, seq_len, ln1_gain, ln1_bias, w_q, b_q, w_k, b_k, w_v, b_v, w_o, b_o, ln2_gain, ln2_bias, w_router, w_gate, w_up, w_down, long_factor, expert_idx, route_mask):
        def row(v):
            return v.reshape(1, -1)

        powers = (np.float32(ROPE_BASE) ** (np.arange(32, dtype=np.float32) * np.float32(2.0) / np.float32(HD))).astype(np.float32)
        base = jnp.asarray(np.tile(powers, 4)[None, :])
        args = (
            x_first, next_emb, jnp.transpose(k_cache, (0, 2, 3, 1)), jnp.transpose(v_cache, (0, 2, 3, 1)), seq_len,
            row(ln1_gain), row(ln1_bias), w_q, row(b_q), w_k, row(b_k), w_v, row(b_v), w_o, row(b_o), row(ln2_gain), row(ln2_bias),
            jnp.transpose(w_router), w_gate, w_up, w_down, row(long_factor), jnp.transpose(expert_idx, (0, 2, 1)), route_mask, base,
        )
        V = pltpu.VMEM
        scratch = [
            V((S, B, D), BF16), V((1, D), F32), V((1, D), F32), V((D, D), BF16), V((1, D), F32), V((D, 512), BF16), V((1, 512), F32),
            V((D, 512), BF16), V((1, 512), F32), V((2, 512, D), BF16), V((1, D), F32), V((1, D), F32), V((1, D), F32), V((E, D), BF16),
            V((E, D, FS), BF16), V((E, D, FS), BF16), V((E, FS, D), BF16), V((1, 32), F32), V((S, 8, B), jnp.int32),
            V((S, B, 8, E), jnp.int32), V((1, 128), F32), pltpu.SMEM((B,), jnp.int32), V((B, KV, HD, T), BF16), V((B, KV, HD, T), BF16),
            V((B, 8, 512), F32), V((S, B, 512), F32), V((S, B, 512), F32), V((B, 2, 32, T), F32), V((B, 2, 32, T), BF16),
            V((2, 8, 128), F32), V((4, 8, 128), F32), V((2, 2, 8, 8, 256), F32), V((2, 8, 8, 256), F32), V((2, 2, 8, 8, 256), F32),
            V((4, 8, 8, 512), F32), V((6, 8, 512), F32), V((6, 8, 512), F32), V((6, 8, 512), F32), V((2, 2, 6, 8, 256), F32),
            V((NCH, R, CW), F32), V((E, R, 128), F32), V((E, R, 2 * FS), F32), V((R, 512), F32), V((2, R, CW), F32), V((R, 8), F32), V((D, E), BF16), V((R, D), BF16), V((E, R, FS), BF16), V((NCH, R, CW), F32),
            V((NCH, R, CW), F32), V((2, R, CW), F32), V((NCH, 2, R, CW), F32), V((NCH, R, CW), F32), V((B, S, KV, HD), F32), V((B, S, KV, HD), F32),
            pltpu.SemaphoreType.DMA((NLOCAL,)), pltpu.SemaphoreType.DMA((NSEND,)), pltpu.SemaphoreType.DMA((NRECV,)),
        ]
        anyspec = pl.BlockSpec(memory_space=pl.ANY)
        outs = [((S, B, D), BF16), ((B, S, KV, HD), BF16), ((B, S, KV, HD), BF16)]
        vmem = pl.BlockSpec(memory_space=pltpu.VMEM)
        parts = pl.pallas_call(
            kernel,
            out_shape=tuple(V(*o) for o in outs),
            in_specs=[anyspec] * len(args),
            out_specs=(vmem,) * 3,
            scratch_shapes=scratch,
            compiler_params=pltpu.CompilerParams(collective_id=0, has_side_effects=True, vmem_limit_bytes=60 * 1024 * 1024),
        )(*args)
        return pl.pallas_call(
            write_kernel,
            out_shape=tuple(jax.ShapeDtypeStruct(*o) for o in outs),
            in_specs=[vmem] * 3,
            out_specs=(anyspec,) * 3,
            scratch_shapes=[pltpu.SemaphoreType.DMA((3,))],
            compiler_params=pltpu.CompilerParams(vmem_limit_bytes=1024 * 1024),
        )(*parts)

    replicated = P()
    in_specs = (P('dp'), P(None, 'dp'), P('dp', 'kv'), P('dp', 'kv'), P('dp')) + (replicated,) * 13 + (P(None, None, 'kv'), P(None, None, 'kv'), P(None, 'kv'), replicated, P(None, 'dp'), P(None, 'dp'))
    out_specs = (P(None, 'dp'), P('dp'), P('dp'))
    return jax.shard_map(layer_steps, mesh=mesh, in_specs=in_specs, out_specs=out_specs, check_vma=False)
```

```python
import functools
import itertools
import math

import jax
import jax.numpy as jnp
import numpy as np
from jax import lax
from jax.experimental import pallas as pl
from jax.experimental.pallas import tpu as pltpu
from jax.sharding import PartitionSpec as P

ROPE_BASE = 10000.0
ROPE_MSCALE = math.sqrt(1.0 + math.log(32.0) / math.log(4096.0))
NORM_EPS = 1e-5
NEG_FILL = -1e30
F32 = jnp.float32
BF16 = jnp.bfloat16

S = 3
B = 16
D = 1024
T = 256
KV = 8
HD = 64
E = 32
FS = 128
R = S * B
NCH = 4
CW = D // NCH
LAST = NCH - 1

GROUPS = 8
SMALL, PARTS = 8, 4
L_SMALL, L_WQ, L_K, L_V, L_WO, L_GU, L_DN, NLOCAL = itertools.accumulate((SMALL, 2, PARTS, PARTS, 1, PARTS, NCH), initial=0)
R_ML, R_O, R_C, R_G, R_P, R_B, NRECV = itertools.accumulate((3, 2, 2, 2, NCH, NCH + 1), initial=0)
S_ML, S_O, S_C, S_G, S_P, S_B, NSEND = range(7)
LN = 128
TWO, FOUR, EIGHT = range(2), range(4), range(8)


def at(i, width=LN):
    return slice(i * width, (i + 1) * width)


def mm(a, b):
    return jnp.dot(a, b, preferred_element_type=F32)


def mm_t(a, b):
    return lax.dot_general(a, b, (((1,), (1,)), ((), ())), preferred_element_type=F32)


def norm_rows(x, gain, bias):
    mean = jnp.mean(x, axis=-1, keepdims=True)
    cen = x - mean
    var = jnp.mean(cen * cen, axis=-1, keepdims=True)
    return (cen * lax.rsqrt(var + NORM_EPS) * gain + bias).astype(BF16)


def lane_iota(shape):
    return lax.broadcasted_iota(jnp.int32, shape, len(shape) - 1)


def kernel(
    x_first, next_emb, k_hbm, v_hbm, seq_hbm, g1_h, b1_h, wq_h, bq_h, wk_h, bk_h, wv_h, bv_h, wo_h, bo_h, g2_h, b2_h,
    wr_h, wg_h, wu_h, wd_h, lf_h, idx_h, rm_h, base_h,
    hb, tkb, tvb,
    xb, g1, b1, wq, bq, wk, bk, wv, bv, wo, bo, g2, b2, wr, wg, wu, wd, lf, idx, rm, base, seq_s, kc, vc,
    qbuf, kbuf, vbuf, sbuf, wbuf, mlb, mlall, obuf, orecv, c2, ex, ga, gb, tl, oall, xm4, gx, raw, qraw, dsum, picks, wrt, h2, ub, pb, ab, db, s2, yb, tkf, tvf,
    lsem, ssem, rsem,
):
    me = lax.axis_index("kv")
    core = me % 2
    chip = me // 2
    partner = me + 1 - 2 * core
    peer = (me + 2) % 4
    diag = (partner + 2) % 4

    def local(src, dst, i):
        return pltpu.make_async_copy(src, dst, lsem.at[i])

    def remote(src, dst, snd, rcv, dev):
        return pltpu.make_async_remote_copy(
            src_ref=src, dst_ref=dst, send_sem=ssem.at[snd], recv_sem=rsem.at[rcv],
            device_id={"kv": dev}, device_id_type=pl.DeviceIdType.MESH)

    small = [
        local(src, dst, L_SMALL + i % SMALL) for i, (src, dst) in enumerate((
            (x_first, xb.at[0]), (next_emb, xb.at[pl.ds(1, S - 1)]), (g1_h, g1), (b1_h, b1), (bq_h, bq), (lf_h, lf), (base_h, base),
            (seq_hbm, seq_s), (bk_h, bk), (bv_h, bv), (bo_h, bo), (g2_h, g2), (b2_h, b2), (wr_h, wr), (idx_h, idx), (rm_h, rm)))
    ]
    first, later = small[:SMALL], small[SMALL:]
    cp_wq = [local(wq_h.at[:, pl.ds(i * 512, 512)], wq.at[:, pl.ds(i * 512, 512)], L_WQ + i) for i in TWO]
    other, own = (1 - core) * 8, core * 8

    def k_part(i):
        sl = pl.ds((other if i < 2 else own) + (i % 2) * 4, 4)
        return local(k_hbm.at[sl], kc.at[sl], L_K + i)

    def v_part(i):
        sl = (pl.ds(other if i < 2 else own, 8), pl.ds((i % 2) * 4, 4))
        return local(v_hbm.at[sl], vc.at[sl], L_V + i)

    cp_k = [k_part(i) for i in FOUR]
    cp_v = [v_part(i) for i in FOUR]
    cp_wkv = [local(wk_h, wk, L_WQ), local(wv_h, wv, L_WQ + 1)]
    cp_wo = [
        local(wo_h.at[pl.ds(kv * 128 + g * 64, 64)], wo.at[g, pl.ds(kv * 64, 64)], L_WO) for kv in range(KV) for g in TWO
    ]

    def up_copy(src, dst, i, sem):
        sl = pl.ds(i * 4, 4)
        return local(src.at[sl], dst.at[sl], sem)

    def down_copy(m, e, n):
        sl = (pl.ds(e, n), pl.ds(0, FS), pl.ds(m * CW, CW))
        return local(wd_h.at[sl], wd.at[sl], L_DN + m)

    for c in first + cp_wq + cp_k[:3] + cp_v[:1] + cp_k[3:]:
        c.start()
    bar = pltpu.get_barrier_semaphore()
    for dev in (partner, peer, diag):
        pl.semaphore_signal(bar, inc=1, device_id={"kv": dev}, device_id_type=pl.DeviceIdType.MESH)
    qbuf[:, 6:8, :] = jnp.zeros((B, 2, 512), F32)

    for c in first:
        c.wait()
    for c in cp_v[1:]:
        c.start()

    lane48 = lane_iota((R, 128))
    inv = 1.0 / (jnp.concatenate([lf[...]] * 4, axis=1) * base[...])
    row_b = lax.broadcasted_iota(jnp.int32, (B, 128), 0)
    len_rows = jnp.zeros((B, 128), jnp.int32)
    for b in range(B):
        len_rows = jnp.where(row_b == b, seq_s[b], len_rows)
    angles = jnp.concatenate([(len_rows + s).astype(F32) for s in range(S)], axis=0) * inv
    cosv = jnp.cos(angles) * ROPE_MSCALE
    sinv = jnp.sin(angles) * ROPE_MSCALE
    low_half = (lane48 % HD) < (HD // 2)

    def rope(x, both=False):
        xf = x.astype(BF16).astype(F32)
        up, down_ = pltpu.roll(xf, 96, 1), pltpu.roll(xf, 32, 1)
        plain = (xf * cosv + jnp.where(low_half, -up, down_) * sinv).astype(BF16).astype(F32)
        if not both:
            return plain
        return plain, (pltpu.roll(xf, HD, 1) * cosv + jnp.where(low_half, -down_, up) * sinv).astype(BF16).astype(F32)

    h1 = norm_rows(xb[...].reshape(R, D).astype(F32), g1[...], b1[...])

    left = lane48 < HD

    def put_q(q, p):
        qa, qa_x = rope(q[:, :LN], True)
        qb, qb_x = rope(q[:, LN:], True)
        pair = (jnp.where(left, qa, qb_x) * 0.125, jnp.where(left, qa_x, qb) * 0.125)
        for g in TWO:
            for s in range(S):
                qbuf[:, 2 * s + g, at(p)] = pair[g][at(s, B)]

    cp_wq[0].wait()
    q_lo = mm(h1, wq[:, :512]) + bq[:, :512]
    qraw[...] = q_lo
    cp_wq[1].wait()
    for c in later + cp_wo + cp_wkv:
        c.start()
    q_hi = mm(h1, wq[:, 512:]) + bq[:, 512:]
    for p in FOUR:
        put_q(qraw[:, p * 256:(p + 1) * 256] if p < 2 else q_hi[:, (p - 2) * 256:(p - 1) * 256], p)

    rowq = lax.broadcasted_iota(jnp.int32, (32, T), 0)
    laneq = lane_iota((32, T))
    diag_mask = (rowq // 8) == (laneq // HD)
    pos = laneq + me * T
    lane8 = lane_iota((8, 128))

    def scores(start, i):
        qv = qbuf[start + i]
        for hh in TWO:
            rep = jnp.concatenate([qv[:, at(hh, T)]] * 4, axis=0)
            lhs = jnp.where(diag_mask, rep, 0.0).astype(BF16)
            sbuf[start + i, hh] = mm(lhs, kc[start + i, at(hh, 4)].reshape(256, T))

    def soft(start, i, acc):
        keep = pos < seq_s[start + i]
        for hh in TWO:
            sc = jnp.where(keep, sbuf[start + i, hh], NEG_FILL)
            m = jnp.max(sc, axis=1, keepdims=True)
            w = jnp.where(keep, jnp.exp(sc - m), 0.0)
            l = jnp.sum(w, axis=1, keepdims=True)
            wbuf[start + i, hh] = w.astype(BF16)
            for j in FOUR:
                spot = i * 16 + hh * 4 + j
                acc = jnp.where(lane8 == spot, m[at(j, 8)], acc)
                acc = jnp.where(lane8 == spot + 8, l[at(j, 8)], acc)
        return acc

    left8 = lane8 < HD

    def values(half, i, hh):
        b = half * 8 + i
        pv = mm_t(wbuf[b, hh], vc[b, at(hh, 4)].reshape(256, T))
        obuf[half, hh, i, :, 0:128] = jnp.where(left8, pv[0:8, 0:128], pv[8:16, 0:128])
        obuf[half, hh, i, :, 128:256] = jnp.where(left8, pv[16:24, 128:256], pv[24:32, 128:256])

    send_ml = [
        remote(mlb.at[1 - core], mlall.at[me], S_ML, R_ML, partner), remote(mlb.at[core], mlall.at[me], S_ML, R_ML + 1, peer),
        remote(mlb.at[1 - core], mlall.at[me], S_ML, R_ML + 2, diag),
    ]
    send_o = [remote(obuf.at[1 - core, hh], orecv.at[hh], S_O, R_O + hh, partner) for hh in TWO]
    zero = jnp.zeros((8, 128), F32)

    cp_k[0].wait()
    for i in FOUR:
        scores(other, i)
    cp_k[1].wait()
    for i in FOUR:
        scores(other, 4 + i)
    acc = zero
    for i in FOUR:
        acc = soft(other, i, acc)
    cp_k[2].wait()
    for i in range(GROUPS):
        sem = L_GU + 2 * (i // 5)
        up_copy(wg_h, wg, i, sem).start()
        up_copy(wu_h, wu, i, sem + 1).start()
    for i in FOUR:
        scores(own, i)
    for i in FOUR:
        acc = soft(other, 4 + i, acc)
    mlb[1 - core] = acc
    pl.semaphore_wait(bar, 3)
    send_ml[0].start()
    send_ml[2].start()

    cp_v[0].wait()
    for i in EIGHT:
        values(1 - core, i, 0)
    acc = zero
    for i in FOUR:
        acc = soft(own, i, acc)
    send_o[0].start()
    cp_k[3].wait()
    for i in FOUR:
        scores(own, 4 + i)
    cp_v[1].wait()
    for m in range(NCH):
        for i in range(GROUPS):
            down_copy(m, i * 4, 4).start()
    for i in EIGHT:
        values(1 - core, i, 1)
    for i in FOUR:
        acc = soft(own, 4 + i, acc)
    mlb[core] = acc
    mlall[me] = acc
    send_o[1].start()
    send_ml[1].start()
    cp_v[2].wait()
    for i in EIGHT:
        values(core, i, 0)

    pick = (lane8 // HD)

    def spread(v, i, p):
        return jnp.take_along_axis(v, pick + (i * 16 + 2 * p), axis=1, mode="promise_in_bounds")

    send_c = [remote(c2.at[hh, chip, pl.ds(0, 6)], c2.at[hh, chip, pl.ds(0, 6)], S_C, R_C + hh, peer) for hh in TWO]
    for hh in TWO:
        if hh == 1:
            cp_v[3].wait()
            for i in EIGHT:
                values(core, i, 1)
        else:
            send_ml[0].wait_recv()
            ml_a = mlall[me]
            ml_b = mlall[partner]
            m_ab = jnp.maximum(ml_a, ml_b)
            f_a = jnp.exp(ml_a - m_ab)
            f_b = jnp.exp(ml_b - m_ab)
        send_o[hh].wait_recv()
        for i in EIGHT:
            oa = obuf[core, hh, i]
            ob = orecv[hh, i]
            for p in TWO:
                ln = at(p)
                c2[hh, chip, :, i, ln] = (
                    oa[:, ln] * spread(f_a, i, 2 * hh + p) + ob[:, ln] * spread(f_b, i, 2 * hh + p))
        send_c[hh].start()

    for c in later + cp_wkv:
        c.wait()
    for c in send_ml[1:]:
        c.wait_recv()
    kn = mm(h1, wk[...]) + bk[...]
    vn = (mm(h1, wv[...]) + bv[...]).astype(BF16)
    vn = vn.astype(F32)
    for p in FOUR:
        ln = at(p)
        for val, buf in ((rope(kn[:, ln]), kbuf), (vn[:, ln], vbuf)):
            for s in range(S):
                buf[s, :, ln] = val[at(s, B)]

    def tails():
        for buf, fin, out in ((kbuf, tkf, tkb), (vbuf, tvf, tvb)):
            for p in FOUR:
                for s in range(S):
                    val = buf[s, :, at(p)]
                    fin[:, s, 2 * p, :] = val[:, :HD]
                    fin[:, s, 2 * p + 1, :] = pltpu.roll(val, HD, 1)[:, :HD]
            out[...] = fin[...].astype(BF16)

    rows = pl.ds(pl.multiple_of(core * 8, 8), 8)
    kt = [kbuf[t, rows, :] for t in range(S)]
    vt = [vbuf[t, rows, :] for t in range(S)]
    trip = [(s, g, t) for s in range(S) for g in TWO for t in range(s + 1)]
    prod = jnp.concatenate([qbuf[rows, 2 * s + g, :] * kt[t] for s, g, t in trip], axis=0)
    hi = prod.astype(BF16)
    lo = (prod - hi.astype(F32)).astype(BF16)
    r2 = lax.broadcasted_iota(jnp.int32, (256, 128), 0)
    ones = jnp.where(((r2 % 128) // HD) == (lane_iota((256, 128)) // HD), 1.0, 0.0).astype(BF16)
    tsc = jnp.concatenate(
        [mm(jnp.concatenate([hi[:, at(p)], lo[:, at(p)]], axis=1), ones) for p in FOUR], axis=1)

    ml = [mlall[d] for d in FOUR]
    for ch in TWO:
        a, b_ = ml[2 * ch], ml[2 * ch + 1]
        mc = jnp.maximum(a, b_)
        lc = (pltpu.roll(a, 120, 1) * jnp.exp(a - mc) + pltpu.roll(b_, 120, 1) * jnp.exp(b_ - mc))
        for i in EIGHT:
            for p in FOUR:
                ln = at(p)
                ex[2 * ch, :, i, ln] = spread(mc, i, p)
                ex[2 * ch + 1, :, i, ln] = spread(lc, i, p)

    for s in range(S):
        for g in TWO:
            j = 2 * s + g
            sc = [tsc[at(n, 8)] for n, key in enumerate(trip) if key[:2] == (s, g)]
            mt = functools.reduce(jnp.maximum, sc)
            wt = [jnp.exp(v - mt) for v in sc]
            lt = functools.reduce(jnp.add, wt)
            ot = functools.reduce(jnp.add, [w.astype(BF16).astype(F32) * v for w, v in zip(wt, vt)])
            m0, l0, m1, l1 = ex[0, j], ex[1, j], ex[2, j], ex[3, j]
            top = jnp.maximum(jnp.maximum(m0, m1), mt)
            f0, f1, ft = jnp.exp(m0 - top), jnp.exp(m1 - top), jnp.exp(mt - top)
            inv_l = 1.0 / (l0 * f0 + l1 * f1 + lt * ft)
            ga[j] = f0 * inv_l
            gb[j] = f1 * inv_l
            tl[j] = ot * (ft * inv_l)

    send_g = [remote(oall.at[core, hh], oall.at[core, hh], S_G, R_G + hh, partner) for hh in TWO]
    for hh in TWO:
        send_c[hh].wait_recv()
        ln = at(hh, T)
        for j in range(6):
            oall[core, hh, j] = c2[hh, 0, j] * ga[j][:, ln] + c2[hh, 1, j] * gb[j][:, ln] + tl[j][:, ln]
        send_g[hh].start()

    eye = jnp.where(lax.broadcasted_iota(jnp.int32, (B, B), 0) == lane_iota((B, B)), 1.0, 0.0)
    picks[...] = jnp.concatenate([mm_t(eye, idx[s].astype(F32)) for s in range(S)], axis=0)

    eye_e = jnp.where(lax.broadcasted_iota(jnp.int32, (E, E), 0) == lane_iota((E, E)), 1.0, 0.0).astype(BF16)
    wrt[...] = lax.dot_general(wr[...], eye_e, (((0,), (0,)), ((), ())), preferred_element_type=F32).astype(BF16)

    here = me < 4

    @pl.when(here)
    def _():
        local(wo, wo, L_WO).wait()
        att = None
        for hh in TWO:
            send_g[hh].wait_recv()
            for g in TWO:
                o_g = jnp.concatenate([oall[h, hh, 2 * s + g] for s in range(S) for h in TWO], axis=0).astype(BF16)
                part = mm(o_g, wo[g, at(hh, T)])
                att = part if att is None else att + part
        xm = (xb[...].reshape(R, D).astype(F32) + att + bo[...]).astype(BF16).astype(F32)
        for n in range(NCH):
            xm4[n] = xm[:, at(n, CW)]
        h2[...] = norm_rows(xm, g2[...], b2[...])

    def act(i):
        for n in FOUR:
            e = i * 4 + n
            raw[e] = mm(h2[...], jnp.concatenate([wg[e], wu[e]], axis=1))

    def mix(i):
        for n in FOUR:
            e = i * 4 + n
            a, up = raw[e, :, :FS], raw[e, :, FS:]
            ub[e] = (gx[e] * (a * (1.0 / (1.0 + jnp.exp(-a)))) * up).astype(BF16)

    def wait_up(sl, sem):
        for n, w in enumerate((wg, wu)):
            local(w.at[sl], w.at[sl], sem + n).wait()

    wait_up(pl.ds(0, 20), L_GU)

    @pl.when(here)
    def _():
        logits = mm(h2[...], wrt[...])
        for i in FOUR:
            act(i)
        lane_e = lane_iota((R, E)).astype(F32)
        chosen = picks[...]
        gates = jnp.zeros((R, E), F32)
        for k in EIGHT:
            on = jnp.concatenate([rm[s, :, k, :] for s in range(S)], axis=0) == 1
            mk = jnp.where(on, logits, NEG_FILL)
            pk = jnp.exp(mk - jnp.max(mk, axis=1, keepdims=True))
            pk = pk / jnp.sum(pk, axis=1, keepdims=True)
            gates = gates + jnp.where(chosen[:, k:k + 1] == lane_e, pk, 0.0)
        for e in range(E):
            gx[e] = jnp.broadcast_to(gates[:, e:e + 1], (R, 128))

        act(4)

    def down(n, first, count, width):
        u = jnp.concatenate([ub[e] for e in range(first, first + count)], axis=1)
        return mm(u, wd[first:first + count, :, n * CW:n * CW + width].reshape(count * FS, width))

    def rounded(x):
        return x.astype(BF16).astype(F32)

    send_a = [remote(pb.at[n], ab.at[n], S_P, R_P + n, partner) for n in range(NCH)]
    send_b = [remote(s2.at[n, chip], s2.at[n, chip], S_B, R_B + n, peer) for n in range(NCH)]
    send_d = [remote(pb.at[0], db.at[0], S_B, R_B + NCH, diag), remote(pb.at[0], db.at[1], S_B, R_B, peer)]
    send_last = [
        remote(s2.at[LAST, chip], s2.at[LAST, chip], S_B, R_B + LAST, diag),
        remote(s2.at[LAST, chip], s2.at[LAST, chip], S_B, R_B + LAST - 1, partner),
    ]
    send_y = [remote(yb.at[n], yb.at[n], S_P, R_P + n, partner) for n in range(NCH)]

    wait_up(pl.ds(20, 12), L_GU + 2)

    @pl.when(here)
    def _():
        for i in range(5, 8):
            act(i)
            mix(i - 5)
        for i in range(3, 7):
            mix(i)

    for m in range(NCH):
        down_copy(m, 0, E).wait()

        @pl.when(here)
        def _():
            if m == 0:
                mix(7)
            for h in TWO:
                dsum[h] = down(m, h * (E // 2), E // 2, CW)
            pb[m] = rounded(dsum[0] + dsum[1])

        @pl.when(core == 0)
        def _():
            send_a[m].start()
            if m == 0:
                send_d[0].start()

        @pl.when(core == 1)
        def _():
            if m == 0:
                send_d[1].start()
            for n in ((), (), (0, 1), (2, LAST))[m]:
                send_a[n].wait_recv()
                s2[n, chip] = ab[n] + pb[n]
                if n == LAST:
                    for c in send_last:
                        c.start()
                if n > 0:
                    send_b[n].start()

    def finish(n):
        yb[n] = xm4[n] + (s2[n, 0] + s2[n, 1])

    def put(n):
        hb[:, :, at(n, CW)] = yb[n].astype(BF16).reshape(S, B, CW)

    @pl.when(core == 1)
    def _():
        tails()
        for c in send_d:
            c.wait_recv()
        s2[0, 1 - chip] = db[0] + db[1]
        for n in range(NCH):
            if n > 0:
                send_b[n].wait_recv()
            finish(n)
            if n < LAST:
                send_y[n].start()
            put(n)
        for ref, snd in ((s2.at[:, chip], S_B), (s2.at[pl.ds(0, 2), chip], S_B), (yb.at[pl.ds(0, LAST)], S_P)):
            remote(ref, ref, snd, R_B, peer).wait_send()

    @pl.when(core == 0)
    def _():
        tails()
        send_d[0].wait_send()
        remote(pb, pb, S_P, R_B, peer).wait_send()
        for n in range(LAST):
            if n == LAST - 1:
                for c in send_last:
                    c.wait_recv()
                finish(LAST)
                put(LAST)
            send_y[n].wait_recv()
            put(n)

    for ref, snd in ((mlall.at[pl.ds(0, 3)], S_ML), (obuf.at[1 - core], S_O), (c2.at[:, chip, pl.ds(0, 6)], S_C), (oall.at[core], S_G)):
        remote(ref, ref, snd, R_ML, partner).wait_send()


def write_kernel(h, tk, tv, h_out, tk_out, tv_out, sem):
    copies = [pltpu.make_async_copy(a, b, sem.at[i]) for i, (a, b) in enumerate(((h, h_out), (tk, tk_out), (tv, tv_out)))]
    for c in copies:
        c.start()
    for c in copies:
        c.wait()


def solution(mesh):
    def layer_steps(x_first, next_emb, k_cache, v_cache, seq_len, ln1_gain, ln1_bias, w_q, b_q, w_k, b_k, w_v, b_v, w_o, b_o, ln2_gain, ln2_bias, w_router, w_gate, w_up, w_down, long_factor, expert_idx, route_mask):
        def row(v):
            return v.reshape(1, -1)

        powers = (np.float32(ROPE_BASE) ** (np.arange(32, dtype=np.float32) * np.float32(2.0) / np.float32(HD))).astype(np.float32)
        base = jnp.asarray(np.tile(powers, 4)[None, :])
        args = (
            x_first, next_emb, jnp.transpose(k_cache, (0, 2, 3, 1)), jnp.transpose(v_cache, (0, 2, 3, 1)), seq_len,
            row(ln1_gain), row(ln1_bias), w_q, row(b_q), w_k, row(b_k), w_v, row(b_v), w_o, row(b_o), row(ln2_gain), row(ln2_bias),
            jnp.transpose(w_router), w_gate, w_up, w_down, row(long_factor), jnp.transpose(expert_idx, (0, 2, 1)), route_mask, base,
        )
        V = pltpu.VMEM
        scratch = [
            V((S, B, D), BF16), V((1, D), F32), V((1, D), F32), V((D, D), BF16), V((1, D), F32), V((D, 512), BF16), V((1, 512), F32),
            V((D, 512), BF16), V((1, 512), F32), V((2, 512, D), BF16), V((1, D), F32), V((1, D), F32), V((1, D), F32), V((E, D), BF16),
            V((E, D, FS), BF16), V((E, D, FS), BF16), V((E, FS, D), BF16), V((1, 32), F32), V((S, 8, B), jnp.int32),
            V((S, B, 8, E), jnp.int32), V((1, 128), F32), pltpu.SMEM((B,), jnp.int32), V((B, KV, HD, T), BF16), V((B, KV, HD, T), BF16),
            V((B, 8, 512), F32), V((S, B, 512), F32), V((S, B, 512), F32), V((B, 2, 32, T), F32), V((B, 2, 32, T), BF16),
            V((2, 8, 128), F32), V((4, 8, 128), F32), V((2, 2, 8, 8, 256), F32), V((2, 8, 8, 256), F32), V((2, 2, 8, 8, 256), F32),
            V((4, 8, 8, 512), F32), V((6, 8, 512), F32), V((6, 8, 512), F32), V((6, 8, 512), F32), V((2, 2, 6, 8, 256), F32),
            V((NCH, R, CW), F32), V((E, R, 128), F32), V((E, R, 2 * FS), F32), V((R, 512), F32), V((2, R, CW), F32), V((R, 8), F32), V((D, E), BF16), V((R, D), BF16), V((E, R, FS), BF16), V((NCH, R, CW), F32),
            V((NCH, R, CW), F32), V((2, R, CW), F32), V((NCH, 2, R, CW), F32), V((NCH, R, CW), F32), V((B, S, KV, HD), F32), V((B, S, KV, HD), F32),
            pltpu.SemaphoreType.DMA((NLOCAL,)), pltpu.SemaphoreType.DMA((NSEND,)), pltpu.SemaphoreType.DMA((NRECV,)),
        ]
        anyspec = pl.BlockSpec(memory_space=pl.ANY)
        outs = [((S, B, D), BF16), ((B, S, KV, HD), BF16), ((B, S, KV, HD), BF16)]
        vmem = pl.BlockSpec(memory_space=pltpu.VMEM)
        parts = pl.pallas_call(
            kernel,
            out_shape=tuple(V(*o) for o in outs),
            in_specs=[anyspec] * len(args),
            out_specs=(vmem,) * 3,
            scratch_shapes=scratch,
            compiler_params=pltpu.CompilerParams(collective_id=0, has_side_effects=True, vmem_limit_bytes=60 * 1024 * 1024),
        )(*args)
        return pl.pallas_call(
            write_kernel,
            out_shape=tuple(jax.ShapeDtypeStruct(*o) for o in outs),
            in_specs=[vmem] * 3,
            out_specs=(anyspec,) * 3,
            scratch_shapes=[pltpu.SemaphoreType.DMA((3,))],
            compiler_params=pltpu.CompilerParams(vmem_limit_bytes=1024 * 1024),
        )(*parts)

    replicated = P()
    in_specs = (P('dp'), P(None, 'dp'), P('dp', 'kv'), P('dp', 'kv'), P('dp')) + (replicated,) * 13 + (P(None, None, 'kv'), P(None, None, 'kv'), P(None, 'kv'), replicated, P(None, 'dp'), P(None, 'dp'))
    out_specs = (P(None, 'dp'), P('dp'), P('dp'))
    return jax.shard_map(layer_steps, mesh=mesh, in_specs=in_specs, out_specs=out_specs, check_vma=False)
```
